32 devices in a mesh: dp: 8 (over y, x, core), tensor: 4 (over z).
Axes of the slice: x: 2, y: 2, z: 4, core: 2. Of those that a mesh axis runs over, the one named last changes fastest.
Arguments:
- tokens: bfloat16 [16, 1024, 768], P('dp', 'tensor'), may hold values from -6 to 6
- prefix_len: int32 [16], P('dp'), may hold values from 102 to 512, as said below
- w_qkv: bfloat16 [768, 3, 768], P('dp', None, 'tensor'), may hold values from -0.21875 to 0.21875
- bias_qv: bfloat16 [2, 768], P(None, ('tensor', 'dp')), may hold values from -0.59765625 to 0.59765625
- w_out: bfloat16 [768, 768], P('tensor', 'dp'), may hold values from -1.5 to 1.5
- w_up: bfloat16 [768, 3072], P('dp', 'tensor'), may hold values from -0.21875 to 0.21875
- bias_up: bfloat16 [3072], P(('tensor', 'dp')), may hold values from -1.796875 to 1.796875
- w_down: bfloat16 [3072, 768], P('tensor', 'dp'), may hold values from -0.15625 to 0.15625
- gains: bfloat16 [2, 768], P(None, ('dp', 'tensor')), may hold values from 0.5 to 1.5
- shifts: bfloat16 [4, 768], P(None, ('dp', 'tensor')), may hold values from -1.1953125 to 1.1953125
- cotangent: bfloat16 [16, 1024, 768], P('dp', 'tensor'), may hold values from -6 to 6
Outputs:
- output: bfloat16 [16, 1024, 768], P('dp', 'tensor')
- token_grad: float32 [16, 1024, 768], P('dp', 'tensor')
- grad_qkv: float32 [768, 3, 768], P('dp', None, 'tensor')
- grad_bias_qv: float32 [2, 768], P(None, ('tensor', 'dp'))
- grad_out: float32 [768, 768], P('tensor', 'dp')
- grad_up: float32 [768, 3072], P('dp', 'tensor')
- grad_bias_up: float32 [3072], P(('tensor', 'dp'))
- grad_down: float32 [3072, 768], P('tensor', 'dp')
- grad_gains: float32 [2, 768], P(None, ('dp', 'tensor'))
- grad_shifts: float32 [4, 768], P(None, ('dp', 'tensor'))
The draws below stay inside these ranges and needn't reach their ends.
Inputs may be any that keep to these rules, and one draw needn't show every extreme that they name: `prefix_len`: the number of leading positions of a sequence that every position sees; the least and the greatest value occur in every draw.
All inputs are finite; a program needn't handle non-finite values.
Results may differ from the reference program's by a relative error of at most 0.02.
Values may be sent and summed in bfloat16 or wider, within the bound.
A program may use at most 192 MiB of HBM per device.

```python
import jax
import jax.numpy as jnp
from jax import lax

D = 768
H = 12
DH = 64
FF = 3072
L = 1024
SEQ_DEV = 2
SEQS = 16
N_DP = 8


def draw_prefix_len(key, part):
    lowest = L // 10
    highest = L // 2
    key_list = jax.random.split(key, 3)
    values = jax.random.randint(key_list[0], (SEQS,), lowest, highest + 1)
    first_slot = jax.random.randint(key_list[1], (), 0, SEQS)
    offset = jax.random.randint(key_list[2], (), 1, SEQS)
    second_slot = (first_slot + offset) % SEQS
    values = values.at[first_slot].set(highest)
    values = values.at[second_slot].set(lowest)
    return values.astype(jnp.int32)


def with_spikes(drawn, rng, source, target, parts, factor):
    def block_of(axis_at):
        return (jnp.arange(drawn.shape[axis_at]) // (drawn.shape[axis_at] // parts)).reshape((-1,) + (1,) * (drawn.ndim - 1 - axis_at))

    first = jax.random.permutation(rng, parts)[block_of(target)]
    other_side = (block_of(target) + parts // 2) % parts
    return jnp.where((block_of(source) == first) | (block_of(source) == other_side), factor * drawn, drawn)


def levels(key, shape, cuts, least, high):
    factor_of, own = 1.0, jax.random.fold_in(key, 6)
    for axis_at, shards_of in cuts:
        heights = jnp.exp(jax.random.uniform(jax.random.fold_in(own, axis_at), (shards_of,), jnp.float32, least / len(cuts), high / len(cuts)))
        factor_of = factor_of * jnp.repeat(heights, shape[axis_at] // shards_of).reshape([-1 if axis == axis_at else 1 for axis in range(len(shape))])
    return factor_of


def noise(stream_key, shape, width, reach, shards=(), kind=jnp.bfloat16):
    loudness = levels(stream_key, shape, shards, -0.22, 0.18) if shards else 1.0
    values = jax.random.normal(stream_key, shape, jnp.float32) * width * loudness
    return jnp.minimum(jnp.maximum(values, -reach), reach).astype(kind)


def heavy_noise(stream_key, shape, scale, most, shards, heavy, kind=jnp.bfloat16):
    values = scale * jax.random.normal(stream_key, shape, jnp.float32)
    if shards:
        values = values * levels(stream_key, shape, shards, -0.22, 0.18)
    return jnp.clip(with_spikes(values, jax.random.fold_in(stream_key, 3), *heavy), -most, most).astype(kind)


def setup_inputs(seed: int = 0) -> dict:
    streams_of = jax.random.split(jax.random.key(seed), 12)
    tokens = noise(streams_of[0], (SEQS, L, D), 1.0, 6.0, ((0, 8), (1, 4)))
    prefix_len = draw_prefix_len(jax.random.fold_in(streams_of[11], 71), 0)
    w_qkv = noise(streams_of[2], (D, 3, D), D ** -0.5, 0.21875, ((0, 8), (2, 4)))
    bias_qv = noise(streams_of[3], (2, D), 0.1, 0.59765625, ((1, 32),))
    w_out = noise(streams_of[4], (D, D), 16 ** -0.5, 1.5, ((0, 4), (1, 8)))
    w_up = noise(streams_of[5], (D, FF), D ** -0.5, 0.21875, ((0, 8), (1, 4)))
    bias_up = noise(streams_of[6], (FF,), 0.3, 1.796875, ((0, 32),))
    w_down = noise(streams_of[7], (FF, D), (FF // 2) ** -0.5, 0.15625, ((0, 4), (1, 8)))
    gains = jnp.clip(1.0 + 0.1 * jax.random.normal(streams_of[8], (2, D), jnp.float32), 0.5, 1.5).astype(jnp.bfloat16)
    shifts = noise(streams_of[9], (4, D), 0.2, 1.1953125, ((1, 32),))
    cotangent = heavy_noise(streams_of[10], (SEQS, L, D), 1.0, 6.0, ((0, 8), (1, 4)), (0, 2, 8, 2.0))
    return dict(tokens=tokens, prefix_len=prefix_len, w_qkv=w_qkv, bias_qv=bias_qv, w_out=w_out, w_up=w_up, bias_up=bias_up, w_down=w_down, gains=gains, shifts=shifts, cotangent=cotangent)


@jax.custom_vjp
def low(v):
    return lax.optimization_barrier(v.astype(jnp.bfloat16)).astype(jnp.float32)

@jax.custom_vjp
def low_back(v):
    return v

def low_keep(v):
    return (low(v), None)

def low_pass(kept, grad):
    return (grad,)

def back_keep(v):
    return (v, None)

def back_low(kept, grad):
    return (low(grad),)
low.defvjp(low_keep, low_pass)
low_back.defvjp(back_keep, back_low)
HIGHEST = lax.Precision.HIGHEST
EPSILON = 1e-05
MASKED_SCORE = -1e+30

def layer_norm(values, gain_row, shift_row):
    center = values - lax.optimization_barrier(jnp.mean(values, axis=-1, keepdims=True))
    inverse = lax.rsqrt(lax.optimization_barrier(jnp.mean(center * center, axis=-1, keepdims=True)) + EPSILON)
    return center * inverse * gain_row + shift_row

def attend_block(queries, key_heads, value_heads, offset, prefix):
    block_rows = queries.shape[0]
    scores = jnp.einsum('qhd,khd->hqk', queries, key_heads, precision=HIGHEST) * DH ** (-0.5)
    scores = low_back(scores)
    row_ids = offset + jnp.arange(block_rows, dtype=jnp.int32)[:, None]
    column_ids = jnp.arange(key_heads.shape[0], dtype=jnp.int32)[None, :]
    allowed = jnp.logical_or(column_ids < prefix, column_ids <= row_ids)
    scores = jnp.where(allowed[None], scores, MASKED_SCORE)
    row_max = lax.optimization_barrier(jnp.max(scores, axis=-1, keepdims=True))
    log_total = jnp.log(lax.optimization_barrier(jnp.sum(jnp.exp(scores - row_max), axis=-1, keepdims=True))) + row_max
    attn_probs = low(jnp.exp(scores - log_total))
    return jnp.einsum('hqk,khd->qhd', attn_probs, value_heads, precision=HIGHEST)

def sequence_attention(inputs):
    queries, key_heads, value_heads, prefix = inputs
    block_rows = min(512, L)
    starts = jnp.arange(0, L, block_rows, dtype=jnp.int32)

    def one_block(offset):
        chosen = lax.dynamic_slice_in_dim(queries, offset.astype(jnp.int32), block_rows, 0)
        return attend_block(chosen, key_heads, value_heads, offset.astype(jnp.int32), prefix)
    pieces = lax.map(jax.checkpoint(one_block), starts)
    return pieces.reshape(L, H * DH)

def forward(tokens, w_qkv, bias_qv, w_out, w_up, bias_up, w_down, gains, shifts, prefix):
    seq_count = tokens.shape[0]
    projected = jnp.einsum('gld,dce->glce', tokens, w_qkv, precision=HIGHEST)
    queries = low(low_back(projected[:, :, 0] + bias_qv[0])).reshape(seq_count, L, H, DH)
    key_heads = low(low_back(projected[:, :, 1])).reshape(seq_count, L, H, DH)
    value_heads = low(low_back(projected[:, :, 2] + bias_qv[1])).reshape(seq_count, L, H, DH)
    context = lax.map(sequence_attention, (queries, key_heads, value_heads, prefix))
    context = low(low_back(context))
    branch = low_back(jnp.einsum('gle,ed->gld', context, w_out, precision=HIGHEST) + shifts[0])
    normed = layer_norm(tokens + branch, gains[0], shifts[1])
    normed_low = low(normed)
    pre_active = low_back(jnp.einsum('gld,df->glf', normed_low, w_up, precision=HIGHEST) + bias_up)
    active = low(jax.nn.gelu(pre_active, approximate=False))
    feed_out = low_back(jnp.einsum('glf,fd->gld', active, w_down, precision=HIGHEST) + shifts[2])
    return layer_norm(normed + feed_out, gains[1], shifts[3])

def reference(tokens, prefix_len, w_qkv, bias_qv, w_out, w_up, bias_up, w_down, gains, shifts, cotangent):
    params = tuple((argument.astype(jnp.float32) for argument in (w_qkv, bias_qv, w_out, w_up, bias_up, w_down, gains, shifts)))
    token_groups = tokens.reshape(N_DP, SEQ_DEV, L, D)
    prefix_groups = prefix_len.reshape(N_DP, SEQ_DEV).astype(jnp.int32)
    cot_groups = cotangent.reshape(N_DP, SEQ_DEV, L, D)

    def group_step(totals, inputs):
        token_group, prefix_group, cot_group = inputs

        def apply_layer(token_values, *weights):
            return forward(token_values, *weights, prefix_group)
        output, pullback = jax.vjp(apply_layer, token_group.astype(jnp.float32), *params)
        gradients = pullback(cot_group.astype(jnp.float32))
        totals = tuple((running + grad_part for running, grad_part in zip(totals, gradients[1:])))
        return (totals, (output.astype(jnp.bfloat16), gradients[0]))
    start_totals = tuple((jnp.zeros(argument.shape, jnp.float32) for argument in params))
    totals, (outputs, token_grads) = lax.scan(group_step, start_totals, (token_groups, prefix_groups, cot_groups))
    return (outputs.reshape(SEQS, L, D), token_grads.reshape(SEQS, L, D), totals[0], totals[1], totals[2], totals[3], totals[4], totals[5], totals[6], totals[7])
```

```python
from functools import partial

import jax
import jax.numpy as jnp
from jax import lax
from jax.experimental import pallas as pl
from jax.experimental.pallas import tpu as pltpu
from jax.sharding import PartitionSpec as P

DH = 64


EPSILON = 1e-05
MASKED_SCORE = -1e30


def norm_forward(values, gain_row, shift_row):
    center = values - jnp.mean(values, axis=-1, keepdims=True)
    inverse = lax.rsqrt(jnp.mean(center * center, axis=-1, keepdims=True) + EPSILON)
    normal = center * inverse
    return (normal * gain_row + shift_row, normal, inverse)


def norm_backward(incoming, normal, inverse, gain_row):
    scaled = incoming * gain_row
    first_mean = jnp.mean(scaled, axis=-1, keepdims=True)
    second_mean = jnp.mean(scaled * normal, axis=-1, keepdims=True)
    outgoing = inverse * (scaled - first_mean - normal * second_mean)
    return (outgoing, jnp.sum(incoming * normal, axis=0), jnp.sum(incoming, axis=0))


def visible_mask(offset, block_rows, length, prefix):
    row_ids = offset + jnp.arange(block_rows, dtype=jnp.int32)[:, None]
    column_ids = jnp.arange(length, dtype=jnp.int32)[None, :]
    return jnp.logical_or(column_ids < prefix, column_ids <= row_ids)


def block_scores(chosen, key_heads, offset, prefix, scaling):
    length = key_heads.shape[0]
    allowed = visible_mask(offset, chosen.shape[0], length, prefix)
    scores = (
        jnp.einsum("qhd,khd->hqk", chosen, key_heads, preferred_element_type=jnp.float32) * scaling
    )
    return jnp.where(allowed[None], scores, MASKED_SCORE)


def attention_forward(queries, key_heads, value_heads, prefix):
    length = key_heads.shape[0]
    block_rows = min(512, length)
    scaling = queries.shape[-1] ** (-0.5)
    outputs = []
    totals = []
    for offset in range(0, length, block_rows):
        scores = block_scores(
            queries[offset : offset + block_rows], key_heads, offset, prefix, scaling
        )
        row_max = jnp.max(scores, axis=-1, keepdims=True)
        log_total = jnp.log(jnp.sum(jnp.exp(scores - row_max), axis=-1, keepdims=True)) + row_max
        attn_probs = jnp.exp(scores - log_total).astype(jnp.bfloat16)
        outputs.append(
            jnp.einsum("hqk,khd->qhd", attn_probs, value_heads, preferred_element_type=jnp.float32)
        )
        totals.append(log_total)
    return (jnp.concatenate(outputs, axis=0), totals)


def attention_backward(queries, key_heads, value_heads, prefix, totals, context_grad):
    length = key_heads.shape[0]
    block_rows = min(512, length)
    scaling = queries.shape[-1] ** (-0.5)
    query_parts = []
    key_grad = jnp.zeros(key_heads.shape, jnp.float32)
    value_grad = jnp.zeros(value_heads.shape, jnp.float32)
    for number, offset in enumerate(range(0, length, block_rows)):
        chosen = queries[offset : offset + block_rows]
        grad_block = context_grad[offset : offset + block_rows]
        scores = block_scores(chosen, key_heads, offset, prefix, scaling)
        attn_probs = jnp.exp(scores - totals[number])
        probs_low = attn_probs.astype(jnp.bfloat16)
        probs_grad = jnp.einsum(
            "qhd,khd->hqk", grad_block, value_heads, preferred_element_type=jnp.float32
        )
        row_dot = jnp.sum(attn_probs * probs_grad, axis=-1, keepdims=True)
        scores_grad = (attn_probs * (probs_grad - row_dot)).astype(jnp.bfloat16)
        query_parts.append(
            jnp.einsum("hqk,khd->qhd", scores_grad, key_heads, preferred_element_type=jnp.float32)
            * scaling
        )
        key_grad = (
            key_grad
            + jnp.einsum("hqk,qhd->khd", scores_grad, chosen, preferred_element_type=jnp.float32)
            * scaling
        )
        value_grad = value_grad + jnp.einsum(
            "hqk,qhd->khd", probs_low, grad_block, preferred_element_type=jnp.float32
        )
    return (jnp.concatenate(query_parts, axis=0), key_grad, value_grad)


def local(
    tokens, prefix_len, w_qkv, bias_qv, w_out, w_up, bias_up, w_down, gains, shifts, cotangent
):
    tensor_count = lax.axis_size("tensor")
    seq_local, shard_rows, model_width = tokens.shape
    length = shard_rows * tensor_count
    full_qkv, full_bias_qv, full_out, full_up, full_bias_up, full_down = (
        lax.all_gather(w_qkv, "dp", axis=0, tiled=True),
        lax.all_gather(bias_qv, "dp", axis=1, tiled=True),
        lax.all_gather(w_out, "dp", axis=1, tiled=True),
        lax.all_gather(w_up, "dp", axis=0, tiled=True),
        lax.all_gather(bias_up, "dp", axis=0, tiled=True),
        lax.all_gather(w_down, "dp", axis=1, tiled=True),
    )
    full_gains, full_shifts = (
        lax.all_gather(gains, ("dp", "tensor"), axis=1, tiled=True),
        lax.all_gather(shifts, ("dp", "tensor"), axis=1, tiled=True),
    )
    full_gains = full_gains.astype(jnp.float32)
    full_shifts = full_shifts.astype(jnp.float32)
    bias_values = full_bias_qv.astype(jnp.float32)
    up_bias = full_bias_up.astype(jnp.float32)
    local_width = full_qkv.shape[2]
    head_count = local_width // DH
    kept_state = []
    outputs = []
    for member in range(seq_local):
        token_rows = tokens[member]
        prefix = prefix_len[member]

        def fold_tokens(piece):
            product = jnp.einsum("rd,dce->rce", piece, full_qkv, preferred_element_type=jnp.float32)
            return (piece, product)

        token_full, projected = fold_tokens(
            lax.all_gather(token_rows, "tensor", axis=0, tiled=True)
        )
        queries = (
            (projected[:, 0] + bias_values[0]).astype(jnp.bfloat16).reshape(length, head_count, DH)
        )
        key_heads = projected[:, 1].astype(jnp.bfloat16).reshape(length, head_count, DH)
        value_heads = (
            (projected[:, 2] + bias_values[1]).astype(jnp.bfloat16).reshape(length, head_count, DH)
        )
        context, totals = attention_forward(queries, key_heads, value_heads, prefix)
        context_low = context.reshape(length, local_width).astype(jnp.bfloat16)
        branch = (
            lax.psum_scatter(
                jnp.dot(context_low, full_out, preferred_element_type=jnp.float32).astype(
                    jnp.bfloat16
                ),
                "tensor",
                scatter_dimension=0,
                tiled=True,
            ).astype(jnp.float32)
            + full_shifts[0]
        )
        normed, normal_one, inverse_one = norm_forward(
            token_rows.astype(jnp.float32) + branch, full_gains[0], full_shifts[1]
        )
        normed_low = normed.astype(jnp.bfloat16)

        def fold_normed(piece):
            product = jnp.dot(piece, full_up, preferred_element_type=jnp.float32)
            return (piece, product)

        normed_full, pre_active = fold_normed(
            lax.all_gather(normed_low, "tensor", axis=0, tiled=True)
        )
        pre_active = pre_active + up_bias
        active_low = jax.nn.gelu(pre_active, approximate=False).astype(jnp.bfloat16)
        feed_out = (
            lax.psum_scatter(
                jnp.dot(active_low, full_down, preferred_element_type=jnp.float32).astype(
                    jnp.bfloat16
                ),
                "tensor",
                scatter_dimension=0,
                tiled=True,
            ).astype(jnp.float32)
            + full_shifts[2]
        )
        result, normal_two, inverse_two = norm_forward(
            normed + feed_out, full_gains[1], full_shifts[3]
        )
        outputs.append(result.astype(jnp.bfloat16))
        kept_state.append(
            (
                token_rows,
                prefix,
                token_full,
                queries,
                key_heads,
                value_heads,
                totals,
                context_low,
                normal_one,
                inverse_one,
                normed_full,
                pre_active,
                active_low,
                normal_two,
                inverse_two,
            )
        )
    back_qkv, back_out, back_up, back_down = (
        lax.all_gather(w_qkv, "dp", axis=0, tiled=True),
        lax.all_gather(w_out, "dp", axis=1, tiled=True),
        lax.all_gather(w_up, "dp", axis=0, tiled=True),
        lax.all_gather(w_down, "dp", axis=1, tiled=True),
    )
    full_shapes = (
        full_qkv.shape,
        full_bias_qv.shape,
        full_out.shape,
        full_up.shape,
        full_bias_up.shape,
        full_down.shape,
    )
    weight_grads = tuple((jnp.zeros(array_shape, jnp.float32) for array_shape in full_shapes))
    gain_grads = jnp.zeros((2, model_width), jnp.float32)
    shift_grads = jnp.zeros((4, model_width), jnp.float32)
    input_grads = []
    for member in range(seq_local):
        (
            token_rows,
            prefix,
            token_full,
            queries,
            key_heads,
            value_heads,
            totals,
            context_low,
            normal_one,
            inverse_one,
            normed_full,
            pre_active,
            active_low,
            normal_two,
            inverse_two,
        ) = kept_state[member]
        incoming = cotangent[member].astype(jnp.float32)
        residual_two, gain_two, shift_two = norm_backward(
            incoming, normal_two, inverse_two, full_gains[1]
        )
        feed_grad = residual_two.astype(jnp.bfloat16)
        fold_piece = lax.all_gather(feed_grad, "tensor", axis=0, tiled=True)
        down_grad = jnp.einsum(
            "rf,rd->fd", active_low, fold_piece, preferred_element_type=jnp.float32
        )
        fold_product = jnp.einsum(
            "rd,fd->rf", fold_piece, back_down, preferred_element_type=jnp.float32
        )
        active_grad = fold_product
        down_grad, active_grad = (down_grad, active_grad)
        layer_value, gelu_pull = jax.vjp(partial(jax.nn.gelu, approximate=False), pre_active)
        upper_grad = gelu_pull(active_grad)[0].astype(jnp.bfloat16)
        normed_grad = residual_two + lax.psum_scatter(
            jnp.einsum("rf,df->rd", upper_grad, back_up, preferred_element_type=jnp.float32).astype(
                jnp.bfloat16
            ),
            "tensor",
            scatter_dimension=0,
            tiled=True,
        ).astype(jnp.float32)
        up_grad = jnp.einsum(
            "ld,lf->df", normed_full, upper_grad, preferred_element_type=jnp.float32
        )
        up_bias_grad = jnp.sum(upper_grad.astype(jnp.float32), axis=0)
        residual_one, gain_one, shift_one = norm_backward(
            normed_grad, normal_one, inverse_one, full_gains[0]
        )
        branch_grad = residual_one.astype(jnp.bfloat16)

        def fold_branch(piece):
            out_grad = jnp.einsum(
                "rk,rd->kd", context_low, piece, preferred_element_type=jnp.float32
            )
            product = jnp.einsum("rd,kd->rk", piece, back_out, preferred_element_type=jnp.float32)
            return (out_grad, product)

        out_grad, context_grad = fold_branch(
            lax.all_gather(branch_grad, "tensor", axis=0, tiled=True)
        )
        context_grad = context_grad.astype(jnp.bfloat16).reshape(length, head_count, DH)
        query_grad, key_grad, value_grad = attention_backward(
            queries, key_heads, value_heads, prefix, totals, context_grad
        )
        mixed_grad = (
            jnp.stack([query_grad, key_grad, value_grad], axis=1)
            .astype(jnp.bfloat16)
            .reshape(length, 3, local_width)
        )
        qkv_grad = jnp.einsum(
            "ld,lce->dce", token_full, mixed_grad, preferred_element_type=jnp.float32
        )
        row_sums = jnp.sum(mixed_grad.astype(jnp.float32), axis=0)
        bias_grad = jnp.stack([row_sums[0], row_sums[2]])
        token_grad = residual_one + lax.psum_scatter(
            jnp.einsum(
                "rce,dce->rd", mixed_grad, back_qkv, preferred_element_type=jnp.float32
            ).astype(jnp.bfloat16),
            "tensor",
            scatter_dimension=0,
            tiled=True,
        ).astype(jnp.float32)
        input_grads.append(token_grad)
        gain_grads = gain_grads + jnp.stack([gain_one, gain_two])
        shift_grads = shift_grads + jnp.stack(
            [
                jnp.sum(branch_grad.astype(jnp.float32), axis=0),
                shift_one,
                jnp.sum(feed_grad.astype(jnp.float32), axis=0),
                shift_two,
            ]
        )
        member_grads = (qkv_grad, bias_grad, out_grad, up_grad, up_bias_grad, down_grad)
        weight_grads = tuple(
            (running + grad_part for running, grad_part in zip(weight_grads, member_grads))
        )
    total_qkv, total_bias, total_out, total_up, total_up_bias, total_down = weight_grads
    weight_grads = (
        lax.psum_scatter(total_qkv, "dp", scatter_dimension=0, tiled=True),
        lax.psum_scatter(total_bias, "dp", scatter_dimension=1, tiled=True),
        lax.psum_scatter(total_out, "dp", scatter_dimension=1, tiled=True),
        lax.psum_scatter(total_up, "dp", scatter_dimension=0, tiled=True),
        lax.psum_scatter(total_up_bias, "dp", scatter_dimension=0, tiled=True),
        lax.psum_scatter(total_down, "dp", scatter_dimension=1, tiled=True),
    )
    gain_share, shift_share = (
        lax.psum_scatter(gain_grads, ("dp", "tensor"), scatter_dimension=1, tiled=True),
        lax.psum_scatter(shift_grads, ("dp", "tensor"), scatter_dimension=1, tiled=True),
    )
    return (
        jnp.stack(outputs),
        jnp.stack(input_grads),
        weight_grads[0],
        weight_grads[1],
        weight_grads[2],
        weight_grads[3],
        weight_grads[4],
        weight_grads[5],
        gain_share,
        shift_share,
    )


MESH_ID = pl.DeviceIdType.MESH
BF = jnp.bfloat16
F32 = jnp.float32
ROWS = 96
SMALL = 16


def place():
    d = lax.axis_index("dp")
    t = lax.axis_index("tensor")
    k, c = d // 2, d % 2
    xb, yb = k % 2, k // 2
    dx = d + 2 - 4 * xb
    dy = d + 4 - 8 * yb
    return d, t, k, c, xb, yb, dx, dy


def remote(src, dst, send, recv, dp, tensor):
    return pltpu.make_async_remote_copy(
        src_ref=src,
        dst_ref=dst,
        send_sem=send,
        recv_sem=recv,
        device_id=(dp, tensor),
        device_id_type=MESH_ID,
    )


def enter(k, c, t, d, dx, dy):
    barrier = pltpu.get_barrier_semaphore()

    def greet(dp, tensor):
        pl.semaphore_signal(barrier, inc=1, device_id=(dp, tensor), device_id_type=MESH_ID)

    greet(dx, t)
    greet(dy, t)
    greet(d + 1 - 2 * c, t)
    for step in range(1, 4):
        other = (t + step) % 4
        greet(2 * k, other)
        greet(2 * k + 1, other)
    pl.semaphore_wait(barrier, 9)


def pair_swap(part):
    def kernel(src, dst, send, recv):
        d, t, k, c, xb, yb, dx, dy = place()
        mate = d + 1 - 2 * c
        barrier = pltpu.get_barrier_semaphore()
        pl.semaphore_signal(barrier, inc=1, device_id=(mate, t), device_id_type=MESH_ID)
        pl.semaphore_wait(barrier, 1)
        rows = src.shape[0] // 4
        copies = [
            remote(
                src.at[pl.ds(i * rows, rows)],
                dst.at[pl.ds(i * rows, rows)],
                send.at[i],
                recv.at[i],
                mate,
                t,
            )
            for i in range(4)
        ]
        for copy in copies:
            copy.start()
        for copy in copies:
            copy.wait()

    return pl.pallas_call(
        kernel,
        out_shape=jax.ShapeDtypeStruct(part.shape, part.dtype),
        in_specs=[pl.BlockSpec(memory_space=pl.ANY)],
        out_specs=pl.BlockSpec(memory_space=pl.ANY),
        scratch_shapes=[pltpu.SemaphoreType.DMA((4,)), pltpu.SemaphoreType.DMA((4,))],
        compiler_params=pltpu.CompilerParams(collective_id=3, has_side_effects=True),
    )(part)


def skewed(chunks, levels):
    for slot in range(chunks + len(levels) - 1):
        for level in reversed(range(len(levels))):
            if 0 <= slot - level < chunks:
                levels[level](slot - level)


def gather_all(tokens, cotangent, shards, chunks):
    half = tokens.shape[1] // 2
    width = tokens.shape[2]
    count = len(shards)
    n_chunks = len(chunks)
    rows_of = [s.shape[0] for s in shards]

    def kernel(*refs):
        tok, cot = refs[0], refs[1]
        own = refs[2 : 2 + count]
        base = 2 + count
        xf, cf = refs[base], refs[base + 1]
        full = refs[base + 2 : base + 2 + count]
        small_other = refs[base + 2 + count]
        (
            stage,
            row_stage,
            local_sem,
            row_sem,
            ex_send,
            ex_recv,
            fw_send,
            fw_recv,
            p_send,
            p_recv,
            z_send,
            z_recv,
            a_send,
            a_recv,
            b_send,
            b_recv,
            o_send,
            o_recv,
        ) = (
            refs[base + 3 + count : base + 3 + 2 * count],
            *refs[base + 3 + 2 * count :],
        )
        d, t, k, c, xb, yb, dx, dy = place()
        mate = d + 1 - 2 * c
        u = t + c * (3 - 2 * t)
        up = t + 1 - 2 * c
        down = t - 1 + 2 * c
        source = t // 2 == c
        enter(k, c, t, d, dx, dy)

        for s in range(count):
            rows = rows_of[s]
            spot = full[s].at[t % 2, pl.ds(d * rows, rows)]

            @pl.when(source)
            def _():
                pltpu.make_async_copy(own[s], stage[s], local_sem.at[s]).start()

            @pl.when(jnp.logical_not(source))
            def _():
                remote(own[s], spot, p_send.at[s], p_recv.at[s], mate, t).start()

        def exchange(which, src, dst):
            for m in range(2):
                goal = 2 * c + m
                for core in range(2):
                    piece = src.at[m, pl.ds(core * half, half)]
                    spot = dst.at[t * 2 + core]
                    here = jnp.logical_and(goal == t, core == c)

                    @pl.when(here)
                    def _():
                        load = pltpu.make_async_copy(piece, row_stage, row_sem)
                        load.start()
                        load.wait()
                        store = pltpu.make_async_copy(row_stage, spot, row_sem)
                        store.start()
                        store.wait()

                    @pl.when(jnp.logical_not(here))
                    def _():
                        remote(
                            piece,
                            spot,
                            ex_send.at[which, 2 * m + core],
                            ex_recv.at[which, t],
                            2 * k + core,
                            goal,
                        ).start()

        def relay(which, dst):
            for origin in range(4):
                spot = dst.at[origin * 2 + c]
                local = jnp.logical_and(origin == t, c == t // 2)

                @pl.when(jnp.logical_not(local))
                def _():
                    remote(
                        spot, spot, ex_send.at[which, 0], ex_recv.at[which, origin], mate, t
                    ).wait_recv()

                remote(
                    spot, spot, fw_send.at[which, origin], fw_recv.at[which, origin], mate, t
                ).start()

        def settle(which, src, dst):
            for origin in range(4):
                spot = dst.at[origin * 2 + 1 - c]
                remote(
                    spot, spot, fw_send.at[which, origin], fw_recv.at[which, origin], mate, t
                ).wait()
            for m in range(2):
                for core in range(2):
                    here = jnp.logical_and(2 * c + m == t, core == c)

                    @pl.when(jnp.logical_not(here))
                    def _():
                        remote(
                            src.at[m, pl.ds(core * half, half)],
                            dst.at[t * 2 + core],
                            ex_send.at[which, 2 * m + core],
                            ex_recv.at[which, t],
                            mate,
                            t,
                        ).wait_send()

        exchange(0, tok, xf)

        for s in range(count):

            @pl.when(source)
            def _():
                rows = rows_of[s]
                spot = full[s].at[t % 2, pl.ds(d * rows, rows)]
                pltpu.make_async_copy(own[s], stage[s], local_sem.at[s]).wait()
                pltpu.make_async_copy(stage[s], spot, local_sem.at[s]).start()

        exchange(1, cot, cf)

        def block(i, b, start, n):
            s, col, cols = chunks[i]
            zz = b + c * (1 - 2 * b)
            rows = rows_of[s]
            return full[s].at[zz, pl.ds(start * rows, n * rows), pl.ds(col, cols)]

        def z_copy(i, b, way, target):
            ref = block(i, b, 2 * k, 2)
            return remote(ref, ref, z_send.at[i, b, way], z_recv.at[i, b], d, target)

        def first_copy(i, b):
            ref = block(i, b, 2 * k, 2)
            return remote(ref, ref, a_send.at[i, b], a_recv.at[i, b], dx if b == 0 else dy, t)

        def first_arrival(i, b):
            near = k + 1 - 2 * xb if b == 0 else k + 2 - 4 * yb
            ref = block(i, b, 2 * near, 2)
            return remote(ref, ref, a_send.at[i, b], a_recv.at[i, b], dx if b == 0 else dy, t)

        def second_copies(i, arriving):
            other = 1 if arriving else 0
            row = yb + other * (1 - 2 * yb)
            ref = block(i, 0, 4 * row, 4)
            col = xb + other * (1 - 2 * xb)
            out = [remote(ref, ref, b_send.at[i, 0], b_recv.at[i, 0], dy, t)]
            for r in range(2):
                ref = block(i, 1, 2 * (2 * r + col), 2)
                out.append(remote(ref, ref, b_send.at[i, 1 + r], b_recv.at[i, 1 + r], dx, t))
            return out

        def spread(i, b):
            @pl.when(jnp.logical_and(u >= b, u < 3))
            def _():
                z_copy(i, b, 0, up).start()

            if b == 1:

                @pl.when(u == 1)
                def _():
                    z_copy(i, 1, 1, down).start()

            first_copy(i, b).start()

        waited = set()

        def own_ready(i):
            s = chunks[i][0]
            if s in waited:
                return
            waited.add(s)
            rows = rows_of[s]
            spot = full[s].at[t % 2, pl.ds(d * rows, rows)]
            twin = full[s].at[t % 2, pl.ds(mate * rows, rows)]
            pltpu.make_async_copy(stage[s], spot, local_sem.at[s]).wait()
            remote(twin, twin, p_send.at[s], p_recv.at[s], mate, t).wait_recv()

        def level_own(i):
            if chunks[i][0] not in waited:

                @pl.when(source)
                def _():
                    own_ready(i)

            for b in range(2):

                @pl.when(u == b)
                def _():
                    spread(i, b)

        def level_line(i):
            for b in (1, 0):

                @pl.when(u != b)
                def _():
                    z_copy(i, b, 0, up).wait_recv()
                    spread(i, b)

        def level_second(i):
            for b in range(2):
                first_arrival(i, b).wait_recv()
            for copy in second_copies(i, False):
                copy.start()

        def level_done(i):
            for copy in second_copies(i, True):
                copy.wait_recv()

        level_own(0)
        relay(0, xf)
        skewed(
            n_chunks,
            [(lambda i: None if i == 0 else level_own(i)), level_line, level_second, level_done],
        )
        relay(1, cf)
        last = count - 1
        swap = remote(full[last], small_other, o_send, o_recv, mate, t)
        swap.start()
        settle(0, tok, xf)
        settle(1, cot, cf)
        for s in range(count):
            rows = rows_of[s]
            spot = full[s].at[t % 2, pl.ds(d * rows, rows)]

            @pl.when(jnp.logical_not(source))
            def _():
                remote(own[s], spot, p_send.at[s], p_recv.at[s], mate, t).wait_send()

        for i in range(n_chunks):
            for b in range(2):

                @pl.when(jnp.logical_and(u >= b, u < 3))
                def _():
                    z_copy(i, b, 0, up).wait_send()

                first_copy(i, b).wait_send()

            @pl.when(u == 1)
            def _():
                z_copy(i, 1, 1, down).wait_send()

            for copy in second_copies(i, False):
                copy.wait_send()
        swap.wait()

    any_spec = pl.BlockSpec(memory_space=pl.ANY)
    dma = pltpu.SemaphoreType.DMA
    full_shapes = [jax.ShapeDtypeStruct((2, 8 * s.shape[0], s.shape[1]), s.dtype) for s in shards]
    length = tokens.shape[1] * 4
    rows_shape = jax.ShapeDtypeStruct((8, half, width), tokens.dtype)
    outs = pl.pallas_call(
        kernel,
        out_shape=[rows_shape, rows_shape, *full_shapes, full_shapes[-1]],
        in_specs=[any_spec] * (2 + count),
        out_specs=[any_spec] * (3 + count),
        scratch_shapes=[
            *[pltpu.VMEM(s.shape, s.dtype) for s in shards],
            pltpu.VMEM((half, width), tokens.dtype),
            dma((count,)),
            dma,
            dma((2, 4)),
            dma((2, 4)),
            dma((2, 4)),
            dma((2, 4)),
            dma((count,)),
            dma((count,)),
            dma((n_chunks, 2, 2)),
            dma((n_chunks, 2)),
            dma((n_chunks, 2)),
            dma((n_chunks, 2)),
            dma((n_chunks, 3)),
            dma((n_chunks, 3)),
            dma,
            dma,
        ],
        compiler_params=pltpu.CompilerParams(collective_id=1, has_side_effects=True),
    )(tokens, cotangent, *shards)
    return (
        outs[0].reshape(length, width),
        outs[1].reshape(length, width),
        outs[2 : 2 + count],
        outs[2 + count],
    )


def reduce_all(output, token_grad, grads, chunks):
    count = len(grads)
    n_chunks = len(chunks)
    length, width = output.shape
    half = length // 8
    rows_of = [g.shape[1] // 8 for g in grads]

    def kernel(*refs):
        res, tgr = refs[0], refs[1]
        part = refs[2 : 2 + count]
        base = 2 + count
        res_out, tgr_out = refs[base], refs[base + 1]
        final = refs[base + 2 : base + 2 + count]
        base += 2 + count
        got1 = refs[base : base + count]
        sum1 = refs[base + count : base + 2 * count]
        got2 = refs[base + 2 * count : base + 3 * count]
        sum2 = refs[base + 3 * count : base + 4 * count]
        got3 = refs[base + 4 * count : base + 5 * count]
        sum3 = refs[base + 5 * count : base + 6 * count]
        got4 = refs[base + 6 * count : base + 7 * count]
        got5 = refs[base + 7 * count : base + 8 * count]
        (
            row_stage,
            row_sem,
            ex_send,
            ex_recv,
            a_send,
            a_recv,
            b_send,
            b_recv,
            z_send,
            z_recv,
            y_send,
            y_recv,
            p_send,
            p_recv,
        ) = refs[base + 8 * count :]
        d, t, k, c, xb, yb, dx, dy = place()
        mate = d + 1 - 2 * c
        u = t + c * (3 - 2 * t)
        up = t + 1 - 2 * c
        down = t - 1 + 2 * c
        source = u <= 1
        enter(k, c, t, d, dx, dy)

        def return_rows(which, src, dst, start):
            for goal in range(4):
                piece = src.at[pl.ds((goal * 2 + c) * half, half)]
                spot = dst.at[t % 2, pl.ds(c * half, half)]
                here = jnp.logical_and(goal == t, c == t // 2)
                copy = remote(
                    piece,
                    spot,
                    ex_send.at[which, goal],
                    ex_recv.at[which, t % 2, c],
                    2 * k + t // 2,
                    goal,
                )

                @pl.when(here)
                def _():
                    if start:
                        load = pltpu.make_async_copy(piece, row_stage, row_sem)
                        load.start()
                        load.wait()
                        store = pltpu.make_async_copy(row_stage, spot, row_sem)
                        store.start()
                        store.wait()

                @pl.when(jnp.logical_not(here))
                def _():
                    if start:
                        copy.start()
                    else:
                        copy.wait_send()

            if not start:
                for m in range(2):
                    for core in range(2):
                        spot = dst.at[m, pl.ds(core * half, half)]
                        here = jnp.logical_and(2 * c + m == t, core == c)

                        @pl.when(jnp.logical_not(here))
                        def _():
                            remote(
                                spot,
                                spot,
                                ex_send.at[which, 0],
                                ex_recv.at[which, m, core],
                                mate,
                                t,
                            ).wait_recv()

        def plane(b):
            return b + c * (1 - 2 * b)

        def first_copies(i):
            s, col, cols = chunks[i]
            rows = rows_of[s]
            spot = pl.ds(col, cols)
            out = [
                remote(
                    part[s].at[plane(0), pl.ds((1 - yb) * 4 * rows, 4 * rows), spot],
                    got1[s].at[0, :, spot],
                    a_send.at[i, 0],
                    a_recv.at[i, 0],
                    dy,
                    t,
                )
            ]
            for r in range(2):
                out.append(
                    remote(
                        part[s].at[plane(1), pl.ds((2 * r + 1 - xb) * 2 * rows, 2 * rows), spot],
                        got1[s].at[1, pl.ds(r * 2 * rows, 2 * rows), spot],
                        a_send.at[i, 1 + r],
                        a_recv.at[i, 1 + r],
                        dx,
                        t,
                    )
                )
            return out

        def second_copies(i):
            s, col, cols = chunks[i]
            rows = rows_of[s]
            spot = pl.ds(col, cols)
            out = []
            for b, far, goal in ((0, 1 - xb, dx), (1, 1 - yb, dy)):
                out.append(
                    remote(
                        sum1[s].at[b, pl.ds(far * 2 * rows, 2 * rows), spot],
                        got2[s].at[b, :, spot],
                        b_send.at[i, b],
                        b_recv.at[i, b],
                        goal,
                        t,
                    )
                )
            return out

        def low(v, s):
            return v.astype(sum1[s].dtype)

        def level_first(i):
            for copy in first_copies(i):
                copy.start()

        def level_second(i):
            s, col, cols = chunks[i]
            rows = rows_of[s]
            spot = pl.ds(col, cols)
            for copy in first_copies(i):
                copy.wait_recv()
            mine = part[s][plane(0), pl.ds(yb * 4 * rows, 4 * rows), spot]
            sum1[s][0, :, spot] = low(mine.astype(F32) + got1[s][0, :, spot].astype(F32), s)
            for r in range(2):
                mine = part[s][plane(1), pl.ds((2 * r + xb) * 2 * rows, 2 * rows), spot]
                there = pl.ds(r * 2 * rows, 2 * rows)
                sum1[s][1, there, spot] = low(
                    mine.astype(F32) + got1[s][1, there, spot].astype(F32), s
                )
            for copy in second_copies(i):
                copy.start()

        def z_copy(i, b):
            s, col, cols = chunks[i]
            spot = pl.ds(col, cols)
            return remote(
                sum3[s].at[b, :, spot],
                got3[s].at[b, :, spot],
                z_send.at[i, b],
                z_recv.at[i, b],
                d,
                down,
            )

        def y_copy(i):
            s, col, cols = chunks[i]
            spot = pl.ds(col, cols)
            return remote(
                sum3[s].at[1, :, spot], got4[s].at[:, spot], y_send.at[i], y_recv.at[i], d, up
            )

        def level_line(i):
            s, col, cols = chunks[i]
            rows = rows_of[s]
            spot = pl.ds(col, cols)
            for copy in second_copies(i):
                copy.wait_recv()
            for b, near in ((0, xb), (1, yb)):
                mine = sum1[s][b, pl.ds(near * 2 * rows, 2 * rows), spot]
                sum2[s][b, :, spot] = mine.astype(F32) + got2[s][b, :, spot].astype(F32)

            @pl.when(u == 3)
            def _():
                for b in range(2):
                    sum3[s][b, :, spot] = low(sum2[s][b, :, spot], s)
                    z_copy(i, b).start()

            @pl.when(u == 0)
            def _():
                sum3[s][1, :, spot] = low(sum2[s][1, :, spot], s)
                y_copy(i).start()

        def level_pass(i):
            s, col, cols = chunks[i]
            spot = pl.ds(col, cols)

            @pl.when(u == 2)
            def _():
                for b in range(2):
                    z_copy(i, b).wait_recv()
                    sum3[s][b, :, spot] = low(
                        sum2[s][b, :, spot] + got3[s][b, :, spot].astype(F32), s
                    )
                    z_copy(i, b).start()

        def level_near(i):
            s, col, cols = chunks[i]
            spot = pl.ds(col, cols)

            @pl.when(u == 1)
            def _():
                z_copy(i, 0).wait_recv()
                sum3[s][0, :, spot] = low(
                    sum2[s][0, :, spot] + got3[s][0, :, spot].astype(F32), s
                )
                z_copy(i, 0).start()
                z_copy(i, 1).wait_recv()
                y_copy(i).wait_recv()
                total = (
                    sum2[s][1, :, spot]
                    + got3[s][1, :, spot].astype(F32)
                    + got4[s][:, spot].astype(F32)
                )
                finish(i, total)

            @pl.when(u == 0)
            def _():
                z_copy(i, 0).wait_recv()
                finish(i, sum2[s][0, :, spot] + got3[s][0, :, spot].astype(F32))

        def p_copy(i):
            s, col, cols = chunks[i]
            rows = rows_of[s]
            spot = pl.ds(col, cols)
            return remote(
                sum1[s].at[0, pl.ds((1 - c) * rows, rows), spot],
                got5[s].at[:, spot],
                p_send.at[i],
                p_recv.at[i],
                mate,
                t,
            )

        def finish(i, total):
            s, col, cols = chunks[i]
            rows = rows_of[s]
            spot = pl.ds(col, cols)
            for copy in second_copies(i):
                copy.wait_send()
            sum2[s][0, :, spot] = total
            sum1[s][0, pl.ds(0, 2 * rows), spot] = low(total, s)
            p_copy(i).start()
            final[s][:, spot] = sum2[s][0, pl.ds(c * rows, rows), spot]

        def level_mate(i):
            s, col, cols = chunks[i]
            spot = pl.ds(col, cols)

            @pl.when(u >= 2)
            def _():
                p_copy(i).wait_recv()
                final[s][:, spot] = got5[s][:, spot].astype(F32)

        return_rows(0, res, res_out, True)
        return_rows(1, tgr, tgr_out, True)
        skewed(
            n_chunks, [level_first, level_second, level_line, level_pass, level_near, level_mate]
        )
        return_rows(0, res, res_out, False)
        return_rows(1, tgr, tgr_out, False)
        for i in range(n_chunks):
            for copy in first_copies(i):
                copy.wait_send()

            @pl.when(u >= 2)
            def _():
                for copy in second_copies(i):
                    copy.wait_send()
                for b in range(2):
                    z_copy(i, b).wait_send()

            @pl.when(u == 1)
            def _():
                z_copy(i, 0).wait_send()

            @pl.when(u == 0)
            def _():
                y_copy(i).wait_send()

            @pl.when(u <= 1)
            def _():
                p_copy(i).wait_send()

    any_spec = pl.BlockSpec(memory_space=pl.ANY)
    vmem = pl.BlockSpec(memory_space=pltpu.VMEM)
    dma = pltpu.SemaphoreType.DMA
    scratch = []
    for kind in range(8):
        for s in range(count):
            rows, cols, kept = rows_of[s], grads[s].shape[2], grads[s].dtype
            shape, dtype = (
                ((2, 4 * rows, cols), kept),
                ((2, 4 * rows, cols), kept),
                ((2, 2 * rows, cols), kept),
                ((2, 2 * rows, cols), F32),
                ((2, 2 * rows, cols), kept),
                ((2, 2 * rows, cols), kept),
                ((2 * rows, cols), kept),
                ((rows, cols), kept),
            )[kind]
            scratch.append(pltpu.VMEM(shape, dtype))
    back = jax.ShapeDtypeStruct((2, 2 * half, width), output.dtype)
    outs = pl.pallas_call(
        kernel,
        out_shape=[
            back,
            back,
            *[jax.ShapeDtypeStruct((r, g.shape[2]), F32) for r, g in zip(rows_of, grads)],
        ],
        in_specs=[any_spec, any_spec] + [vmem] * count,
        out_specs=[any_spec, any_spec] + [vmem] * count,
        scratch_shapes=[
            *scratch,
            pltpu.VMEM((half, width), output.dtype),
            dma,
            dma((2, 4)),
            dma((2, 2, 2)),
            dma((n_chunks, 3)),
            dma((n_chunks, 3)),
            dma((n_chunks, 2)),
            dma((n_chunks, 2)),
            dma((n_chunks, 2)),
            dma((n_chunks, 2)),
            dma((n_chunks,)),
            dma((n_chunks,)),
            dma((n_chunks,)),
            dma((n_chunks,)),
        ],
        compiler_params=pltpu.CompilerParams(
            collective_id=2, has_side_effects=True, vmem_limit_bytes=60 * 1024 * 1024
        ),
    )(output, token_grad, *grads)
    return outs[0], outs[1], outs[2:]


BLOCK = 256


def lane_half(shape, h):
    lane = lax.broadcasted_iota(jnp.int32, shape, 1)
    return lane < DH if h == 0 else lane >= DH


def reach(row_block, blocks):
    return max(row_block + 1, blocks // 2)


def dot_nt(a, b):
    return lax.dot_general(a, b, (((1,), (1,)), ((), ())), preferred_element_type=F32)


def dot_tn(a, b):
    return lax.dot_general(a, b, (((0,), (0,)), ((), ())), preferred_element_type=F32)


def attend(queries, keys, values, prefix):
    length, width = queries.shape
    blocks = length // BLOCK
    pairs = width // 128

    def kernel(prefix_ref, q_ref, k_ref, v_ref, o_ref, lt_ref):
        limit = prefix_ref[0]
        for qb in range(blocks):
            rows = pl.ds(qb * BLOCK, BLOCK)
            span = reach(qb, blocks) * BLOCK
            q = q_ref[rows, :] * jnp.asarray(DH**-0.5, BF)
            heads = []
            for h in range(2):
                half = lane_half((BLOCK, 128), h)
                s = dot_nt(jnp.where(half, q, jnp.zeros_like(q)), k_ref[pl.ds(0, span), :])
                clear = qb * BLOCK
                row = lax.broadcasted_iota(jnp.int32, (BLOCK, span - clear), 0) + clear
                col = lax.broadcasted_iota(jnp.int32, (BLOCK, span - clear), 1) + clear
                seen = col <= row
                if clear < length // 2:
                    seen = jnp.logical_or(seen, col < limit)
                tail = jnp.where(seen, s[:, clear:], MASKED_SCORE)
                s = jnp.concatenate([s[:, :clear], tail], axis=1) if clear else tail
                top = jnp.max(s, axis=1, keepdims=True)
                p = jnp.exp(s - top)
                total = jnp.sum(p, axis=1, keepdims=True)
                log_total = top + jnp.log(total)
                lt_ref[h, 0:1, rows] = jnp.transpose(
                    jnp.broadcast_to(log_total, (BLOCK, 128))
                )[0:1, :]
                p = (p * (1.0 / total)).astype(BF)
                heads.append(
                    jnp.dot(p, v_ref[pl.ds(0, span), :], preferred_element_type=F32)
                )
            o_ref[rows, :] = jnp.where(lane_half((BLOCK, 128), 0), heads[0], heads[1]).astype(BF)

    pair = pl.BlockSpec((length, 128), lambda i: (0, i))
    return pl.pallas_call(
        kernel,
        grid=(pairs,),
        out_shape=[
            jax.ShapeDtypeStruct((length, width), BF),
            jax.ShapeDtypeStruct((2 * pairs, 8, length), F32),
        ],
        in_specs=[pl.BlockSpec(memory_space=pltpu.SMEM), pair, pair, pair],
        out_specs=[pair, pl.BlockSpec((2, 8, length), lambda i: (i, 0, 0))],
    )(prefix, queries, keys, values)


def attend_back(queries, keys, values, prefix, totals, context, context_grad):
    length, width = queries.shape
    blocks = length // BLOCK
    pairs = width // 128

    def kernel(prefix_ref, q_ref, k_ref, v_ref, lt_ref, o_ref, do_ref, dq_ref, dk_ref, dv_ref, acc):
        limit = prefix_ref[0]
        scaling = jnp.asarray(DH**-0.5, BF)
        head_row = lax.broadcasted_iota(jnp.int32, (8, 128), 0)
        lane = lax.broadcasted_iota(jnp.int32, (8, 128), 1)
        pick = (lane // DH == head_row).astype(F32)
        row_dots = []
        for qb in range(blocks):
            rows = pl.ds(qb * BLOCK, BLOCK)
            both = do_ref[rows, :].astype(F32) * o_ref[rows, :].astype(F32)
            row_dots.append(
                lax.dot_general(
                    pick,
                    both,
                    (((1,), (1,)), ((), ())),
                    precision=lax.Precision.HIGHEST,
                    preferred_element_type=F32,
                )
            )
        acc[...] = jnp.zeros_like(acc)
        for kb in range(blocks):
            keys_at = pl.ds(kb * BLOCK, BLOCK)
            key = k_ref[keys_at, :]
            value = v_ref[keys_at, :]
            dk = jnp.zeros((BLOCK, 128), F32)
            dv = jnp.zeros((BLOCK, 128), F32)
            for qb in range(blocks):
                if kb >= reach(qb, blocks):
                    continue
                rows = pl.ds(qb * BLOCK, BLOCK)
                q_pair = q_ref[rows, :] * scaling
                do_pair = do_ref[rows, :]
                for h in range(2):
                    half = lane_half((BLOCK, 128), h)
                    zero = jnp.zeros((BLOCK, 128), BF)
                    q = jnp.where(half, q_pair, zero)
                    do = jnp.where(half, do_pair, zero)
                    s = dot_nt(key, q)
                    if kb >= qb:
                        key_id = lax.broadcasted_iota(jnp.int32, (BLOCK, BLOCK), 0) + kb * BLOCK
                        row_id = lax.broadcasted_iota(jnp.int32, (BLOCK, BLOCK), 1) + qb * BLOCK
                        seen = key_id <= row_id
                        if kb * BLOCK < length // 2:
                            seen = jnp.logical_or(seen, key_id < limit)
                        s = jnp.where(seen, s, MASKED_SCORE)
                    p = jnp.exp(s - lt_ref[h, 0:1, rows])
                    dp = dot_nt(value, do)
                    ds = (p * (dp - row_dots[qb][h : h + 1, :])).astype(BF)
                    dv = dv + jnp.dot(p.astype(BF), do, preferred_element_type=F32)
                    dk = dk + jnp.dot(ds, q, preferred_element_type=F32)
                    acc[rows, :] += dot_tn(ds, jnp.where(half, key, zero))
            dk_ref[keys_at, :] = dk.astype(BF)
            dv_ref[keys_at, :] = dv.astype(BF)
        dq_ref[...] = (acc[...] * DH**-0.5).astype(BF)

    pair = pl.BlockSpec((length, 128), lambda i: (0, i))
    shape = jax.ShapeDtypeStruct((length, width), BF)
    return pl.pallas_call(
        kernel,
        grid=(pairs,),
        out_shape=[shape] * 3,
        in_specs=[
            pl.BlockSpec(memory_space=pltpu.SMEM),
            pair,
            pair,
            pair,
            pl.BlockSpec((2, 8, length), lambda i: (i, 0, 0)),
            pair,
            pair,
        ],
        out_specs=[pair] * 3,
        scratch_shapes=[pltpu.VMEM((length, 128), F32)],
    )(prefix, queries, keys, values, totals, context, context_grad)


def chip_local(
    tokens, prefix_len, w_qkv, bias_qv, w_out, w_up, bias_up, w_down, gains, shifts, cotangent
):
    d, t, k, c, _, _, _, _ = place()
    model_width = tokens.shape[2]
    length = tokens.shape[1] * 4
    part = w_qkv.shape[2]
    hidden = w_up.shape[1]

    def lanes(v):
        return jnp.pad(v, ((0, 0), (0, 128 - v.shape[1])))

    limits = jnp.concatenate([prefix_len // 16, prefix_len % 16]).astype(BF)[None]
    small = jnp.concatenate(
        [lanes(v) for v in (bias_qv, bias_up[None], gains, shifts, limits)], axis=0
    )
    small = jnp.pad(small, ((0, SMALL - small.shape[0]), (0, 0)))
    shards = (
        w_qkv.reshape(ROWS, 3 * part),
        w_out.T,
        w_up,
        w_down.T,
        small,
    )
    half = hidden // 2
    chunks = (
        (4, 0, 128),
        (0, 0, 3 * part),
        (1, 0, part),
        (2, 0, half),
        (2, half, half),
        (3, 0, half),
        (3, half, half),
    )
    x, cot, (g_qkv, g_out, g_up, g_down, g_small), small_other = gather_all(
        tokens, cotangent, shards, chunks
    )

    mine = g_small.reshape(2, 8, SMALL, 128)
    theirs = small_other.reshape(2, 8, SMALL, 128)
    first = jnp.where(c == 0, mine, theirs)
    every = jnp.concatenate([first, jnp.where(c == 0, theirs, mine)], axis=0)
    per = bias_qv.shape[1]
    bias_values = mine[:, :, 0:2, :per].astype(F32)
    bias_values = bias_values.transpose(2, 0, 1, 3).reshape(2, 2 * part)
    up_bias = mine[:, :, 2, : bias_up.shape[0]].astype(F32).reshape(2, hidden)
    rows = every[:, :, 3:9, :per].astype(F32).transpose(2, 1, 0, 3).reshape(6, model_width)
    full_gains, full_shifts = rows[:2], rows[2:]
    source = lax.dynamic_index_in_dim(every[0, :, 9, :4].astype(F32), 2 * k + t // 2, 0, False)
    member = t % 2
    high = jnp.where(member == 0, source[0], source[1])
    low_part = jnp.where(member == 0, source[2], source[3])
    prefix = (high * 16 + low_part).astype(jnp.int32)[None]

    def kind(i):
        return jnp.concatenate(
            [g_qkv[z, :, i * part : (i + 1) * part] for z in range(2)], axis=1
        )

    def project(i):
        return jnp.dot(x, kind(i), preferred_element_type=F32)

    queries = (project(0) + bias_values[0]).astype(BF)
    key_heads = project(1).astype(BF)
    value_heads = (project(2) + bias_values[1]).astype(BF)
    context, totals = attend(queries, key_heads, value_heads, prefix)
    branch_part = sum(
        jnp.einsum(
            "rk,dk->rd", context[:, z * part : (z + 1) * part], g_out[z], preferred_element_type=F32
        )
        for z in range(2)
    ).astype(BF)
    branch = (
        branch_part.astype(F32) + pair_swap(branch_part).astype(F32) + full_shifts[0]
    )
    normed, normal_one, inverse_one = norm_forward(
        x.astype(F32) + branch, full_gains[0], full_shifts[1]
    )
    normed_low = normed.astype(BF)
    pre = [
        jnp.dot(normed_low, g_up[z], preferred_element_type=F32) + up_bias[z] for z in range(2)
    ]
    active = [jax.nn.gelu(v, approximate=False).astype(BF) for v in pre]
    feed_part = sum(
        jnp.einsum("rf,df->rd", active[z], g_down[z], preferred_element_type=F32)
        for z in range(2)
    ).astype(BF)
    feed_out = feed_part.astype(F32) + pair_swap(feed_part).astype(F32) + full_shifts[2]
    result, normal_two, inverse_two = norm_forward(
        normed + feed_out, full_gains[1], full_shifts[3]
    )
    incoming = cot.astype(F32)
    residual_two, gain_two, shift_two = norm_backward(
        incoming, normal_two, inverse_two, full_gains[1]
    )
    feed_grad = residual_two.astype(BF)
    upper = []
    for z in range(2):
        active_grad = jnp.dot(feed_grad, g_down[z], preferred_element_type=F32)
        _, pull = jax.vjp(partial(jax.nn.gelu, approximate=False), pre[z])
        upper.append(pull(active_grad)[0].astype(BF))
    normed_part = sum(
        jnp.einsum("rf,df->rd", upper[z], g_up[z], preferred_element_type=F32) for z in range(2)
    ).astype(BF)
    normed_grad = residual_two + (
        normed_part.astype(F32) + pair_swap(normed_part).astype(F32)
    )
    residual_one, gain_one, shift_one = norm_backward(
        normed_grad, normal_one, inverse_one, full_gains[0]
    )
    branch_grad = residual_one.astype(BF)
    context_grad = jnp.concatenate(
        [jnp.dot(branch_grad, g_out[z], preferred_element_type=F32) for z in range(2)], axis=1
    ).astype(BF)
    mixed = attend_back(queries, key_heads, value_heads, prefix, totals, context, context_grad)
    mixed_low = [
        jnp.concatenate([m[:, z * part : (z + 1) * part] for m in mixed], axis=1)
        for z in range(2)
    ]
    token_part = sum(
        jnp.einsum("re,de->rd", mixed_low[z], g_qkv[z], preferred_element_type=F32)
        for z in range(2)
    ).astype(BF)
    token_grad = residual_one + (token_part.astype(F32) + pair_swap(token_part).astype(F32))

    def outer(a, b):
        return jnp.einsum("rm,rn->mn", a, b, preferred_element_type=F32).astype(BF)

    grads = (
        jnp.stack([outer(x, mixed_low[z]) for z in range(2)]),
        jnp.stack(
            [outer(branch_grad, context[:, z * part : (z + 1) * part]) for z in range(2)]
        ),
        jnp.stack([outer(normed_low, upper[z]) for z in range(2)]),
        jnp.stack([outer(feed_grad, active[z]) for z in range(2)]),
    )
    up_bias_grad = jnp.stack([jnp.sum(v.astype(F32), axis=0) for v in upper])
    bias_grad = jnp.stack(
        [jnp.sum(m.astype(F32), axis=0) for m in (mixed[0], mixed[2])]
    )
    row_grads = jnp.stack(
        [
            gain_one,
            gain_two,
            jnp.sum(branch_grad.astype(F32), axis=0),
            shift_one,
            jnp.sum(feed_grad.astype(F32), axis=0),
            shift_two,
        ]
    )
    spread_bias = bias_grad.reshape(2, 2, 8, per).transpose(1, 2, 0, 3)
    spread_rows = row_grads.reshape(6, 8, 4, per).transpose(2, 1, 0, 3)
    spread_rows = lax.dynamic_slice_in_dim(spread_rows, 2 * c, 2, 0)
    spread_up = up_bias_grad.reshape(2, 8, 1, bias_up.shape[0])

    def wide(v):
        return jnp.pad(v, ((0, 0), (0, 0), (0, 0), (0, 128 - v.shape[3])))

    tiles = jnp.concatenate(
        [wide(spread_bias), wide(spread_up), wide(spread_rows[:, :, :2].reshape(2, 8, 1, 2 * per)),
         wide(spread_rows[:, :, 2:].reshape(2, 8, 1, 4 * per)),
         jnp.zeros((2, 8, 3, 128), F32)],
        axis=2,
    ).reshape(2, 64, 128)
    back_chunks = (
        (3, 0, half),
        (3, half, half),
        (2, 0, half),
        (2, half, half),
        (1, 0, part),
        (0, 0, 3 * part),
        (4, 0, 128),
    )
    out_rows, token_rows, finals = reduce_all(
        result.astype(BF), token_grad.astype(BF), (*grads, tiles), back_chunks
    )
    tile = finals[4]
    return (
        out_rows,
        token_rows.astype(F32),
        finals[0].reshape(w_qkv.shape),
        tile[0:2, :per],
        finals[1].T,
        finals[2],
        tile[2, : bias_up.shape[0]],
        finals[3].T,
        tile[3, : 2 * per].reshape(2, per),
        tile[4, : 4 * per].reshape(4, per),
    )


def solution(mesh):
    return jax.shard_map(
        chip_local if dict(mesh.shape) == {"dp": 8, "tensor": 4} else local,
        mesh=mesh,
        in_specs=(
            P("dp", "tensor", None),
            P("dp"),
            P("dp", None, "tensor"),
            P(None, ("tensor", "dp")),
            P("tensor", "dp"),
            P("dp", "tensor"),
            P(("tensor", "dp")),
            P("tensor", "dp"),
            P(None, ("dp", "tensor")),
            P(None, ("dp", "tensor")),
            P("dp", "tensor", None),
        ),
        out_specs=(
            P("dp", "tensor", None),
            P("dp", "tensor", None),
            P("dp", None, "tensor"),
            P(None, ("tensor", "dp")),
            P("tensor", "dp"),
            P("dp", "tensor"),
            P(("tensor", "dp")),
            P("tensor", "dp"),
            P(None, ("dp", "tensor")),
            P(None, ("dp", "tensor")),
        ),
        check_vma=False,
    )
```

```python
from functools import partial

import jax
import jax.numpy as jnp
from jax import lax
from jax.experimental import pallas as pl
from jax.experimental.pallas import tpu as pltpu
from jax.sharding import PartitionSpec as P

DH = 64


EPSILON = 1e-05
MASKED_SCORE = -1e30


def norm_forward(values, gain_row, shift_row):
    center = values - jnp.mean(values, axis=-1, keepdims=True)
    inverse = lax.rsqrt(jnp.mean(center * center, axis=-1, keepdims=True) + EPSILON)
    normal = center * inverse
    return (normal * gain_row + shift_row, normal, inverse)


def norm_backward(incoming, normal, inverse, gain_row):
    scaled = incoming * gain_row
    first_mean = jnp.mean(scaled, axis=-1, keepdims=True)
    second_mean = jnp.mean(scaled * normal, axis=-1, keepdims=True)
    outgoing = inverse * (scaled - first_mean - normal * second_mean)
    return (outgoing, jnp.sum(incoming * normal, axis=0), jnp.sum(incoming, axis=0))


def visible_mask(offset, block_rows, length, prefix):
    row_ids = offset + jnp.arange(block_rows, dtype=jnp.int32)[:, None]
    column_ids = jnp.arange(length, dtype=jnp.int32)[None, :]
    return jnp.logical_or(column_ids < prefix, column_ids <= row_ids)


def block_scores(chosen, key_heads, offset, prefix, scaling):
    length = key_heads.shape[0]
    allowed = visible_mask(offset, chosen.shape[0], length, prefix)
    scores = (
        jnp.einsum("qhd,khd->hqk", chosen, key_heads, preferred_element_type=jnp.float32) * scaling
    )
    return jnp.where(allowed[None], scores, MASKED_SCORE)


def attention_forward(queries, key_heads, value_heads, prefix):
    length = key_heads.shape[0]
    block_rows = min(512, length)
    scaling = queries.shape[-1] ** (-0.5)
    outputs = []
    totals = []
    for offset in range(0, length, block_rows):
        scores = block_scores(
            queries[offset : offset + block_rows], key_heads, offset, prefix, scaling
        )
        row_max = jnp.max(scores, axis=-1, keepdims=True)
        log_total = jnp.log(jnp.sum(jnp.exp(scores - row_max), axis=-1, keepdims=True)) + row_max
        attn_probs = jnp.exp(scores - log_total).astype(jnp.bfloat16)
        outputs.append(
            jnp.einsum("hqk,khd->qhd", attn_probs, value_heads, preferred_element_type=jnp.float32)
        )
        totals.append(log_total)
    return (jnp.concatenate(outputs, axis=0), totals)


def attention_backward(queries, key_heads, value_heads, prefix, totals, context_grad):
    length = key_heads.shape[0]
    block_rows = min(512, length)
    scaling = queries.shape[-1] ** (-0.5)
    query_parts = []
    key_grad = jnp.zeros(key_heads.shape, jnp.float32)
    value_grad = jnp.zeros(value_heads.shape, jnp.float32)
    for number, offset in enumerate(range(0, length, block_rows)):
        chosen = queries[offset : offset + block_rows]
        grad_block = context_grad[offset : offset + block_rows]
        scores = block_scores(chosen, key_heads, offset, prefix, scaling)
        attn_probs = jnp.exp(scores - totals[number])
        probs_low = attn_probs.astype(jnp.bfloat16)
        probs_grad = jnp.einsum(
            "qhd,khd->hqk", grad_block, value_heads, preferred_element_type=jnp.float32
        )
        row_dot = jnp.sum(attn_probs * probs_grad, axis=-1, keepdims=True)
        scores_grad = (attn_probs * (probs_grad - row_dot)).astype(jnp.bfloat16)
        query_parts.append(
            jnp.einsum("hqk,khd->qhd", scores_grad, key_heads, preferred_element_type=jnp.float32)
            * scaling
        )
        key_grad = (
            key_grad
            + jnp.einsum("hqk,qhd->khd", scores_grad, chosen, preferred_element_type=jnp.float32)
            * scaling
        )
        value_grad = value_grad + jnp.einsum(
            "hqk,qhd->khd", probs_low, grad_block, preferred_element_type=jnp.float32
        )
    return (jnp.concatenate(query_parts, axis=0), key_grad, value_grad)


def local(
    tokens, prefix_len, w_qkv, bias_qv, w_out, w_up, bias_up, w_down, gains, shifts, cotangent
):
    tensor_count = lax.axis_size("tensor")
    seq_local, shard_rows, model_width = tokens.shape
    length = shard_rows * tensor_count
    full_qkv, full_bias_qv, full_out, full_up, full_bias_up, full_down = (
        lax.all_gather(w_qkv, "dp", axis=0, tiled=True),
        lax.all_gather(bias_qv, "dp", axis=1, tiled=True),
        lax.all_gather(w_out, "dp", axis=1, tiled=True),
        lax.all_gather(w_up, "dp", axis=0, tiled=True),
        lax.all_gather(bias_up, "dp", axis=0, tiled=True),
        lax.all_gather(w_down, "dp", axis=1, tiled=True),
    )
    full_gains, full_shifts = (
        lax.all_gather(gains, ("dp", "tensor"), axis=1, tiled=True),
        lax.all_gather(shifts, ("dp", "tensor"), axis=1, tiled=True),
    )
    full_gains = full_gains.astype(jnp.float32)
    full_shifts = full_shifts.astype(jnp.float32)
    bias_values = full_bias_qv.astype(jnp.float32)
    up_bias = full_bias_up.astype(jnp.float32)
    local_width = full_qkv.shape[2]
    head_count = local_width // DH
    kept_state = []
    outputs = []
    for member in range(seq_local):
        token_rows = tokens[member]
        prefix = prefix_len[member]

        def fold_tokens(piece):
            product = jnp.einsum("rd,dce->rce", piece, full_qkv, preferred_element_type=jnp.float32)
            return (piece, product)

        token_full, projected = fold_tokens(
            lax.all_gather(token_rows, "tensor", axis=0, tiled=True)
        )
        queries = (
            (projected[:, 0] + bias_values[0]).astype(jnp.bfloat16).reshape(length, head_count, DH)
        )
        key_heads = projected[:, 1].astype(jnp.bfloat16).reshape(length, head_count, DH)
        value_heads = (
            (projected[:, 2] + bias_values[1]).astype(jnp.bfloat16).reshape(length, head_count, DH)
        )
        context, totals = attention_forward(queries, key_heads, value_heads, prefix)
        context_low = context.reshape(length, local_width).astype(jnp.bfloat16)
        branch = (
            lax.psum_scatter(
                jnp.dot(context_low, full_out, preferred_element_type=jnp.float32).astype(
                    jnp.bfloat16
                ),
                "tensor",
                scatter_dimension=0,
                tiled=True,
            ).astype(jnp.float32)
            + full_shifts[0]
        )
        normed, normal_one, inverse_one = norm_forward(
            token_rows.astype(jnp.float32) + branch, full_gains[0], full_shifts[1]
        )
        normed_low = normed.astype(jnp.bfloat16)

        def fold_normed(piece):
            product = jnp.dot(piece, full_up, preferred_element_type=jnp.float32)
            return (piece, product)

        normed_full, pre_active = fold_normed(
            lax.all_gather(normed_low, "tensor", axis=0, tiled=True)
        )
        pre_active = pre_active + up_bias
        active_low = jax.nn.gelu(pre_active, approximate=False).astype(jnp.bfloat16)
        feed_out = (
            lax.psum_scatter(
                jnp.dot(active_low, full_down, preferred_element_type=jnp.float32).astype(
                    jnp.bfloat16
                ),
                "tensor",
                scatter_dimension=0,
                tiled=True,
            ).astype(jnp.float32)
            + full_shifts[2]
        )
        result, normal_two, inverse_two = norm_forward(
            normed + feed_out, full_gains[1], full_shifts[3]
        )
        outputs.append(result.astype(jnp.bfloat16))
        kept_state.append(
            (
                token_rows,
                prefix,
                token_full,
                queries,
                key_heads,
                value_heads,
                totals,
                context_low,
                normal_one,
                inverse_one,
                normed_full,
                pre_active,
                active_low,
                normal_two,
                inverse_two,
            )
        )
    back_qkv, back_out, back_up, back_down = (
        lax.all_gather(w_qkv, "dp", axis=0, tiled=True),
        lax.all_gather(w_out, "dp", axis=1, tiled=True),
        lax.all_gather(w_up, "dp", axis=0, tiled=True),
        lax.all_gather(w_down, "dp", axis=1, tiled=True),
    )
    full_shapes = (
        full_qkv.shape,
        full_bias_qv.shape,
        full_out.shape,
        full_up.shape,
        full_bias_up.shape,
        full_down.shape,
    )
    weight_grads = tuple((jnp.zeros(array_shape, jnp.float32) for array_shape in full_shapes))
    gain_grads = jnp.zeros((2, model_width), jnp.float32)
    shift_grads = jnp.zeros((4, model_width), jnp.float32)
    input_grads = []
    for member in range(seq_local):
        (
            token_rows,
            prefix,
            token_full,
            queries,
            key_heads,
            value_heads,
            totals,
            context_low,
            normal_one,
            inverse_one,
            normed_full,
            pre_active,
            active_low,
            normal_two,
            inverse_two,
        ) = kept_state[member]
        incoming = cotangent[member].astype(jnp.float32)
        residual_two, gain_two, shift_two = norm_backward(
            incoming, normal_two, inverse_two, full_gains[1]
        )
        feed_grad = residual_two.astype(jnp.bfloat16)
        fold_piece = lax.all_gather(feed_grad, "tensor", axis=0, tiled=True)
        down_grad = jnp.einsum(
            "rf,rd->fd", active_low, fold_piece, preferred_element_type=jnp.float32
        )
        fold_product = jnp.einsum(
            "rd,fd->rf", fold_piece, back_down, preferred_element_type=jnp.float32
        )
        active_grad = fold_product
        down_grad, active_grad = (down_grad, active_grad)
        layer_value, gelu_pull = jax.vjp(partial(jax.nn.gelu, approximate=False), pre_active)
        upper_grad = gelu_pull(active_grad)[0].astype(jnp.bfloat16)
        normed_grad = residual_two + lax.psum_scatter(
            jnp.einsum("rf,df->rd", upper_grad, back_up, preferred_element_type=jnp.float32).astype(
                jnp.bfloat16
            ),
            "tensor",
            scatter_dimension=0,
            tiled=True,
        ).astype(jnp.float32)
        up_grad = jnp.einsum(
            "ld,lf->df", normed_full, upper_grad, preferred_element_type=jnp.float32
        )
        up_bias_grad = jnp.sum(upper_grad.astype(jnp.float32), axis=0)
        residual_one, gain_one, shift_one = norm_backward(
            normed_grad, normal_one, inverse_one, full_gains[0]
        )
        branch_grad = residual_one.astype(jnp.bfloat16)

        def fold_branch(piece):
            out_grad = jnp.einsum(
                "rk,rd->kd", context_low, piece, preferred_element_type=jnp.float32
            )
            product = jnp.einsum("rd,kd->rk", piece, back_out, preferred_element_type=jnp.float32)
            return (out_grad, product)

        out_grad, context_grad = fold_branch(
            lax.all_gather(branch_grad, "tensor", axis=0, tiled=True)
        )
        context_grad = context_grad.astype(jnp.bfloat16).reshape(length, head_count, DH)
        query_grad, key_grad, value_grad = attention_backward(
            queries, key_heads, value_heads, prefix, totals, context_grad
        )
        mixed_grad = (
            jnp.stack([query_grad, key_grad, value_grad], axis=1)
            .astype(jnp.bfloat16)
            .reshape(length, 3, local_width)
        )
        qkv_grad = jnp.einsum(
            "ld,lce->dce", token_full, mixed_grad, preferred_element_type=jnp.float32
        )
        row_sums = jnp.sum(mixed_grad.astype(jnp.float32), axis=0)
        bias_grad = jnp.stack([row_sums[0], row_sums[2]])
        token_grad = residual_one + lax.psum_scatter(
            jnp.einsum(
                "rce,dce->rd", mixed_grad, back_qkv, preferred_element_type=jnp.float32
            ).astype(jnp.bfloat16),
            "tensor",
            scatter_dimension=0,
            tiled=True,
        ).astype(jnp.float32)
        input_grads.append(token_grad)
        gain_grads = gain_grads + jnp.stack([gain_one, gain_two])
        shift_grads = shift_grads + jnp.stack(
            [
                jnp.sum(branch_grad.astype(jnp.float32), axis=0),
                shift_one,
                jnp.sum(feed_grad.astype(jnp.float32), axis=0),
                shift_two,
            ]
        )
        member_grads = (qkv_grad, bias_grad, out_grad, up_grad, up_bias_grad, down_grad)
        weight_grads = tuple(
            (running + grad_part for running, grad_part in zip(weight_grads, member_grads))
        )
    total_qkv, total_bias, total_out, total_up, total_up_bias, total_down = weight_grads
    weight_grads = (
        lax.psum_scatter(total_qkv, "dp", scatter_dimension=0, tiled=True),
        lax.psum_scatter(total_bias, "dp", scatter_dimension=1, tiled=True),
        lax.psum_scatter(total_out, "dp", scatter_dimension=1, tiled=True),
        lax.psum_scatter(total_up, "dp", scatter_dimension=0, tiled=True),
        lax.psum_scatter(total_up_bias, "dp", scatter_dimension=0, tiled=True),
        lax.psum_scatter(total_down, "dp", scatter_dimension=1, tiled=True),
    )
    gain_share, shift_share = (
        lax.psum_scatter(gain_grads, ("dp", "tensor"), scatter_dimension=1, tiled=True),
        lax.psum_scatter(shift_grads, ("dp", "tensor"), scatter_dimension=1, tiled=True),
    )
    return (
        jnp.stack(outputs),
        jnp.stack(input_grads),
        weight_grads[0],
        weight_grads[1],
        weight_grads[2],
        weight_grads[3],
        weight_grads[4],
        weight_grads[5],
        gain_share,
        shift_share,
    )


MESH_ID = pl.DeviceIdType.MESH
BF = jnp.bfloat16
F32 = jnp.float32
ROWS = 96
SMALL = 16


def place():
    d = lax.axis_index("dp")
    t = lax.axis_index("tensor")
    k, c = d // 2, d % 2
    xb, yb = k % 2, k // 2
    dx = d + 2 - 4 * xb
    dy = d + 4 - 8 * yb
    return d, t, k, c, xb, yb, dx, dy


def remote(src, dst, send, recv, dp, tensor):
    return pltpu.make_async_remote_copy(
        src_ref=src,
        dst_ref=dst,
        send_sem=send,
        recv_sem=recv,
        device_id=(dp, tensor),
        device_id_type=MESH_ID,
    )


def enter(k, c, t, d, dx, dy):
    barrier = pltpu.get_barrier_semaphore()

    def greet(dp, tensor):
        pl.semaphore_signal(barrier, inc=1, device_id=(dp, tensor), device_id_type=MESH_ID)

    greet(dx, t)
    greet(dy, t)
    greet(d + 1 - 2 * c, t)
    for step in range(1, 4):
        other = (t + step) % 4
        greet(2 * k, other)
        greet(2 * k + 1, other)
    pl.semaphore_wait(barrier, 9)


def pair_swap(part):
    def kernel(src, dst, send, recv):
        d, t, k, c, xb, yb, dx, dy = place()
        mate = d + 1 - 2 * c
        barrier = pltpu.get_barrier_semaphore()
        pl.semaphore_signal(barrier, inc=1, device_id=(mate, t), device_id_type=MESH_ID)
        pl.semaphore_wait(barrier, 1)
        rows = src.shape[0] // 4
        copies = [
            remote(
                src.at[pl.ds(i * rows, rows)],
                dst.at[pl.ds(i * rows, rows)],
                send.at[i],
                recv.at[i],
                mate,
                t,
            )
            for i in range(4)
        ]
        for copy in copies:
            copy.start()
        for copy in copies:
            copy.wait()

    return pl.pallas_call(
        kernel,
        out_shape=jax.ShapeDtypeStruct(part.shape, part.dtype),
        in_specs=[pl.BlockSpec(memory_space=pl.ANY)],
        out_specs=pl.BlockSpec(memory_space=pl.ANY),
        scratch_shapes=[pltpu.SemaphoreType.DMA((4,)), pltpu.SemaphoreType.DMA((4,))],
        compiler_params=pltpu.CompilerParams(collective_id=3, has_side_effects=True),
    )(part)


def skewed(chunks, levels):
    for slot in range(chunks + len(levels) - 1):
        for level in reversed(range(len(levels))):
            if 0 <= slot - level < chunks:
                levels[level](slot - level)


def gather_attend(tokens, cotangent, shards, chunks, per):
    half = tokens.shape[1] // 2
    width = tokens.shape[2]
    count = len(shards)
    n_chunks = len(chunks)
    rows_of = [s.shape[0] for s in shards]
    length = tokens.shape[1] * 4
    part = shards[0].shape[1] // 3
    heads_width = 2 * part
    blocks = length // BLOCK

    def kernel(*refs):
        tok, cot = refs[0], refs[1]
        own = refs[2 : 2 + count]
        base = 2 + count
        xf, cf = refs[base], refs[base + 1]
        full = refs[base + 2 : base + 2 + count]
        small_other, q_out, k_out, v_out, o_out, lt_out = refs[base + 2 + count : base + 8 + count]
        stage = refs[base + 8 + count : base + 8 + 2 * count]
        (
            x_rows,
            weight,
            small_low,
            small_rows,
            load_sem,
            row_stage,
            local_sem,
            row_sem,
            ex_send,
            ex_recv,
            fw_send,
            fw_recv,
            p_send,
            p_recv,
            z_send,
            z_recv,
            a_send,
            a_recv,
            b_send,
            b_recv,
            o_send,
            o_recv,
        ) = refs[base + 8 + 2 * count :]
        d, t, k, c, xb, yb, dx, dy = place()
        mate = d + 1 - 2 * c
        u = t + c * (3 - 2 * t)
        up = t + 1 - 2 * c
        down = t - 1 + 2 * c
        source = t // 2 == c
        enter(k, c, t, d, dx, dy)

        for s in range(count):
            rows = rows_of[s]
            spot = full[s].at[t % 2, pl.ds(d * rows, rows)]

            @pl.when(source)
            def _():
                pltpu.make_async_copy(own[s], stage[s], local_sem.at[s]).start()

            @pl.when(jnp.logical_not(source))
            def _():
                remote(own[s], spot, p_send.at[s], p_recv.at[s], mate, t).start()

        def exchange(which, src, dst):
            for m in range(2):
                goal = 2 * c + m
                for core in range(2):
                    piece = src.at[m, pl.ds(core * half, half)]
                    spot = dst.at[t * 2 + core]
                    here = jnp.logical_and(goal == t, core == c)

                    @pl.when(here)
                    def _():
                        load = pltpu.make_async_copy(piece, row_stage, row_sem)
                        load.start()
                        load.wait()
                        store = pltpu.make_async_copy(row_stage, spot, row_sem)
                        store.start()
                        store.wait()

                    @pl.when(jnp.logical_not(here))
                    def _():
                        remote(
                            piece,
                            spot,
                            ex_send.at[which, 2 * m + core],
                            ex_recv.at[which, t],
                            2 * k + core,
                            goal,
                        ).start()

        def relay(which, dst):
            for origin in range(4):
                spot = dst.at[origin * 2 + c]
                local = jnp.logical_and(origin == t, c == t // 2)

                @pl.when(jnp.logical_not(local))
                def _():
                    remote(
                        spot, spot, ex_send.at[which, 0], ex_recv.at[which, origin], mate, t
                    ).wait_recv()

                remote(
                    spot, spot, fw_send.at[which, origin], fw_recv.at[which, origin], mate, t
                ).start()

        def arrived(which, dst):
            for origin in range(4):
                spot = dst.at[origin * 2 + 1 - c]
                remote(
                    spot, spot, fw_send.at[which, origin], fw_recv.at[which, origin], mate, t
                ).wait_recv()

        def settle(which, src, dst):
            for origin in range(4):
                spot = dst.at[origin * 2 + 1 - c]
                remote(
                    spot, spot, fw_send.at[which, origin], fw_recv.at[which, origin], mate, t
                ).wait_send()
            for m in range(2):
                for core in range(2):
                    here = jnp.logical_and(2 * c + m == t, core == c)

                    @pl.when(jnp.logical_not(here))
                    def _():
                        remote(
                            src.at[m, pl.ds(core * half, half)],
                            dst.at[t * 2 + core],
                            ex_send.at[which, 2 * m + core],
                            ex_recv.at[which, t],
                            mate,
                            t,
                        ).wait_send()

        def placed(s):
            @pl.when(source)
            def _():
                rows = rows_of[s]
                spot = full[s].at[t % 2, pl.ds(d * rows, rows)]
                pltpu.make_async_copy(own[s], stage[s], local_sem.at[s]).wait()
                pltpu.make_async_copy(stage[s], spot, local_sem.at[s]).start()

        def block(i, b, start, n):
            s, col, cols = chunks[i]
            zz = b + c * (1 - 2 * b)
            rows = rows_of[s]
            return full[s].at[zz, pl.ds(start * rows, n * rows), pl.ds(col, cols)]

        def z_copy(i, b, way, target):
            ref = block(i, b, 2 * k, 2)
            return remote(ref, ref, z_send.at[i, b, way], z_recv.at[i, b], d, target)

        def first_copy(i, b):
            ref = block(i, b, 2 * k, 2)
            return remote(ref, ref, a_send.at[i, b], a_recv.at[i, b], dx if b == 0 else dy, t)

        def first_arrival(i, b):
            near = k + 1 - 2 * xb if b == 0 else k + 2 - 4 * yb
            ref = block(i, b, 2 * near, 2)
            return remote(ref, ref, a_send.at[i, b], a_recv.at[i, b], dx if b == 0 else dy, t)

        def second_copies(i, arriving):
            other = 1 if arriving else 0
            row = yb + other * (1 - 2 * yb)
            ref = block(i, 0, 4 * row, 4)
            col = xb + other * (1 - 2 * xb)
            out = [remote(ref, ref, b_send.at[i, 0], b_recv.at[i, 0], dy, t)]
            for r in range(2):
                ref = block(i, 1, 2 * (2 * r + col), 2)
                out.append(remote(ref, ref, b_send.at[i, 1 + r], b_recv.at[i, 1 + r], dx, t))
            return out

        def spread(i, b):
            @pl.when(jnp.logical_and(u >= b, u < 3))
            def _():
                z_copy(i, b, 0, up).start()

            if b == 1:

                @pl.when(u == 1)
                def _():
                    z_copy(i, 1, 1, down).start()

            first_copy(i, b).start()

        waited = set()

        def own_ready(i):
            s = chunks[i][0]
            if s in waited:
                return
            waited.add(s)
            rows = rows_of[s]
            spot = full[s].at[t % 2, pl.ds(d * rows, rows)]
            twin = full[s].at[t % 2, pl.ds(mate * rows, rows)]
            pltpu.make_async_copy(stage[s], spot, local_sem.at[s]).wait()
            remote(twin, twin, p_send.at[s], p_recv.at[s], mate, t).wait_recv()

        def level_own(i):
            if chunks[i][0] not in waited:

                @pl.when(source)
                def _():
                    own_ready(i)

            for b in range(2):

                @pl.when(u == b)
                def _():
                    spread(i, b)

        def level_line(i):
            for b in (1, 0):

                @pl.when(u != b)
                def _():
                    z_copy(i, b, 0, up).wait_recv()
                    spread(i, b)

        def level_second(i):
            for b in range(2):
                first_arrival(i, b).wait_recv()
            for copy in second_copies(i, False):
                copy.start()

        def level_done(i):
            for copy in second_copies(i, True):
                copy.wait_recv()

        def expand(plane, kind):
            rows = small_rows[plane, pl.ds(kind, 8, stride=SMALL), :]
            spots = lax.broadcasted_iota(jnp.int32, (128, part), 0)
            lane = lax.broadcasted_iota(jnp.int32, (128, part), 1)
            wide = jnp.dot(
                rows,
                (spots == lane % per).astype(F32),
                precision=lax.Precision.HIGHEST,
                preferred_element_type=F32,
            )
            row = lax.broadcasted_iota(jnp.int32, (8, part), 0)
            lane = lax.broadcasted_iota(jnp.int32, (8, part), 1)
            return jnp.sum(jnp.where(lane // per == row, wide, 0.0), axis=0, keepdims=True)

        def prefix_of():
            tile = small_rows[0, pl.ds((2 * k + t // 2) * SMALL + 9, 1), 0:128]
            lane = lax.broadcasted_iota(jnp.int32, (1, 128), 1)
            member = t % 2
            value = 16.0 * jnp.sum(jnp.where(lane == member, tile, 0.0), axis=1, keepdims=True)
            value += jnp.sum(jnp.where(lane == 2 + member, tile, 0.0), axis=1, keepdims=True)
            return value

        def project():
            bias_q = jnp.concatenate([expand(0, 0), expand(1, 0)], axis=1)
            bias_v = jnp.concatenate([expand(0, 1), expand(1, 1)], axis=1)

            @pl.loop(0, blocks)
            def _(block_id):
                rows = pl.ds(block_id * BLOCK, BLOCK)
                both = [
                    jnp.dot(x_rows[rows, :], weight[z], preferred_element_type=F32)
                    for z in range(2)
                ]

                def kind(i):
                    return jnp.concatenate([v[:, i * part : (i + 1) * part] for v in both], axis=1)

                q_out[rows, :] = (kind(0) + bias_q).astype(BF)
                k_out[rows, :] = kind(1).astype(BF)
                v_out[rows, :] = (kind(2) + bias_v).astype(BF)

        load_rows = [
            pltpu.make_async_copy(xf.at[i], x_rows.at[pl.ds(i * half, half)], load_sem.at[i])
            for i in range(8)
        ]
        load_weight = pltpu.make_async_copy(full[0], weight, load_sem.at[8])
        last = count - 1
        swap = remote(full[last], small_other, o_send, o_recv, mate, t)

        placed(last)
        placed(0)
        level_own(0)
        level_own(1)
        exchange(0, tok, xf)
        for s in range(1, last):
            placed(s)
        level_line(0)
        level_line(1)
        level_second(0)
        level_own(2)
        level_own(3)
        level_second(1)
        relay(0, xf)
        level_line(2)
        level_own(4)
        level_done(0)
        swap.start()
        small_load = pltpu.make_async_copy(full[last], small_low, load_sem.at[9])
        small_load.start()
        arrived(0, xf)
        for copy in load_rows:
            copy.start()
        level_line(3)
        level_second(2)
        for i in range(5, n_chunks):
            level_own(i)
        small_load.wait()
        small_rows[...] = small_low[...].astype(F32)
        level_done(1)
        load_weight.start()
        level_second(3)
        exchange(1, cot, cf)
        for copy in load_rows:
            copy.wait()
        load_weight.wait()
        project()
        todo = []
        for i in range(4, n_chunks):
            todo.append(partial(level_line, i))
            todo.append(partial(level_second, i))
        todo.append(lambda: relay(1, cf))
        work = [
            partial(attend_rows, q_out, k_out, v_out, o_out, lt_out, prefix_of(), pair, qb)
            for pair in range(heads_width // 128)
            for qb in range(blocks)
        ]
        for step in range(max(len(todo), len(work))):
            if step < len(todo):
                todo[step]()
            if step < len(work):
                work[step]()
        for i in range(2, n_chunks):
            level_done(i)
        arrived(1, cf)
        settle(0, tok, xf)
        settle(1, cot, cf)
        for s in range(count):
            rows = rows_of[s]
            spot = full[s].at[t % 2, pl.ds(d * rows, rows)]

            @pl.when(jnp.logical_not(source))
            def _():
                remote(own[s], spot, p_send.at[s], p_recv.at[s], mate, t).wait_send()

        for i in range(n_chunks):
            for b in range(2):

                @pl.when(jnp.logical_and(u >= b, u < 3))
                def _():
                    z_copy(i, b, 0, up).wait_send()

                first_copy(i, b).wait_send()

            @pl.when(u == 1)
            def _():
                z_copy(i, 1, 1, down).wait_send()

            for copy in second_copies(i, False):
                copy.wait_send()
        swap.wait()

    any_spec = pl.BlockSpec(memory_space=pl.ANY)
    vmem = pl.BlockSpec(memory_space=pltpu.VMEM)
    dma = pltpu.SemaphoreType.DMA
    full_shapes = [jax.ShapeDtypeStruct((2, 8 * s.shape[0], s.shape[1]), s.dtype) for s in shards]
    rows_shape = jax.ShapeDtypeStruct((8, half, width), tokens.dtype)
    head_shape = jax.ShapeDtypeStruct((length, heads_width), BF)
    lt_shape = jax.ShapeDtypeStruct((heads_width // DH, 8, length), F32)
    outs = pl.pallas_call(
        kernel,
        out_shape=[
            rows_shape,
            rows_shape,
            *full_shapes,
            full_shapes[-1],
            *[head_shape] * 4,
            lt_shape,
        ],
        in_specs=[any_spec] * (2 + count),
        out_specs=[any_spec] * (3 + count) + [vmem] * 5,
        scratch_shapes=[
            *[pltpu.VMEM(s.shape, s.dtype) for s in shards],
            pltpu.VMEM((length, width), BF),
            pltpu.VMEM((2, 8 * shards[0].shape[0], shards[0].shape[1]), BF),
            pltpu.VMEM((2, 8 * SMALL, 128), BF),
            pltpu.VMEM((2, 8 * SMALL, 128), F32),
            dma((10,)),
            pltpu.VMEM((half, width), tokens.dtype),
            dma((count,)),
            dma,
            dma((2, 4)),
            dma((2, 4)),
            dma((2, 4)),
            dma((2, 4)),
            dma((count,)),
            dma((count,)),
            dma((n_chunks, 2, 2)),
            dma((n_chunks, 2)),
            dma((n_chunks, 2)),
            dma((n_chunks, 2)),
            dma((n_chunks, 3)),
            dma((n_chunks, 3)),
            dma,
            dma,
        ],
        compiler_params=pltpu.CompilerParams(
            collective_id=1, has_side_effects=True, vmem_limit_bytes=60 * 1024 * 1024
        ),
    )(tokens, cotangent, *shards)
    return (
        outs[0].reshape(length, width),
        outs[1].reshape(length, width),
        outs[2 : 2 + count],
        outs[2 + count],
        outs[3 + count :],
    )


def reduce_all(output, token_grad, grads, chunks):
    count = len(grads)
    n_chunks = len(chunks)
    length, width = output.shape
    half = length // 8
    rows_of = [g.shape[1] // 8 for g in grads]

    def kernel(*refs):
        res, tgr = refs[0], refs[1]
        part = refs[2 : 2 + count]
        base = 2 + count
        res_out, tgr_out = refs[base], refs[base + 1]
        final = refs[base + 2 : base + 2 + count]
        base += 2 + count
        got1 = refs[base : base + count]
        sum1 = refs[base + count : base + 2 * count]
        got2 = refs[base + 2 * count : base + 3 * count]
        sum2 = refs[base + 3 * count : base + 4 * count]
        got3 = refs[base + 4 * count : base + 5 * count]
        sum3 = refs[base + 5 * count : base + 6 * count]
        got4 = refs[base + 6 * count : base + 7 * count]
        got5 = refs[base + 7 * count : base + 8 * count]
        (
            row_stage,
            row_sem,
            ex_send,
            ex_recv,
            a_send,
            a_recv,
            b_send,
            b_recv,
            z_send,
            z_recv,
            y_send,
            y_recv,
            p_send,
            p_recv,
        ) = refs[base + 8 * count :]
        d, t, k, c, xb, yb, dx, dy = place()
        mate = d + 1 - 2 * c
        u = t + c * (3 - 2 * t)
        up = t + 1 - 2 * c
        down = t - 1 + 2 * c
        source = u <= 1
        enter(k, c, t, d, dx, dy)

        def return_rows(which, src, dst, start):
            for goal in range(4):
                piece = src.at[pl.ds((goal * 2 + c) * half, half)]
                spot = dst.at[t % 2, pl.ds(c * half, half)]
                here = jnp.logical_and(goal == t, c == t // 2)
                copy = remote(
                    piece,
                    spot,
                    ex_send.at[which, goal],
                    ex_recv.at[which, t % 2, c],
                    2 * k + t // 2,
                    goal,
                )

                @pl.when(here)
                def _():
                    if start:
                        load = pltpu.make_async_copy(piece, row_stage, row_sem)
                        load.start()
                        load.wait()
                        store = pltpu.make_async_copy(row_stage, spot, row_sem)
                        store.start()
                        store.wait()

                @pl.when(jnp.logical_not(here))
                def _():
                    if start:
                        copy.start()
                    else:
                        copy.wait_send()

            if not start:
                for m in range(2):
                    for core in range(2):
                        spot = dst.at[m, pl.ds(core * half, half)]
                        here = jnp.logical_and(2 * c + m == t, core == c)

                        @pl.when(jnp.logical_not(here))
                        def _():
                            remote(
                                spot,
                                spot,
                                ex_send.at[which, 0],
                                ex_recv.at[which, m, core],
                                mate,
                                t,
                            ).wait_recv()

        def plane(b):
            return b + c * (1 - 2 * b)

        def first_copies(i):
            s, col, cols = chunks[i]
            rows = rows_of[s]
            spot = pl.ds(col, cols)
            out = [
                remote(
                    part[s].at[plane(0), pl.ds((1 - yb) * 4 * rows, 4 * rows), spot],
                    got1[s].at[0, :, spot],
                    a_send.at[i, 0],
                    a_recv.at[i, 0],
                    dy,
                    t,
                )
            ]
            for r in range(2):
                out.append(
                    remote(
                        part[s].at[plane(1), pl.ds((2 * r + 1 - xb) * 2 * rows, 2 * rows), spot],
                        got1[s].at[1, pl.ds(r * 2 * rows, 2 * rows), spot],
                        a_send.at[i, 1 + r],
                        a_recv.at[i, 1 + r],
                        dx,
                        t,
                    )
                )
            return out

        def second_copies(i):
            s, col, cols = chunks[i]
            rows = rows_of[s]
            spot = pl.ds(col, cols)
            out = []
            for b, far, goal in ((0, 1 - xb, dx), (1, 1 - yb, dy)):
                out.append(
                    remote(
                        sum1[s].at[b, pl.ds(far * 2 * rows, 2 * rows), spot],
                        got2[s].at[b, :, spot],
                        b_send.at[i, b],
                        b_recv.at[i, b],
                        goal,
                        t,
                    )
                )
            return out

        def low(v, s):
            return v.astype(sum1[s].dtype)

        def level_first(i):
            for copy in first_copies(i):
                copy.start()

        def level_second(i):
            s, col, cols = chunks[i]
            rows = rows_of[s]
            spot = pl.ds(col, cols)
            for copy in first_copies(i):
                copy.wait_recv()
            mine = part[s][plane(0), pl.ds(yb * 4 * rows, 4 * rows), spot]
            sum1[s][0, :, spot] = low(mine.astype(F32) + got1[s][0, :, spot].astype(F32), s)
            for r in range(2):
                mine = part[s][plane(1), pl.ds((2 * r + xb) * 2 * rows, 2 * rows), spot]
                there = pl.ds(r * 2 * rows, 2 * rows)
                sum1[s][1, there, spot] = low(
                    mine.astype(F32) + got1[s][1, there, spot].astype(F32), s
                )
            for copy in second_copies(i):
                copy.start()

        def z_copy(i, b):
            s, col, cols = chunks[i]
            spot = pl.ds(col, cols)
            return remote(
                sum3[s].at[b, :, spot],
                got3[s].at[b, :, spot],
                z_send.at[i, b],
                z_recv.at[i, b],
                d,
                down,
            )

        def y_copy(i):
            s, col, cols = chunks[i]
            spot = pl.ds(col, cols)
            return remote(
                sum3[s].at[1, :, spot], got4[s].at[:, spot], y_send.at[i], y_recv.at[i], d, up
            )

        def level_line(i):
            s, col, cols = chunks[i]
            rows = rows_of[s]
            spot = pl.ds(col, cols)
            for copy in second_copies(i):
                copy.wait_recv()
            for b, near in ((0, xb), (1, yb)):
                mine = sum1[s][b, pl.ds(near * 2 * rows, 2 * rows), spot]
                sum2[s][b, :, spot] = mine.astype(F32) + got2[s][b, :, spot].astype(F32)

            @pl.when(u == 3)
            def _():
                for b in range(2):
                    sum3[s][b, :, spot] = low(sum2[s][b, :, spot], s)
                    z_copy(i, b).start()

            @pl.when(u == 0)
            def _():
                sum3[s][1, :, spot] = low(sum2[s][1, :, spot], s)
                y_copy(i).start()

        def level_pass(i):
            s, col, cols = chunks[i]
            spot = pl.ds(col, cols)

            @pl.when(u == 2)
            def _():
                for b in range(2):
                    z_copy(i, b).wait_recv()
                    sum3[s][b, :, spot] = low(
                        sum2[s][b, :, spot] + got3[s][b, :, spot].astype(F32), s
                    )
                    z_copy(i, b).start()

        def level_near(i):
            s, col, cols = chunks[i]
            spot = pl.ds(col, cols)

            @pl.when(u == 1)
            def _():
                z_copy(i, 0).wait_recv()
                sum3[s][0, :, spot] = low(
                    sum2[s][0, :, spot] + got3[s][0, :, spot].astype(F32), s
                )
                z_copy(i, 0).start()
                z_copy(i, 1).wait_recv()
                y_copy(i).wait_recv()
                total = (
                    sum2[s][1, :, spot]
                    + got3[s][1, :, spot].astype(F32)
                    + got4[s][:, spot].astype(F32)
                )
                finish(i, total)

            @pl.when(u == 0)
            def _():
                z_copy(i, 0).wait_recv()
                finish(i, sum2[s][0, :, spot] + got3[s][0, :, spot].astype(F32))

        def p_copy(i):
            s, col, cols = chunks[i]
            rows = rows_of[s]
            spot = pl.ds(col, cols)
            return remote(
                sum1[s].at[0, pl.ds((1 - c) * rows, rows), spot],
                got5[s].at[:, spot],
                p_send.at[i],
                p_recv.at[i],
                mate,
                t,
            )

        def finish(i, total):
            s, col, cols = chunks[i]
            rows = rows_of[s]
            spot = pl.ds(col, cols)
            for copy in second_copies(i):
                copy.wait_send()
            sum2[s][0, :, spot] = total
            sum1[s][0, pl.ds(0, 2 * rows), spot] = low(total, s)
            p_copy(i).start()
            final[s][:, spot] = sum2[s][0, pl.ds(c * rows, rows), spot]

        def level_mate(i):
            s, col, cols = chunks[i]
            spot = pl.ds(col, cols)

            @pl.when(u >= 2)
            def _():
                p_copy(i).wait_recv()
                final[s][:, spot] = got5[s][:, spot].astype(F32)

        return_rows(0, res, res_out, True)
        return_rows(1, tgr, tgr_out, True)
        skewed(
            n_chunks, [level_first, level_second, level_line, level_pass, level_near, level_mate]
        )
        return_rows(0, res, res_out, False)
        return_rows(1, tgr, tgr_out, False)
        for i in range(n_chunks):
            for copy in first_copies(i):
                copy.wait_send()

            @pl.when(u >= 2)
            def _():
                for copy in second_copies(i):
                    copy.wait_send()
                for b in range(2):
                    z_copy(i, b).wait_send()

            @pl.when(u == 1)
            def _():
                z_copy(i, 0).wait_send()

            @pl.when(u == 0)
            def _():
                y_copy(i).wait_send()

            @pl.when(u <= 1)
            def _():
                p_copy(i).wait_send()

    any_spec = pl.BlockSpec(memory_space=pl.ANY)
    vmem = pl.BlockSpec(memory_space=pltpu.VMEM)
    dma = pltpu.SemaphoreType.DMA
    scratch = []
    for kind in range(8):
        for s in range(count):
            rows, cols, kept = rows_of[s], grads[s].shape[2], grads[s].dtype
            shape, dtype = (
                ((2, 4 * rows, cols), kept),
                ((2, 4 * rows, cols), kept),
                ((2, 2 * rows, cols), kept),
                ((2, 2 * rows, cols), F32),
                ((2, 2 * rows, cols), kept),
                ((2, 2 * rows, cols), kept),
                ((2 * rows, cols), kept),
                ((rows, cols), kept),
            )[kind]
            scratch.append(pltpu.VMEM(shape, dtype))
    back = jax.ShapeDtypeStruct((2, 2 * half, width), output.dtype)
    outs = pl.pallas_call(
        kernel,
        out_shape=[
            back,
            back,
            *[jax.ShapeDtypeStruct((r, g.shape[2]), F32) for r, g in zip(rows_of, grads)],
        ],
        in_specs=[any_spec, any_spec] + [vmem] * count,
        out_specs=[any_spec, any_spec] + [vmem] * count,
        scratch_shapes=[
            *scratch,
            pltpu.VMEM((half, width), output.dtype),
            dma,
            dma((2, 4)),
            dma((2, 2, 2)),
            dma((n_chunks, 3)),
            dma((n_chunks, 3)),
            dma((n_chunks, 2)),
            dma((n_chunks, 2)),
            dma((n_chunks, 2)),
            dma((n_chunks, 2)),
            dma((n_chunks,)),
            dma((n_chunks,)),
            dma((n_chunks,)),
            dma((n_chunks,)),
        ],
        compiler_params=pltpu.CompilerParams(
            collective_id=2, has_side_effects=True, vmem_limit_bytes=60 * 1024 * 1024
        ),
    )(output, token_grad, *grads)
    return outs[0], outs[1], outs[2:]


BLOCK = 256


def lane_half(shape, h):
    lane = lax.broadcasted_iota(jnp.int32, shape, 1)
    return lane < DH if h == 0 else lane >= DH


def reach(row_block, blocks):
    return max(row_block + 1, blocks // 2)


def dot_nt(a, b):
    return lax.dot_general(a, b, (((1,), (1,)), ((), ())), preferred_element_type=F32)


def dot_tn(a, b):
    return lax.dot_general(a, b, (((0,), (0,)), ((), ())), preferred_element_type=F32)


def attend_rows(q_ref, k_ref, v_ref, o_ref, lt_ref, limit, pair, qb):
    length = q_ref.shape[0]
    blocks = length // BLOCK
    lanes = pl.ds(pair * 128, 128)
    rows = pl.ds(qb * BLOCK, BLOCK)
    span = reach(qb, blocks) * BLOCK
    q = q_ref[rows, lanes] * jnp.asarray(DH**-0.5, BF)
    heads = []
    for h in range(2):
        half = lane_half((BLOCK, 128), h)
        s = dot_nt(jnp.where(half, q, jnp.zeros_like(q)), k_ref[pl.ds(0, span), lanes])
        clear = qb * BLOCK
        row = lax.broadcasted_iota(jnp.int32, (BLOCK, span - clear), 0) + clear
        col = lax.broadcasted_iota(jnp.int32, (BLOCK, span - clear), 1) + clear
        seen = col <= row
        if clear < length // 2:
            seen = jnp.logical_or(seen, col.astype(F32) < limit)
        tail = jnp.where(seen, s[:, clear:], MASKED_SCORE)
        s = jnp.concatenate([s[:, :clear], tail], axis=1) if clear else tail
        top = jnp.max(s, axis=1, keepdims=True)
        p = jnp.exp(s - top)
        total = jnp.sum(p, axis=1, keepdims=True)
        log_total = top + jnp.log(total)
        lt_ref[2 * pair + h, 0:1, rows] = jnp.transpose(
            jnp.broadcast_to(log_total, (BLOCK, 128))
        )[0:1, :]
        p = (p * (1.0 / total)).astype(BF)
        heads.append(jnp.dot(p, v_ref[pl.ds(0, span), lanes], preferred_element_type=F32))
    o_ref[rows, lanes] = jnp.where(lane_half((BLOCK, 128), 0), heads[0], heads[1]).astype(BF)


def attend_back(queries, keys, values, prefix, totals, context, context_grad):
    length, width = queries.shape
    blocks = length // BLOCK
    pairs = width // 128

    def kernel(prefix_ref, q_ref, k_ref, v_ref, lt_ref, o_ref, do_ref, dq_ref, dk_ref, dv_ref, acc):
        limit = prefix_ref[0]
        scaling = jnp.asarray(DH**-0.5, BF)
        head_row = lax.broadcasted_iota(jnp.int32, (8, 128), 0)
        lane = lax.broadcasted_iota(jnp.int32, (8, 128), 1)
        pick = (lane // DH == head_row).astype(F32)
        row_dots = []
        for qb in range(blocks):
            rows = pl.ds(qb * BLOCK, BLOCK)
            both = do_ref[rows, :].astype(F32) * o_ref[rows, :].astype(F32)
            row_dots.append(
                lax.dot_general(
                    pick,
                    both,
                    (((1,), (1,)), ((), ())),
                    precision=lax.Precision.HIGHEST,
                    preferred_element_type=F32,
                )
            )
        acc[...] = jnp.zeros_like(acc)
        for kb in range(blocks):
            keys_at = pl.ds(kb * BLOCK, BLOCK)
            key = k_ref[keys_at, :]
            value = v_ref[keys_at, :]
            dk = jnp.zeros((BLOCK, 128), F32)
            dv = jnp.zeros((BLOCK, 128), F32)
            for qb in range(blocks):
                if kb >= reach(qb, blocks):
                    continue
                rows = pl.ds(qb * BLOCK, BLOCK)
                q_pair = q_ref[rows, :] * scaling
                do_pair = do_ref[rows, :]
                for h in range(2):
                    half = lane_half((BLOCK, 128), h)
                    zero = jnp.zeros((BLOCK, 128), BF)
                    q = jnp.where(half, q_pair, zero)
                    do = jnp.where(half, do_pair, zero)
                    s = dot_nt(key, q)
                    if kb >= qb:
                        key_id = lax.broadcasted_iota(jnp.int32, (BLOCK, BLOCK), 0) + kb * BLOCK
                        row_id = lax.broadcasted_iota(jnp.int32, (BLOCK, BLOCK), 1) + qb * BLOCK
                        seen = key_id <= row_id
                        if kb * BLOCK < length // 2:
                            seen = jnp.logical_or(seen, key_id < limit)
                        s = jnp.where(seen, s, MASKED_SCORE)
                    p = jnp.exp(s - lt_ref[h, 0:1, rows])
                    dp = dot_nt(value, do)
                    ds = (p * (dp - row_dots[qb][h : h + 1, :])).astype(BF)
                    dv = dv + jnp.dot(p.astype(BF), do, preferred_element_type=F32)
                    dk = dk + jnp.dot(ds, q, preferred_element_type=F32)
                    acc[rows, :] += dot_tn(ds, jnp.where(half, key, zero))
            dk_ref[keys_at, :] = dk.astype(BF)
            dv_ref[keys_at, :] = dv.astype(BF)
        dq_ref[...] = (acc[...] * DH**-0.5).astype(BF)

    pair = pl.BlockSpec((length, 128), lambda i: (0, i))
    shape = jax.ShapeDtypeStruct((length, width), BF)
    return pl.pallas_call(
        kernel,
        grid=(pairs,),
        out_shape=[shape] * 3,
        in_specs=[
            pl.BlockSpec(memory_space=pltpu.SMEM),
            pair,
            pair,
            pair,
            pl.BlockSpec((2, 8, length), lambda i: (i, 0, 0)),
            pair,
            pair,
        ],
        out_specs=[pair] * 3,
        scratch_shapes=[pltpu.VMEM((length, 128), F32)],
    )(prefix, queries, keys, values, totals, context, context_grad)


def chip_local(
    tokens, prefix_len, w_qkv, bias_qv, w_out, w_up, bias_up, w_down, gains, shifts, cotangent
):
    d, t, k, c, _, _, _, _ = place()
    model_width = tokens.shape[2]
    length = tokens.shape[1] * 4
    part = w_qkv.shape[2]
    hidden = w_up.shape[1]

    def lanes(v):
        return jnp.pad(v, ((0, 0), (0, 128 - v.shape[1])))

    limits = jnp.concatenate([prefix_len // 16, prefix_len % 16]).astype(BF)[None]
    small = jnp.concatenate(
        [lanes(v) for v in (bias_qv, bias_up[None], gains, shifts, limits)], axis=0
    )
    small = jnp.pad(small, ((0, SMALL - small.shape[0]), (0, 0)))
    shards = (
        w_qkv.reshape(ROWS, 3 * part),
        w_out.T,
        w_up,
        w_down.T,
        small,
    )
    half = hidden // 2
    chunks = (
        (4, 0, 128),
        (0, 0, 3 * part),
        (1, 0, part),
        (2, 0, half),
        (2, half, half),
        (3, 0, half),
        (3, half, half),
    )
    x, cot, (g_qkv, g_out, g_up, g_down, g_small), small_other, heads = gather_attend(
        tokens, cotangent, shards, chunks, bias_qv.shape[1]
    )
    queries, key_heads, value_heads, context, totals = heads

    mine = g_small.reshape(2, 8, SMALL, 128)
    theirs = small_other.reshape(2, 8, SMALL, 128)
    first = jnp.where(c == 0, mine, theirs)
    every = jnp.concatenate([first, jnp.where(c == 0, theirs, mine)], axis=0)
    per = bias_qv.shape[1]
    up_bias = mine[:, :, 2, : bias_up.shape[0]].astype(F32).reshape(2, hidden)
    rows = every[:, :, 3:9, :per].astype(F32).transpose(2, 1, 0, 3).reshape(6, model_width)
    full_gains, full_shifts = rows[:2], rows[2:]
    source = lax.dynamic_index_in_dim(every[0, :, 9, :4].astype(F32), 2 * k + t // 2, 0, False)
    member = t % 2
    high = jnp.where(member == 0, source[0], source[1])
    low_part = jnp.where(member == 0, source[2], source[3])
    prefix = (high * 16 + low_part).astype(jnp.int32)[None]

    branch_part = sum(
        jnp.einsum(
            "rk,dk->rd", context[:, z * part : (z + 1) * part], g_out[z], preferred_element_type=F32
        )
        for z in range(2)
    ).astype(BF)
    branch = (
        branch_part.astype(F32) + pair_swap(branch_part).astype(F32) + full_shifts[0]
    )
    normed, normal_one, inverse_one = norm_forward(
        x.astype(F32) + branch, full_gains[0], full_shifts[1]
    )
    normed_low = normed.astype(BF)
    pre = [
        jnp.dot(normed_low, g_up[z], preferred_element_type=F32) + up_bias[z] for z in range(2)
    ]
    active = [jax.nn.gelu(v, approximate=False).astype(BF) for v in pre]
    feed_part = sum(
        jnp.einsum("rf,df->rd", active[z], g_down[z], preferred_element_type=F32)
        for z in range(2)
    ).astype(BF)
    feed_out = feed_part.astype(F32) + pair_swap(feed_part).astype(F32) + full_shifts[2]
    result, normal_two, inverse_two = norm_forward(
        normed + feed_out, full_gains[1], full_shifts[3]
    )
    incoming = cot.astype(F32)
    residual_two, gain_two, shift_two = norm_backward(
        incoming, normal_two, inverse_two, full_gains[1]
    )
    feed_grad = residual_two.astype(BF)
    upper = []
    for z in range(2):
        active_grad = jnp.dot(feed_grad, g_down[z], preferred_element_type=F32)
        _, pull = jax.vjp(partial(jax.nn.gelu, approximate=False), pre[z])
        upper.append(pull(active_grad)[0].astype(BF))
    normed_part = sum(
        jnp.einsum("rf,df->rd", upper[z], g_up[z], preferred_element_type=F32) for z in range(2)
    ).astype(BF)
    normed_grad = residual_two + (
        normed_part.astype(F32) + pair_swap(normed_part).astype(F32)
    )
    residual_one, gain_one, shift_one = norm_backward(
        normed_grad, normal_one, inverse_one, full_gains[0]
    )
    branch_grad = residual_one.astype(BF)
    context_grad = jnp.concatenate(
        [jnp.dot(branch_grad, g_out[z], preferred_element_type=F32) for z in range(2)], axis=1
    ).astype(BF)
    mixed = attend_back(queries, key_heads, value_heads, prefix, totals, context, context_grad)
    mixed_low = [
        jnp.concatenate([m[:, z * part : (z + 1) * part] for m in mixed], axis=1)
        for z in range(2)
    ]
    token_part = sum(
        jnp.einsum("re,de->rd", mixed_low[z], g_qkv[z], preferred_element_type=F32)
        for z in range(2)
    ).astype(BF)
    token_grad = residual_one + (token_part.astype(F32) + pair_swap(token_part).astype(F32))

    def outer(a, b):
        return jnp.einsum("rm,rn->mn", a, b, preferred_element_type=F32).astype(BF)

    grads = (
        jnp.stack([outer(x, mixed_low[z]) for z in range(2)]),
        jnp.stack(
            [outer(branch_grad, context[:, z * part : (z + 1) * part]) for z in range(2)]
        ),
        jnp.stack([outer(normed_low, upper[z]) for z in range(2)]),
        jnp.stack([outer(feed_grad, active[z]) for z in range(2)]),
    )
    up_bias_grad = jnp.stack([jnp.sum(v.astype(F32), axis=0) for v in upper])
    bias_grad = jnp.stack(
        [jnp.sum(m.astype(F32), axis=0) for m in (mixed[0], mixed[2])]
    )
    row_grads = jnp.stack(
        [
            gain_one,
            gain_two,
            jnp.sum(branch_grad.astype(F32), axis=0),
            shift_one,
            jnp.sum(feed_grad.astype(F32), axis=0),
            shift_two,
        ]
    )
    spread_bias = bias_grad.reshape(2, 2, 8, per).transpose(1, 2, 0, 3)
    spread_rows = row_grads.reshape(6, 8, 4, per).transpose(2, 1, 0, 3)
    spread_rows = lax.dynamic_slice_in_dim(spread_rows, 2 * c, 2, 0)
    spread_up = up_bias_grad.reshape(2, 8, 1, bias_up.shape[0])

    def wide(v):
        return jnp.pad(v, ((0, 0), (0, 0), (0, 0), (0, 128 - v.shape[3])))

    tiles = jnp.concatenate(
        [wide(spread_bias), wide(spread_up), wide(spread_rows[:, :, :2].reshape(2, 8, 1, 2 * per)),
         wide(spread_rows[:, :, 2:].reshape(2, 8, 1, 4 * per)),
         jnp.zeros((2, 8, 3, 128), F32)],
        axis=2,
    ).reshape(2, 64, 128)
    back_chunks = (
        (3, 0, half),
        (3, half, half),
        (2, 0, half),
        (2, half, half),
        (1, 0, part),
        (0, 0, 3 * part),
        (4, 0, 128),
    )
    out_rows, token_rows, finals = reduce_all(
        result.astype(BF), token_grad.astype(BF), (*grads, tiles), back_chunks
    )
    tile = finals[4]
    return (
        out_rows,
        token_rows.astype(F32),
        finals[0].reshape(w_qkv.shape),
        tile[0:2, :per],
        finals[1].T,
        finals[2],
        tile[2, : bias_up.shape[0]],
        finals[3].T,
        tile[3, : 2 * per].reshape(2, per),
        tile[4, : 4 * per].reshape(4, per),
    )


def solution(mesh):
    return jax.shard_map(
        chip_local if dict(mesh.shape) == {"dp": 8, "tensor": 4} else local,
        mesh=mesh,
        in_specs=(
            P("dp", "tensor", None),
            P("dp"),
            P("dp", None, "tensor"),
            P(None, ("tensor", "dp")),
            P("tensor", "dp"),
            P("dp", "tensor"),
            P(("tensor", "dp")),
            P("tensor", "dp"),
            P(None, ("dp", "tensor")),
            P(None, ("dp", "tensor")),
            P("dp", "tensor", None),
        ),
        out_specs=(
            P("dp", "tensor", None),
            P("dp", "tensor", None),
            P("dp", None, "tensor"),
            P(None, ("tensor", "dp")),
            P("tensor", "dp"),
            P("dp", "tensor"),
            P(("tensor", "dp")),
            P("tensor", "dp"),
            P(None, ("dp", "tensor")),
            P(None, ("dp", "tensor")),
        ),
        check_vma=False,
    )
```

```python
from functools import partial

import jax
import jax.numpy as jnp
from jax import lax
from jax.experimental import pallas as pl
from jax.experimental.pallas import tpu as pltpu
from jax.sharding import PartitionSpec as P

DH = 64


EPSILON = 1e-05
MASKED_SCORE = -1e30


def norm_forward(values, gain_row, shift_row):
    center = values - jnp.mean(values, axis=-1, keepdims=True)
    inverse = lax.rsqrt(jnp.mean(center * center, axis=-1, keepdims=True) + EPSILON)
    normal = center * inverse
    return (normal * gain_row + shift_row, normal, inverse)


def norm_backward(incoming, normal, inverse, gain_row):
    scaled = incoming * gain_row
    first_mean = jnp.mean(scaled, axis=-1, keepdims=True)
    second_mean = jnp.mean(scaled * normal, axis=-1, keepdims=True)
    outgoing = inverse * (scaled - first_mean - normal * second_mean)
    return (outgoing, jnp.sum(incoming * normal, axis=0), jnp.sum(incoming, axis=0))


def visible_mask(offset, block_rows, length, prefix):
    row_ids = offset + jnp.arange(block_rows, dtype=jnp.int32)[:, None]
    column_ids = jnp.arange(length, dtype=jnp.int32)[None, :]
    return jnp.logical_or(column_ids < prefix, column_ids <= row_ids)


def block_scores(chosen, key_heads, offset, prefix, scaling):
    length = key_heads.shape[0]
    allowed = visible_mask(offset, chosen.shape[0], length, prefix)
    scores = (
        jnp.einsum("qhd,khd->hqk", chosen, key_heads, preferred_element_type=jnp.float32) * scaling
    )
    return jnp.where(allowed[None], scores, MASKED_SCORE)


def attention_forward(queries, key_heads, value_heads, prefix):
    length = key_heads.shape[0]
    block_rows = min(512, length)
    scaling = queries.shape[-1] ** (-0.5)
    outputs = []
    totals = []
    for offset in range(0, length, block_rows):
        scores = block_scores(
            queries[offset : offset + block_rows], key_heads, offset, prefix, scaling
        )
        row_max = jnp.max(scores, axis=-1, keepdims=True)
        log_total = jnp.log(jnp.sum(jnp.exp(scores - row_max), axis=-1, keepdims=True)) + row_max
        attn_probs = jnp.exp(scores - log_total).astype(jnp.bfloat16)
        outputs.append(
            jnp.einsum("hqk,khd->qhd", attn_probs, value_heads, preferred_element_type=jnp.float32)
        )
        totals.append(log_total)
    return (jnp.concatenate(outputs, axis=0), totals)


def attention_backward(queries, key_heads, value_heads, prefix, totals, context_grad):
    length = key_heads.shape[0]
    block_rows = min(512, length)
    scaling = queries.shape[-1] ** (-0.5)
    query_parts = []
    key_grad = jnp.zeros(key_heads.shape, jnp.float32)
    value_grad = jnp.zeros(value_heads.shape, jnp.float32)
    for number, offset in enumerate(range(0, length, block_rows)):
        chosen = queries[offset : offset + block_rows]
        grad_block = context_grad[offset : offset + block_rows]
        scores = block_scores(chosen, key_heads, offset, prefix, scaling)
        attn_probs = jnp.exp(scores - totals[number])
        probs_low = attn_probs.astype(jnp.bfloat16)
        probs_grad = jnp.einsum(
            "qhd,khd->hqk", grad_block, value_heads, preferred_element_type=jnp.float32
        )
        row_dot = jnp.sum(attn_probs * probs_grad, axis=-1, keepdims=True)
        scores_grad = (attn_probs * (probs_grad - row_dot)).astype(jnp.bfloat16)
        query_parts.append(
            jnp.einsum("hqk,khd->qhd", scores_grad, key_heads, preferred_element_type=jnp.float32)
            * scaling
        )
        key_grad = (
            key_grad
            + jnp.einsum("hqk,qhd->khd", scores_grad, chosen, preferred_element_type=jnp.float32)
            * scaling
        )
        value_grad = value_grad + jnp.einsum(
            "hqk,qhd->khd", probs_low, grad_block, preferred_element_type=jnp.float32
        )
    return (jnp.concatenate(query_parts, axis=0), key_grad, value_grad)


def local(
    tokens, prefix_len, w_qkv, bias_qv, w_out, w_up, bias_up, w_down, gains, shifts, cotangent
):
    tensor_count = lax.axis_size("tensor")
    seq_local, shard_rows, model_width = tokens.shape
    length = shard_rows * tensor_count
    full_qkv, full_bias_qv, full_out, full_up, full_bias_up, full_down = (
        lax.all_gather(w_qkv, "dp", axis=0, tiled=True),
        lax.all_gather(bias_qv, "dp", axis=1, tiled=True),
        lax.all_gather(w_out, "dp", axis=1, tiled=True),
        lax.all_gather(w_up, "dp", axis=0, tiled=True),
        lax.all_gather(bias_up, "dp", axis=0, tiled=True),
        lax.all_gather(w_down, "dp", axis=1, tiled=True),
    )
    full_gains, full_shifts = (
        lax.all_gather(gains, ("dp", "tensor"), axis=1, tiled=True),
        lax.all_gather(shifts, ("dp", "tensor"), axis=1, tiled=True),
    )
    full_gains = full_gains.astype(jnp.float32)
    full_shifts = full_shifts.astype(jnp.float32)
    bias_values = full_bias_qv.astype(jnp.float32)
    up_bias = full_bias_up.astype(jnp.float32)
    local_width = full_qkv.shape[2]
    head_count = local_width // DH
    kept_state = []
    outputs = []
    for member in range(seq_local):
        token_rows = tokens[member]
        prefix = prefix_len[member]

        def fold_tokens(piece):
            product = jnp.einsum("rd,dce->rce", piece, full_qkv, preferred_element_type=jnp.float32)
            return (piece, product)

        token_full, projected = fold_tokens(
            lax.all_gather(token_rows, "tensor", axis=0, tiled=True)
        )
        queries = (
            (projected[:, 0] + bias_values[0]).astype(jnp.bfloat16).reshape(length, head_count, DH)
        )
        key_heads = projected[:, 1].astype(jnp.bfloat16).reshape(length, head_count, DH)
        value_heads = (
            (projected[:, 2] + bias_values[1]).astype(jnp.bfloat16).reshape(length, head_count, DH)
        )
        context, totals = attention_forward(queries, key_heads, value_heads, prefix)
        context_low = context.reshape(length, local_width).astype(jnp.bfloat16)
        branch = (
            lax.psum_scatter(
                jnp.dot(context_low, full_out, preferred_element_type=jnp.float32).astype(
                    jnp.bfloat16
                ),
                "tensor",
                scatter_dimension=0,
                tiled=True,
            ).astype(jnp.float32)
            + full_shifts[0]
        )
        normed, normal_one, inverse_one = norm_forward(
            token_rows.astype(jnp.float32) + branch, full_gains[0], full_shifts[1]
        )
        normed_low = normed.astype(jnp.bfloat16)

        def fold_normed(piece):
            product = jnp.dot(piece, full_up, preferred_element_type=jnp.float32)
            return (piece, product)

        normed_full, pre_active = fold_normed(
            lax.all_gather(normed_low, "tensor", axis=0, tiled=True)
        )
        pre_active = pre_active + up_bias
        active_low = jax.nn.gelu(pre_active, approximate=False).astype(jnp.bfloat16)
        feed_out = (
            lax.psum_scatter(
                jnp.dot(active_low, full_down, preferred_element_type=jnp.float32).astype(
                    jnp.bfloat16
                ),
                "tensor",
                scatter_dimension=0,
                tiled=True,
            ).astype(jnp.float32)
            + full_shifts[2]
        )
        result, normal_two, inverse_two = norm_forward(
            normed + feed_out, full_gains[1], full_shifts[3]
        )
        outputs.append(result.astype(jnp.bfloat16))
        kept_state.append(
            (
                token_rows,
                prefix,
                token_full,
                queries,
                key_heads,
                value_heads,
                totals,
                context_low,
                normal_one,
                inverse_one,
                normed_full,
                pre_active,
                active_low,
                normal_two,
                inverse_two,
            )
        )
    back_qkv, back_out, back_up, back_down = (
        lax.all_gather(w_qkv, "dp", axis=0, tiled=True),
        lax.all_gather(w_out, "dp", axis=1, tiled=True),
        lax.all_gather(w_up, "dp", axis=0, tiled=True),
        lax.all_gather(w_down, "dp", axis=1, tiled=True),
    )
    full_shapes = (
        full_qkv.shape,
        full_bias_qv.shape,
        full_out.shape,
        full_up.shape,
        full_bias_up.shape,
        full_down.shape,
    )
    weight_grads = tuple((jnp.zeros(array_shape, jnp.float32) for array_shape in full_shapes))
    gain_grads = jnp.zeros((2, model_width), jnp.float32)
    shift_grads = jnp.zeros((4, model_width), jnp.float32)
    input_grads = []
    for member in range(seq_local):
        (
            token_rows,
            prefix,
            token_full,
            queries,
            key_heads,
            value_heads,
            totals,
            context_low,
            normal_one,
            inverse_one,
            normed_full,
            pre_active,
            active_low,
            normal_two,
            inverse_two,
        ) = kept_state[member]
        incoming = cotangent[member].astype(jnp.float32)
        residual_two, gain_two, shift_two = norm_backward(
            incoming, normal_two, inverse_two, full_gains[1]
        )
        feed_grad = residual_two.astype(jnp.bfloat16)
        fold_piece = lax.all_gather(feed_grad, "tensor", axis=0, tiled=True)
        down_grad = jnp.einsum(
            "rf,rd->fd", active_low, fold_piece, preferred_element_type=jnp.float32
        )
        fold_product = jnp.einsum(
            "rd,fd->rf", fold_piece, back_down, preferred_element_type=jnp.float32
        )
        active_grad = fold_product
        down_grad, active_grad = (down_grad, active_grad)
        layer_value, gelu_pull = jax.vjp(partial(jax.nn.gelu, approximate=False), pre_active)
        upper_grad = gelu_pull(active_grad)[0].astype(jnp.bfloat16)
        normed_grad = residual_two + lax.psum_scatter(
            jnp.einsum("rf,df->rd", upper_grad, back_up, preferred_element_type=jnp.float32).astype(
                jnp.bfloat16
            ),
            "tensor",
            scatter_dimension=0,
            tiled=True,
        ).astype(jnp.float32)
        up_grad = jnp.einsum(
            "ld,lf->df", normed_full, upper_grad, preferred_element_type=jnp.float32
        )
        up_bias_grad = jnp.sum(upper_grad.astype(jnp.float32), axis=0)
        residual_one, gain_one, shift_one = norm_backward(
            normed_grad, normal_one, inverse_one, full_gains[0]
        )
        branch_grad = residual_one.astype(jnp.bfloat16)

        def fold_branch(piece):
            out_grad = jnp.einsum(
                "rk,rd->kd", context_low, piece, preferred_element_type=jnp.float32
            )
            product = jnp.einsum("rd,kd->rk", piece, back_out, preferred_element_type=jnp.float32)
            return (out_grad, product)

        out_grad, context_grad = fold_branch(
            lax.all_gather(branch_grad, "tensor", axis=0, tiled=True)
        )
        context_grad = context_grad.astype(jnp.bfloat16).reshape(length, head_count, DH)
        query_grad, key_grad, value_grad = attention_backward(
            queries, key_heads, value_heads, prefix, totals, context_grad
        )
        mixed_grad = (
            jnp.stack([query_grad, key_grad, value_grad], axis=1)
            .astype(jnp.bfloat16)
            .reshape(length, 3, local_width)
        )
        qkv_grad = jnp.einsum(
            "ld,lce->dce", token_full, mixed_grad, preferred_element_type=jnp.float32
        )
        row_sums = jnp.sum(mixed_grad.astype(jnp.float32), axis=0)
        bias_grad = jnp.stack([row_sums[0], row_sums[2]])
        token_grad = residual_one + lax.psum_scatter(
            jnp.einsum(
                "rce,dce->rd", mixed_grad, back_qkv, preferred_element_type=jnp.float32
            ).astype(jnp.bfloat16),
            "tensor",
            scatter_dimension=0,
            tiled=True,
        ).astype(jnp.float32)
        input_grads.append(token_grad)
        gain_grads = gain_grads + jnp.stack([gain_one, gain_two])
        shift_grads = shift_grads + jnp.stack(
            [
                jnp.sum(branch_grad.astype(jnp.float32), axis=0),
                shift_one,
                jnp.sum(feed_grad.astype(jnp.float32), axis=0),
                shift_two,
            ]
        )
        member_grads = (qkv_grad, bias_grad, out_grad, up_grad, up_bias_grad, down_grad)
        weight_grads = tuple(
            (running + grad_part for running, grad_part in zip(weight_grads, member_grads))
        )
    total_qkv, total_bias, total_out, total_up, total_up_bias, total_down = weight_grads
    weight_grads = (
        lax.psum_scatter(total_qkv, "dp", scatter_dimension=0, tiled=True),
        lax.psum_scatter(total_bias, "dp", scatter_dimension=1, tiled=True),
        lax.psum_scatter(total_out, "dp", scatter_dimension=1, tiled=True),
        lax.psum_scatter(total_up, "dp", scatter_dimension=0, tiled=True),
        lax.psum_scatter(total_up_bias, "dp", scatter_dimension=0, tiled=True),
        lax.psum_scatter(total_down, "dp", scatter_dimension=1, tiled=True),
    )
    gain_share, shift_share = (
        lax.psum_scatter(gain_grads, ("dp", "tensor"), scatter_dimension=1, tiled=True),
        lax.psum_scatter(shift_grads, ("dp", "tensor"), scatter_dimension=1, tiled=True),
    )
    return (
        jnp.stack(outputs),
        jnp.stack(input_grads),
        weight_grads[0],
        weight_grads[1],
        weight_grads[2],
        weight_grads[3],
        weight_grads[4],
        weight_grads[5],
        gain_share,
        shift_share,
    )


MESH_ID = pl.DeviceIdType.MESH
BF = jnp.bfloat16
F32 = jnp.float32
ROWS = 96
SMALL = 16


def place():
    d = lax.axis_index("dp")
    t = lax.axis_index("tensor")
    k, c = d // 2, d % 2
    xb, yb = k % 2, k // 2
    dx = d + 2 - 4 * xb
    dy = d + 4 - 8 * yb
    return d, t, k, c, xb, yb, dx, dy


def remote(src, dst, send, recv, dp, tensor):
    return pltpu.make_async_remote_copy(
        src_ref=src,
        dst_ref=dst,
        send_sem=send,
        recv_sem=recv,
        device_id=(dp, tensor),
        device_id_type=MESH_ID,
    )


def enter(k, c, t, d, dx, dy):
    barrier = pltpu.get_barrier_semaphore()

    def greet(dp, tensor):
        pl.semaphore_signal(barrier, inc=1, device_id=(dp, tensor), device_id_type=MESH_ID)

    greet(dx, t)
    greet(dy, t)
    greet(d + 1 - 2 * c, t)
    for step in range(1, 4):
        other = (t + step) % 4
        greet(2 * k, other)
        greet(2 * k + 1, other)
    pl.semaphore_wait(barrier, 9)


def pair_swap(part):
    def kernel(src, dst, send, recv):
        d, t, k, c, xb, yb, dx, dy = place()
        mate = d + 1 - 2 * c
        barrier = pltpu.get_barrier_semaphore()
        pl.semaphore_signal(barrier, inc=1, device_id=(mate, t), device_id_type=MESH_ID)
        pl.semaphore_wait(barrier, 1)
        rows = src.shape[0] // 4
        copies = [
            remote(
                src.at[pl.ds(i * rows, rows)],
                dst.at[pl.ds(i * rows, rows)],
                send.at[i],
                recv.at[i],
                mate,
                t,
            )
            for i in range(4)
        ]
        for copy in copies:
            copy.start()
        for copy in copies:
            copy.wait()

    return pl.pallas_call(
        kernel,
        out_shape=jax.ShapeDtypeStruct(part.shape, part.dtype),
        in_specs=[pl.BlockSpec(memory_space=pl.ANY)],
        out_specs=pl.BlockSpec(memory_space=pl.ANY),
        scratch_shapes=[pltpu.SemaphoreType.DMA((4,)), pltpu.SemaphoreType.DMA((4,))],
        compiler_params=pltpu.CompilerParams(collective_id=3, has_side_effects=True),
    )(part)


def skewed(chunks, levels):
    for slot in range(chunks + len(levels) - 1):
        for level in reversed(range(len(levels))):
            if 0 <= slot - level < chunks:
                levels[level](slot - level)


def gather_attend(tokens, cotangent, shards, chunks, per):
    half = tokens.shape[1] // 2
    width = tokens.shape[2]
    count = len(shards)
    n_chunks = len(chunks)
    rows_of = [s.shape[0] for s in shards]
    length = tokens.shape[1] * 4
    part = shards[0].shape[1] // 3
    heads_width = 2 * part
    blocks = length // BLOCK

    def kernel(*refs):
        tok, cot = refs[0], refs[1]
        own = refs[2 : 2 + count]
        base = 2 + count
        xf, cf = refs[base], refs[base + 1]
        full = refs[base + 2 : base + 2 + count]
        small_other, q_out, k_out, v_out, o_out, lt_out, limit_out = refs[
            base + 2 + count : base + 9 + count
        ]
        stage = refs[base + 9 + count : base + 9 + 2 * count]
        (
            x_rows,
            weight,
            small_low,
            small_rows,
            load_sem,
            row_stage,
            local_sem,
            row_sem,
            ex_send,
            ex_recv,
            fw_send,
            fw_recv,
            p_send,
            p_recv,
            z_send,
            z_recv,
            a_send,
            a_recv,
            b_send,
            b_recv,
            o_send,
            o_recv,
        ) = refs[base + 9 + 2 * count :]
        d, t, k, c, xb, yb, dx, dy = place()
        mate = d + 1 - 2 * c
        u = t + c * (3 - 2 * t)
        up = t + 1 - 2 * c
        down = t - 1 + 2 * c
        source = t // 2 == c
        enter(k, c, t, d, dx, dy)

        for s in range(count):
            rows = rows_of[s]
            spot = full[s].at[t % 2, pl.ds(d * rows, rows)]

            @pl.when(source)
            def _():
                pltpu.make_async_copy(own[s], stage[s], local_sem.at[s]).start()

            @pl.when(jnp.logical_not(source))
            def _():
                remote(own[s], spot, p_send.at[s], p_recv.at[s], mate, t).start()

        def exchange(which, src, dst):
            for m in range(2):
                goal = 2 * c + m
                for core in range(2):
                    piece = src.at[m, pl.ds(core * half, half)]
                    spot = dst.at[t * 2 + core]
                    here = jnp.logical_and(goal == t, core == c)

                    @pl.when(here)
                    def _():
                        load = pltpu.make_async_copy(piece, row_stage, row_sem)
                        load.start()
                        load.wait()
                        store = pltpu.make_async_copy(row_stage, spot, row_sem)
                        store.start()
                        store.wait()

                    @pl.when(jnp.logical_not(here))
                    def _():
                        remote(
                            piece,
                            spot,
                            ex_send.at[which, 2 * m + core],
                            ex_recv.at[which, t],
                            2 * k + core,
                            goal,
                        ).start()

        def relay(which, dst):
            for origin in range(4):
                spot = dst.at[origin * 2 + c]
                local = jnp.logical_and(origin == t, c == t // 2)

                @pl.when(jnp.logical_not(local))
                def _():
                    remote(
                        spot, spot, ex_send.at[which, 0], ex_recv.at[which, origin], mate, t
                    ).wait_recv()

                remote(
                    spot, spot, fw_send.at[which, origin], fw_recv.at[which, origin], mate, t
                ).start()

        def arrived(which, dst):
            for origin in range(4):
                spot = dst.at[origin * 2 + 1 - c]
                remote(
                    spot, spot, fw_send.at[which, origin], fw_recv.at[which, origin], mate, t
                ).wait_recv()

        def settle(which, src, dst):
            for origin in range(4):
                spot = dst.at[origin * 2 + 1 - c]
                remote(
                    spot, spot, fw_send.at[which, origin], fw_recv.at[which, origin], mate, t
                ).wait_send()
            for m in range(2):
                for core in range(2):
                    here = jnp.logical_and(2 * c + m == t, core == c)

                    @pl.when(jnp.logical_not(here))
                    def _():
                        remote(
                            src.at[m, pl.ds(core * half, half)],
                            dst.at[t * 2 + core],
                            ex_send.at[which, 2 * m + core],
                            ex_recv.at[which, t],
                            mate,
                            t,
                        ).wait_send()

        def placed(s):
            @pl.when(source)
            def _():
                rows = rows_of[s]
                spot = full[s].at[t % 2, pl.ds(d * rows, rows)]
                pltpu.make_async_copy(own[s], stage[s], local_sem.at[s]).wait()
                pltpu.make_async_copy(stage[s], spot, local_sem.at[s]).start()

        def block(i, b, start, n):
            s, col, cols = chunks[i]
            zz = b + c * (1 - 2 * b)
            rows = rows_of[s]
            return full[s].at[zz, pl.ds(start * rows, n * rows), pl.ds(col, cols)]

        def z_copy(i, b, way, target):
            ref = block(i, b, 2 * k, 2)
            return remote(ref, ref, z_send.at[i, b, way], z_recv.at[i, b], d, target)

        def first_copy(i, b):
            ref = block(i, b, 2 * k, 2)
            return remote(ref, ref, a_send.at[i, b], a_recv.at[i, b], dx if b == 0 else dy, t)

        def first_arrival(i, b):
            near = k + 1 - 2 * xb if b == 0 else k + 2 - 4 * yb
            ref = block(i, b, 2 * near, 2)
            return remote(ref, ref, a_send.at[i, b], a_recv.at[i, b], dx if b == 0 else dy, t)

        def second_copies(i, arriving):
            other = 1 if arriving else 0
            row = yb + other * (1 - 2 * yb)
            ref = block(i, 0, 4 * row, 4)
            col = xb + other * (1 - 2 * xb)
            out = [remote(ref, ref, b_send.at[i, 0], b_recv.at[i, 0], dy, t)]
            for r in range(2):
                ref = block(i, 1, 2 * (2 * r + col), 2)
                out.append(remote(ref, ref, b_send.at[i, 1 + r], b_recv.at[i, 1 + r], dx, t))
            return out

        def spread(i, b):
            @pl.when(jnp.logical_and(u >= b, u < 3))
            def _():
                z_copy(i, b, 0, up).start()

            if b == 1:

                @pl.when(u == 1)
                def _():
                    z_copy(i, 1, 1, down).start()

            first_copy(i, b).start()

        waited = set()

        def own_ready(i):
            s = chunks[i][0]
            if s in waited:
                return
            waited.add(s)
            rows = rows_of[s]
            spot = full[s].at[t % 2, pl.ds(d * rows, rows)]
            twin = full[s].at[t % 2, pl.ds(mate * rows, rows)]
            pltpu.make_async_copy(stage[s], spot, local_sem.at[s]).wait()
            remote(twin, twin, p_send.at[s], p_recv.at[s], mate, t).wait_recv()

        def level_own(i):
            if chunks[i][0] not in waited:

                @pl.when(source)
                def _():
                    own_ready(i)

            for b in range(2):

                @pl.when(u == b)
                def _():
                    spread(i, b)

        def level_line(i):
            for b in (1, 0):

                @pl.when(u != b)
                def _():
                    z_copy(i, b, 0, up).wait_recv()
                    spread(i, b)

        def level_second(i):
            for b in range(2):
                first_arrival(i, b).wait_recv()
            for copy in second_copies(i, False):
                copy.start()

        def level_done(i):
            for copy in second_copies(i, True):
                copy.wait_recv()

        def expand(plane, kind):
            rows = small_rows[plane, pl.ds(kind, 8, stride=SMALL), :]
            spots = lax.broadcasted_iota(jnp.int32, (128, part), 0)
            lane = lax.broadcasted_iota(jnp.int32, (128, part), 1)
            wide = jnp.dot(
                rows,
                (spots == lane % per).astype(F32),
                precision=lax.Precision.HIGHEST,
                preferred_element_type=F32,
            )
            row = lax.broadcasted_iota(jnp.int32, (8, part), 0)
            lane = lax.broadcasted_iota(jnp.int32, (8, part), 1)
            return jnp.sum(jnp.where(lane // per == row, wide, 0.0), axis=0, keepdims=True)

        def prefix_of():
            tile = small_rows[0, pl.ds((2 * k + t // 2) * SMALL + 9, 1), 0:128]
            lane = lax.broadcasted_iota(jnp.int32, (1, 128), 1)
            member = t % 2
            value = 16.0 * jnp.sum(jnp.where(lane == member, tile, 0.0), axis=1, keepdims=True)
            value += jnp.sum(jnp.where(lane == 2 + member, tile, 0.0), axis=1, keepdims=True)
            return value

        def project():
            bias_q = jnp.concatenate([expand(0, 0), expand(1, 0)], axis=1)
            bias_v = jnp.concatenate([expand(0, 1), expand(1, 1)], axis=1)

            @pl.loop(0, blocks)
            def _(block_id):
                rows = pl.ds(block_id * BLOCK, BLOCK)
                both = [
                    jnp.dot(x_rows[rows, :], weight[z], preferred_element_type=F32)
                    for z in range(2)
                ]

                def kind(i):
                    return jnp.concatenate([v[:, i * part : (i + 1) * part] for v in both], axis=1)

                q_out[rows, :] = (kind(0) + bias_q).astype(BF)
                k_out[rows, :] = kind(1).astype(BF)
                v_out[rows, :] = (kind(2) + bias_v).astype(BF)

        load_rows = [
            pltpu.make_async_copy(xf.at[i], x_rows.at[pl.ds(i * half, half)], load_sem.at[i])
            for i in range(8)
        ]
        load_weight = pltpu.make_async_copy(full[0], weight, load_sem.at[8])
        last = count - 1
        swap = remote(full[last], small_other, o_send, o_recv, mate, t)

        placed(last)
        placed(0)
        level_own(0)
        level_own(1)
        exchange(0, tok, xf)
        for s in range(1, last):
            placed(s)
        level_line(0)
        level_line(1)
        level_second(0)
        level_own(2)
        level_own(3)
        level_second(1)
        relay(0, xf)
        level_line(2)
        level_own(4)
        level_done(0)
        swap.start()
        small_load = pltpu.make_async_copy(full[last], small_low, load_sem.at[9])
        small_load.start()
        arrived(0, xf)
        for copy in load_rows:
            copy.start()
        level_line(3)
        level_second(2)
        for i in range(5, n_chunks):
            level_own(i)
        small_load.wait()
        small_rows[...] = small_low[...].astype(F32)
        level_done(1)
        load_weight.start()
        level_second(3)
        exchange(1, cot, cf)
        for copy in load_rows:
            copy.wait()
        load_weight.wait()
        limit_out[...] = jnp.broadcast_to(prefix_of(), limit_out.shape)
        project()
        todo = []
        for i in range(4, n_chunks):
            todo.append(partial(level_line, i))
            todo.append(partial(level_second, i))
        todo.append(lambda: relay(1, cf))
        work = [
            partial(attend_rows, q_out, k_out, v_out, o_out, lt_out, prefix_of(), pair, qb)
            for pair in range(heads_width // 128)
            for qb in range(blocks)
        ]
        for step in range(max(len(todo), len(work))):
            if step < len(todo):
                todo[step]()
            if step < len(work):
                work[step]()
        for i in range(2, n_chunks):
            level_done(i)
        arrived(1, cf)
        settle(0, tok, xf)
        settle(1, cot, cf)
        for s in range(count):
            rows = rows_of[s]
            spot = full[s].at[t % 2, pl.ds(d * rows, rows)]

            @pl.when(jnp.logical_not(source))
            def _():
                remote(own[s], spot, p_send.at[s], p_recv.at[s], mate, t).wait_send()

        for i in range(n_chunks):
            for b in range(2):

                @pl.when(jnp.logical_and(u >= b, u < 3))
                def _():
                    z_copy(i, b, 0, up).wait_send()

                first_copy(i, b).wait_send()

            @pl.when(u == 1)
            def _():
                z_copy(i, 1, 1, down).wait_send()

            for copy in second_copies(i, False):
                copy.wait_send()
        swap.wait()

    any_spec = pl.BlockSpec(memory_space=pl.ANY)
    vmem = pl.BlockSpec(memory_space=pltpu.VMEM)
    dma = pltpu.SemaphoreType.DMA
    full_shapes = [jax.ShapeDtypeStruct((2, 8 * s.shape[0], s.shape[1]), s.dtype) for s in shards]
    rows_shape = jax.ShapeDtypeStruct((8, half, width), tokens.dtype)
    head_shape = jax.ShapeDtypeStruct((length, heads_width), BF)
    lt_shape = jax.ShapeDtypeStruct((heads_width // DH, 8, length), F32)
    outs = pl.pallas_call(
        kernel,
        out_shape=[
            rows_shape,
            rows_shape,
            *full_shapes,
            full_shapes[-1],
            *[head_shape] * 4,
            lt_shape,
            jax.ShapeDtypeStruct((8, 128), F32),
        ],
        in_specs=[any_spec] * (2 + count),
        out_specs=[any_spec] * (3 + count) + [vmem] * 6,
        scratch_shapes=[
            *[pltpu.VMEM(s.shape, s.dtype) for s in shards],
            pltpu.VMEM((length, width), BF),
            pltpu.VMEM((2, 8 * shards[0].shape[0], shards[0].shape[1]), BF),
            pltpu.VMEM((2, 8 * SMALL, 128), BF),
            pltpu.VMEM((2, 8 * SMALL, 128), F32),
            dma((10,)),
            pltpu.VMEM((half, width), tokens.dtype),
            dma((count,)),
            dma,
            dma((2, 4)),
            dma((2, 4)),
            dma((2, 4)),
            dma((2, 4)),
            dma((count,)),
            dma((count,)),
            dma((n_chunks, 2, 2)),
            dma((n_chunks, 2)),
            dma((n_chunks, 2)),
            dma((n_chunks, 2)),
            dma((n_chunks, 3)),
            dma((n_chunks, 3)),
            dma,
            dma,
        ],
        compiler_params=pltpu.CompilerParams(
            collective_id=1, has_side_effects=True, vmem_limit_bytes=60 * 1024 * 1024
        ),
    )(tokens, cotangent, *shards)
    return (
        outs[0].reshape(length, width),
        outs[1].reshape(length, width),
        outs[2 : 2 + count],
        outs[2 + count],
        outs[3 + count :],
    )


def back_reduce(output, residual, x, weight, heads, totals, limit, ready, tile, chunks):
    part_cols = weight.shape[2] // 3
    heads_width = 2 * part_cols
    grads = [jax.ShapeDtypeStruct(weight.shape, BF), *ready]
    count = len(grads)
    n_chunks = len(chunks)
    length, width = output.shape
    half = length // 8
    blocks = length // BLOCK
    rows_of = [g.shape[1] // 8 for g in grads]

    def kernel(*refs):
        res, residual_hbm, x_hbm, weight_hbm = refs[:4]
        q_ref, k_ref, v_ref, o_ref, do_ref, lt_ref, limit_ref, tile_ref = refs[4:12]
        others = refs[12 : 11 + count]
        base = 11 + count
        res_out, tgr_out, tile_own, tile_mate = refs[base : base + 4]
        final = refs[base + 4 : base + 4 + count]
        base += 4 + count
        got1 = refs[base : base + count]
        sum1 = refs[base + count : base + 2 * count]
        got2 = refs[base + 2 * count : base + 3 * count]
        sum2 = refs[base + 3 * count : base + 4 * count]
        got3 = refs[base + 4 * count : base + 5 * count]
        sum3 = refs[base + 5 * count : base + 6 * count]
        got4 = refs[base + 6 * count : base + 7 * count]
        got5 = refs[base + 7 * count : base + 8 * count]
        (
            row_stage,
            row_sem,
            ex_send,
            ex_recv,
            a_send,
            a_recv,
            b_send,
            b_recv,
            z_send,
            z_recv,
            y_send,
            y_recv,
            p_send,
            p_recv,
            grad_own,
            x_rows,
            weight_rows,
            residual_rows,
            dots,
            acc,
            acc_rows,
            dq,
            dk,
            dv,
            mixed,
            mate_part,
            mate_got,
            own_part,
            row_out,
            load_sem,
            s_send,
            s_recv,
            t_send,
            t_recv,
            tile_sum,
            tile_got,
        ) = refs[base + 8 * count :]
        part = (grad_own, *others)
        d, t, k, c, xb, yb, dx, dy = place()
        mate = d + 1 - 2 * c
        u = t + c * (3 - 2 * t)
        up = t + 1 - 2 * c
        down = t - 1 + 2 * c
        source = u <= 1
        enter(k, c, t, d, dx, dy)

        def return_rows(which, src, dst, start):
            for goal in range(4):
                piece = src.at[pl.ds((goal * 2 + c) * half, half)]
                spot = dst.at[t % 2, pl.ds(c * half, half)]
                here = jnp.logical_and(goal == t, c == t // 2)
                copy = remote(
                    piece,
                    spot,
                    ex_send.at[which, goal],
                    ex_recv.at[which, t % 2, c],
                    2 * k + t // 2,
                    goal,
                )

                @pl.when(here)
                def _():
                    if start:
                        load = pltpu.make_async_copy(piece, row_stage, row_sem)
                        load.start()
                        load.wait()
                        store = pltpu.make_async_copy(row_stage, spot, row_sem)
                        store.start()
                        store.wait()

                @pl.when(jnp.logical_not(here))
                def _():
                    if start:
                        copy.start()
                    else:
                        copy.wait_send()

            if not start:
                for m in range(2):
                    for core in range(2):
                        spot = dst.at[m, pl.ds(core * half, half)]
                        here = jnp.logical_and(2 * c + m == t, core == c)

                        @pl.when(jnp.logical_not(here))
                        def _():
                            remote(
                                spot,
                                spot,
                                ex_send.at[which, 0],
                                ex_recv.at[which, m, core],
                                mate,
                                t,
                            ).wait_recv()

        def plane(b):
            return b + c * (1 - 2 * b)

        def first_copies(i):
            s, col, cols = chunks[i]
            rows = rows_of[s]
            spot = pl.ds(col, cols)
            out = [
                remote(
                    part[s].at[plane(0), pl.ds((1 - yb) * 4 * rows, 4 * rows), spot],
                    got1[s].at[0, :, spot],
                    a_send.at[i, 0],
                    a_recv.at[i, 0],
                    dy,
                    t,
                )
            ]
            for r in range(2):
                out.append(
                    remote(
                        part[s].at[plane(1), pl.ds((2 * r + 1 - xb) * 2 * rows, 2 * rows), spot],
                        got1[s].at[1, pl.ds(r * 2 * rows, 2 * rows), spot],
                        a_send.at[i, 1 + r],
                        a_recv.at[i, 1 + r],
                        dx,
                        t,
                    )
                )
            return out

        def second_copies(i):
            s, col, cols = chunks[i]
            rows = rows_of[s]
            spot = pl.ds(col, cols)
            out = []
            for b, far, goal in ((0, 1 - xb, dx), (1, 1 - yb, dy)):
                out.append(
                    remote(
                        sum1[s].at[b, pl.ds(far * 2 * rows, 2 * rows), spot],
                        got2[s].at[b, :, spot],
                        b_send.at[i, b],
                        b_recv.at[i, b],
                        goal,
                        t,
                    )
                )
            return out

        def low(v, s):
            return v.astype(sum1[s].dtype)

        def level_first(i):
            for copy in first_copies(i):
                copy.start()

        def level_second(i):
            s, col, cols = chunks[i]
            rows = rows_of[s]
            spot = pl.ds(col, cols)
            for copy in first_copies(i):
                copy.wait_recv()
            mine = part[s][plane(0), pl.ds(yb * 4 * rows, 4 * rows), spot]
            sum1[s][0, :, spot] = low(mine.astype(F32) + got1[s][0, :, spot].astype(F32), s)
            for r in range(2):
                mine = part[s][plane(1), pl.ds((2 * r + xb) * 2 * rows, 2 * rows), spot]
                there = pl.ds(r * 2 * rows, 2 * rows)
                sum1[s][1, there, spot] = low(
                    mine.astype(F32) + got1[s][1, there, spot].astype(F32), s
                )
            for copy in second_copies(i):
                copy.start()

        def z_copy(i, b):
            s, col, cols = chunks[i]
            spot = pl.ds(col, cols)
            return remote(
                sum3[s].at[b, :, spot],
                got3[s].at[b, :, spot],
                z_send.at[i, b],
                z_recv.at[i, b],
                d,
                down,
            )

        def y_copy(i):
            s, col, cols = chunks[i]
            spot = pl.ds(col, cols)
            return remote(
                sum3[s].at[1, :, spot], got4[s].at[:, spot], y_send.at[i], y_recv.at[i], d, up
            )

        def level_line(i):
            s, col, cols = chunks[i]
            rows = rows_of[s]
            spot = pl.ds(col, cols)
            for copy in second_copies(i):
                copy.wait_recv()
            for b, near in ((0, xb), (1, yb)):
                mine = sum1[s][b, pl.ds(near * 2 * rows, 2 * rows), spot]
                sum2[s][b, :, spot] = mine.astype(F32) + got2[s][b, :, spot].astype(F32)

            @pl.when(u == 3)
            def _():
                for b in range(2):
                    sum3[s][b, :, spot] = low(sum2[s][b, :, spot], s)
                    z_copy(i, b).start()

            @pl.when(u == 0)
            def _():
                sum3[s][1, :, spot] = low(sum2[s][1, :, spot], s)
                y_copy(i).start()

        def level_pass(i):
            s, col, cols = chunks[i]
            spot = pl.ds(col, cols)

            @pl.when(u == 2)
            def _():
                for b in range(2):
                    z_copy(i, b).wait_recv()
                    sum3[s][b, :, spot] = low(
                        sum2[s][b, :, spot] + got3[s][b, :, spot].astype(F32), s
                    )
                    z_copy(i, b).start()

        def level_near(i):
            s, col, cols = chunks[i]
            spot = pl.ds(col, cols)

            @pl.when(u == 1)
            def _():
                z_copy(i, 0).wait_recv()
                sum3[s][0, :, spot] = low(
                    sum2[s][0, :, spot] + got3[s][0, :, spot].astype(F32), s
                )
                z_copy(i, 0).start()
                z_copy(i, 1).wait_recv()
                y_copy(i).wait_recv()
                total = (
                    sum2[s][1, :, spot]
                    + got3[s][1, :, spot].astype(F32)
                    + got4[s][:, spot].astype(F32)
                )
                finish(i, total)

            @pl.when(u == 0)
            def _():
                z_copy(i, 0).wait_recv()
                finish(i, sum2[s][0, :, spot] + got3[s][0, :, spot].astype(F32))

        def p_copy(i):
            s, col, cols = chunks[i]
            rows = rows_of[s]
            spot = pl.ds(col, cols)
            return remote(
                sum1[s].at[0, pl.ds((1 - c) * rows, rows), spot],
                got5[s].at[:, spot],
                p_send.at[i],
                p_recv.at[i],
                mate,
                t,
            )

        def finish(i, total):
            s, col, cols = chunks[i]
            rows = rows_of[s]
            spot = pl.ds(col, cols)
            for copy in second_copies(i):
                copy.wait_send()
            sum2[s][0, :, spot] = total
            sum1[s][0, pl.ds(0, 2 * rows), spot] = low(total, s)
            p_copy(i).start()
            final[s][:, spot] = sum2[s][0, pl.ds(c * rows, rows), spot]

        def level_mate(i):
            s, col, cols = chunks[i]
            spot = pl.ds(col, cols)

            @pl.when(u >= 2)
            def _():
                p_copy(i).wait_recv()
                final[s][:, spot] = got5[s][:, spot].astype(F32)

        loads = [
            pltpu.make_async_copy(x_hbm, x_rows, load_sem.at[0]),
            pltpu.make_async_copy(weight_hbm, weight_rows, load_sem.at[1]),
            pltpu.make_async_copy(residual_hbm, residual_rows, load_sem.at[2]),
        ]

        def attention(pair, kb):
            if kb == 0:
                back_start(pair, o_ref, do_ref, dots, acc)
            back_block(
                pair, kb, q_ref, k_ref, v_ref, lt_ref, do_ref, dots, acc, dk, dv, limit_ref[0:1, 0:1]
            )
            if kb == blocks - 1:
                dq[:, pl.ds(pair * 128, 128)] = (acc[...] * DH**-0.5).astype(BF)

        def mate_copy(i):
            return remote(mate_part.at[i], mate_got.at[i], t_send.at[0, i], t_recv.at[0, i], mate, t)

        def mix(i):
            rows = pl.ds(i * BLOCK, BLOCK)
            kinds = [ref[rows, :] for ref in (dq, dk, dv)]
            share = jnp.zeros((BLOCK, width), F32)
            for z in range(2):
                both = jnp.concatenate(
                    [v[:, z * part_cols : (z + 1) * part_cols] for v in kinds], axis=1
                )
                mixed[z, rows, :] = both
                share = share + dot_nt(both, weight_rows[z])
            acc_rows[...] = share
            mate_part[i] = acc_rows[pl.ds((1 - c) * half, half), :].astype(BF)
            own_part[i] = (
                acc_rows[pl.ds(c * half, half), :]
                + residual_rows[pl.ds((2 * i + c) * half, half), :]
            )
            mate_copy(i).start()

        def row_copy(i):
            return remote(
                row_out.at[i],
                tgr_out.at[t % 2, pl.ds(c * half, half)],
                t_send.at[1, i],
                t_recv.at[1, 2 * (t % 2) + c],
                2 * k + t // 2,
                i,
            )

        def send_rows(i):
            mate_copy(i).wait_recv()
            row_out[i] = (own_part[i] + mate_got[i].astype(F32)).astype(BF)
            here = jnp.logical_and(i == t, c == t // 2)

            @pl.when(here)
            def _():
                store = pltpu.make_async_copy(
                    row_out.at[i], tgr_out.at[t % 2, pl.ds(c * half, half)], row_sem
                )
                store.start()
                store.wait()

            @pl.when(jnp.logical_not(here))
            def _():
                row_copy(i).start()

        def settle_rows():
            for i in range(4):
                mate_copy(i).wait_send()

                @pl.when(jnp.logical_not(jnp.logical_and(i == t, c == t // 2)))
                def _():
                    row_copy(i).wait_send()

            for m in range(2):
                for core in range(2):
                    spot = tgr_out.at[m, pl.ds(core * half, half)]

                    @pl.when(jnp.logical_not(jnp.logical_and(2 * c + m == t, core == c)))
                    def _():
                        remote(
                            row_out.at[0],
                            spot,
                            t_send.at[1, 0],
                            t_recv.at[1, 2 * m + core],
                            mate,
                            t,
                        ).wait_recv()

        def weight_grad(j):
            rows = pl.ds(j * BLOCK, BLOCK)
            for z in range(2):
                grad_own[z, rows, :] = dot_tn(x_rows[:, rows], mixed[z]).astype(BF)

        def tile_copy(stage, goal_dp, goal_t, slot):
            return remote(
                tile_sum.at[stage],
                tile_got.at[slot],
                s_send.at[slot],
                s_recv.at[slot],
                goal_dp,
                goal_t,
            )

        def tile_start():
            tile_sum[0] = tile_ref[...]
            for row, ref in ((0, dq), (2, dv)):
                sums = jnp.sum(ref[...].astype(F32), axis=0, keepdims=True)
                for z in range(2):
                    tile_sum[0, row + z : row + z + 1, 0:part_cols] = sums[
                        :, z * part_cols : (z + 1) * part_cols
                    ]
            tile_copy(0, dx, t, 0).start()

        def tile_second():
            tile_copy(0, dx, t, 0).wait_recv()
            tile_sum[1] = tile_sum[0] + tile_got[0]
            tile_copy(1, dy, t, 1).start()

        def tile_third():
            tile_copy(1, dy, t, 1).wait_recv()
            tile_sum[2] = tile_sum[1] + tile_got[1]
            for step in range(1, 4):
                tile_copy(2, d, (t + step) % 4, 1 + step).start()

        def tile_fourth():
            for step in range(1, 4):
                tile_copy(2, d, t, 1 + step).wait_recv()
            tile_sum[3] = (tile_sum[2] + tile_got[2]) + (tile_got[3] + tile_got[4])
            tile_copy(3, mate, t, 5).start()

        def tile_last():
            tile_copy(3, mate, t, 5).wait_recv()
            tile_own[...] = tile_sum[3]
            tile_mate[...] = tile_got[5]
            for slot, stage in enumerate((0, 1, 2, 2, 2, 3)):
                tile_copy(stage, mate, t, slot).wait_send()

        levels = [level_first, level_second, level_line, level_pass, level_near, level_mate]
        work = [partial(attention, pair, kb) for pair in range(heads_width // 128) for kb in range(blocks)]
        work += [partial(mix, i) for i in range(blocks)]
        work += [partial(weight_grad, j) for j in range(width // BLOCK)]
        for copy in loads:
            copy.start()
        level_first(0)
        level_first(1)
        return_rows(0, res, res_out, True)
        for copy in loads:
            copy.wait()
        done = 0
        for slot in range(n_chunks + 5):
            if slot < n_chunks - 1:
                upto = -(-len(work) * (slot + 1) // (n_chunks - 1))
                for unit in work[done:upto]:
                    unit()
                done = upto
            if slot == n_chunks - 2:
                tile_start()
            for lag, level in enumerate(levels):
                i = slot + 1 - lag
                if lag == 0 and i < 2:
                    continue
                if 0 <= i < n_chunks:
                    level(i)
            if slot == n_chunks - 2:
                for i in range(4):
                    send_rows(i)
            if slot >= n_chunks - 1:
                tail = slot - (n_chunks - 1)
                if tail < 4:
                    (tile_second, tile_third, tile_fourth, tile_last)[tail]()
        return_rows(0, res, res_out, False)
        settle_rows()
        for i in range(n_chunks):
            for copy in first_copies(i):
                copy.wait_send()

            @pl.when(u >= 2)
            def _():
                for copy in second_copies(i):
                    copy.wait_send()
                for b in range(2):
                    z_copy(i, b).wait_send()

            @pl.when(u == 1)
            def _():
                z_copy(i, 0).wait_send()

            @pl.when(u == 0)
            def _():
                y_copy(i).wait_send()

            @pl.when(u <= 1)
            def _():
                p_copy(i).wait_send()

    any_spec = pl.BlockSpec(memory_space=pl.ANY)
    vmem = pl.BlockSpec(memory_space=pltpu.VMEM)
    dma = pltpu.SemaphoreType.DMA
    scratch = []
    for kind in range(8):
        for s in range(count):
            rows, cols, kept = rows_of[s], grads[s].shape[2], grads[s].dtype
            shape, dtype = (
                ((2, 4 * rows, cols), kept),
                ((2, 4 * rows, cols), kept),
                ((2, 2 * rows, cols), kept),
                ((2, 2 * rows, cols), F32),
                ((2, 2 * rows, cols), kept),
                ((2, 2 * rows, cols), kept),
                ((2 * rows, cols), kept),
                ((rows, cols), kept),
            )[kind]
            scratch.append(pltpu.VMEM(shape, dtype))
    back = jax.ShapeDtypeStruct((2, 2 * half, width), output.dtype)
    tiles = jax.ShapeDtypeStruct(tile.shape, F32)
    outs = pl.pallas_call(
        kernel,
        out_shape=[
            back,
            back,
            tiles,
            tiles,
            *[jax.ShapeDtypeStruct((r, g.shape[2]), F32) for r, g in zip(rows_of, grads)],
        ],
        in_specs=[any_spec] * 4 + [vmem] * (7 + count),
        out_specs=[any_spec, any_spec] + [vmem] * (2 + count),
        scratch_shapes=[
            *scratch,
            pltpu.VMEM((half, width), output.dtype),
            dma,
            dma((2, 4)),
            dma((2, 2, 2)),
            dma((n_chunks, 3)),
            dma((n_chunks, 3)),
            dma((n_chunks, 2)),
            dma((n_chunks, 2)),
            dma((n_chunks, 2)),
            dma((n_chunks, 2)),
            dma((n_chunks,)),
            dma((n_chunks,)),
            dma((n_chunks,)),
            dma((n_chunks,)),
            pltpu.VMEM(weight.shape, BF),
            pltpu.VMEM((length, width), BF),
            pltpu.VMEM(weight.shape, BF),
            pltpu.VMEM((length, width), F32),
            pltpu.VMEM((8, length), F32),
            pltpu.VMEM((length, 128), F32),
            pltpu.VMEM((BLOCK, width), F32),
            pltpu.VMEM((length, heads_width), BF),
            pltpu.VMEM((length, heads_width), BF),
            pltpu.VMEM((length, heads_width), BF),
            pltpu.VMEM((2, length, 3 * part_cols), BF),
            pltpu.VMEM((4, half, width), BF),
            pltpu.VMEM((4, half, width), BF),
            pltpu.VMEM((4, half, width), F32),
            pltpu.VMEM((4, half, width), BF),
            dma((3,)),
            dma((6,)),
            dma((6,)),
            dma((2, 4)),
            dma((2, 4)),
            pltpu.VMEM((4, *tile.shape), F32),
            pltpu.VMEM((6, *tile.shape), F32),
        ],
        compiler_params=pltpu.CompilerParams(
            collective_id=2, has_side_effects=True, vmem_limit_bytes=62 * 1024 * 1024
        ),
    )(output, residual, x, weight, *heads, totals, limit, tile, *ready)
    return outs[0], outs[1], outs[2], outs[3], outs[4:]


BLOCK = 256


def lane_half(shape, h):
    lane = lax.broadcasted_iota(jnp.int32, shape, 1)
    return lane < DH if h == 0 else lane >= DH


def reach(row_block, blocks):
    return max(row_block + 1, blocks // 2)


def dot_nt(a, b):
    return lax.dot_general(a, b, (((1,), (1,)), ((), ())), preferred_element_type=F32)


def dot_tn(a, b):
    return lax.dot_general(a, b, (((0,), (0,)), ((), ())), preferred_element_type=F32)


def attend_rows(q_ref, k_ref, v_ref, o_ref, lt_ref, limit, pair, qb):
    length = q_ref.shape[0]
    blocks = length // BLOCK
    lanes = pl.ds(pair * 128, 128)
    rows = pl.ds(qb * BLOCK, BLOCK)
    span = reach(qb, blocks) * BLOCK
    q = q_ref[rows, lanes] * jnp.asarray(DH**-0.5, BF)
    heads = []
    for h in range(2):
        half = lane_half((BLOCK, 128), h)
        s = dot_nt(jnp.where(half, q, jnp.zeros_like(q)), k_ref[pl.ds(0, span), lanes])
        clear = qb * BLOCK
        row = lax.broadcasted_iota(jnp.int32, (BLOCK, span - clear), 0) + clear
        col = lax.broadcasted_iota(jnp.int32, (BLOCK, span - clear), 1) + clear
        seen = col <= row
        if clear < length // 2:
            seen = jnp.logical_or(seen, col.astype(F32) < limit)
        tail = jnp.where(seen, s[:, clear:], MASKED_SCORE)
        s = jnp.concatenate([s[:, :clear], tail], axis=1) if clear else tail
        top = jnp.max(s, axis=1, keepdims=True)
        p = jnp.exp(s - top)
        total = jnp.sum(p, axis=1, keepdims=True)
        log_total = top + jnp.log(total)
        lt_ref[2 * pair + h, 0:1, rows] = jnp.transpose(
            jnp.broadcast_to(log_total, (BLOCK, 128))
        )[0:1, :]
        p = (p * (1.0 / total)).astype(BF)
        heads.append(jnp.dot(p, v_ref[pl.ds(0, span), lanes], preferred_element_type=F32))
    o_ref[rows, lanes] = jnp.where(lane_half((BLOCK, 128), 0), heads[0], heads[1]).astype(BF)


def back_start(pair, o_ref, do_ref, dots, acc):
    head_row = lax.broadcasted_iota(jnp.int32, (8, 128), 0)
    lane = lax.broadcasted_iota(jnp.int32, (8, 128), 1)
    pick = (lane // DH == head_row).astype(F32)
    lanes = pl.ds(pair * 128, 128)
    dots[...] = lax.dot_general(
        pick,
        do_ref[:, lanes].astype(F32) * o_ref[:, lanes].astype(F32),
        (((1,), (1,)), ((), ())),
        precision=lax.Precision.HIGHEST,
        preferred_element_type=F32,
    )
    acc[...] = jnp.zeros_like(acc)


def back_block(pair, kb, q_ref, k_ref, v_ref, lt_ref, do_ref, dots, acc, dk_ref, dv_ref, limit):
    length = q_ref.shape[0]
    blocks = length // BLOCK
    lanes = pl.ds(pair * 128, 128)
    keys_at = pl.ds(kb * BLOCK, BLOCK)
    key = k_ref[keys_at, lanes]
    value = v_ref[keys_at, lanes]
    zero = jnp.zeros((BLOCK, 128), BF)
    dk = jnp.zeros((BLOCK, 128), F32)
    dv = jnp.zeros((BLOCK, 128), F32)
    for qb in range(blocks):
        if kb >= reach(qb, blocks):
            continue
        rows = pl.ds(qb * BLOCK, BLOCK)
        q_pair = q_ref[rows, lanes] * jnp.asarray(DH**-0.5, BF)
        do_pair = do_ref[rows, lanes]
        for h in range(2):
            half = lane_half((BLOCK, 128), h)
            q = jnp.where(half, q_pair, zero)
            do = jnp.where(half, do_pair, zero)
            s = dot_nt(key, q)
            if kb >= qb:
                key_id = lax.broadcasted_iota(jnp.int32, (BLOCK, BLOCK), 0) + kb * BLOCK
                row_id = lax.broadcasted_iota(jnp.int32, (BLOCK, BLOCK), 1) + qb * BLOCK
                seen = key_id <= row_id
                if kb * BLOCK < length // 2:
                    seen = jnp.logical_or(seen, key_id.astype(F32) < limit)
                s = jnp.where(seen, s, MASKED_SCORE)
            p = jnp.exp(s - lt_ref[2 * pair + h, 0:1, rows])
            dp = dot_nt(value, do)
            ds = (p * (dp - dots[h : h + 1, rows])).astype(BF)
            dv = dv + jnp.dot(p.astype(BF), do, preferred_element_type=F32)
            dk = dk + jnp.dot(ds, q, preferred_element_type=F32)
            acc[rows, :] += dot_tn(ds, jnp.where(half, key, zero))
    dk_ref[keys_at, lanes] = dk.astype(BF)
    dv_ref[keys_at, lanes] = dv.astype(BF)


def chip_local(
    tokens, prefix_len, w_qkv, bias_qv, w_out, w_up, bias_up, w_down, gains, shifts, cotangent
):
    d, t, k, c, _, _, _, _ = place()
    model_width = tokens.shape[2]
    length = tokens.shape[1] * 4
    part = w_qkv.shape[2]
    hidden = w_up.shape[1]

    def lanes(v):
        return jnp.pad(v, ((0, 0), (0, 128 - v.shape[1])))

    limits = jnp.concatenate([prefix_len // 16, prefix_len % 16]).astype(BF)[None]
    small = jnp.concatenate(
        [lanes(v) for v in (bias_qv, bias_up[None], gains, shifts, limits)], axis=0
    )
    small = jnp.pad(small, ((0, SMALL - small.shape[0]), (0, 0)))
    shards = (
        w_qkv.reshape(ROWS, 3 * part),
        w_out.T,
        w_up,
        w_down.T,
        small,
    )
    half = hidden // 2
    chunks = (
        (4, 0, 128),
        (0, 0, 3 * part),
        (1, 0, part),
        (2, 0, half),
        (2, half, half),
        (3, 0, half),
        (3, half, half),
    )
    x, cot, (g_qkv, g_out, g_up, g_down, g_small), small_other, heads = gather_attend(
        tokens, cotangent, shards, chunks, bias_qv.shape[1]
    )
    queries, key_heads, value_heads, context, totals, limit = heads

    mine = g_small.reshape(2, 8, SMALL, 128)
    theirs = small_other.reshape(2, 8, SMALL, 128)
    first = jnp.where(c == 0, mine, theirs)
    every = jnp.concatenate([first, jnp.where(c == 0, theirs, mine)], axis=0)
    per = bias_qv.shape[1]
    up_bias = mine[:, :, 2, : bias_up.shape[0]].astype(F32).reshape(2, hidden)
    rows = every[:, :, 3:9, :per].astype(F32).transpose(2, 1, 0, 3).reshape(6, model_width)
    full_gains, full_shifts = rows[:2], rows[2:]

    branch_part = sum(
        jnp.einsum(
            "rk,dk->rd", context[:, z * part : (z + 1) * part], g_out[z], preferred_element_type=F32
        )
        for z in range(2)
    ).astype(BF)
    branch = (
        branch_part.astype(F32) + pair_swap(branch_part).astype(F32) + full_shifts[0]
    )
    normed, normal_one, inverse_one = norm_forward(
        x.astype(F32) + branch, full_gains[0], full_shifts[1]
    )
    normed_low = normed.astype(BF)
    pre = [
        jnp.dot(normed_low, g_up[z], preferred_element_type=F32) + up_bias[z] for z in range(2)
    ]
    active = [jax.nn.gelu(v, approximate=False).astype(BF) for v in pre]
    feed_part = sum(
        jnp.einsum("rf,df->rd", active[z], g_down[z], preferred_element_type=F32)
        for z in range(2)
    ).astype(BF)
    feed_out = feed_part.astype(F32) + pair_swap(feed_part).astype(F32) + full_shifts[2]
    result, normal_two, inverse_two = norm_forward(
        normed + feed_out, full_gains[1], full_shifts[3]
    )
    incoming = cot.astype(F32)
    residual_two, gain_two, shift_two = norm_backward(
        incoming, normal_two, inverse_two, full_gains[1]
    )
    feed_grad = residual_two.astype(BF)
    upper = []
    for z in range(2):
        active_grad = jnp.dot(feed_grad, g_down[z], preferred_element_type=F32)
        _, pull = jax.vjp(partial(jax.nn.gelu, approximate=False), pre[z])
        upper.append(pull(active_grad)[0].astype(BF))
    normed_part = sum(
        jnp.einsum("rf,df->rd", upper[z], g_up[z], preferred_element_type=F32) for z in range(2)
    ).astype(BF)
    normed_grad = residual_two + (
        normed_part.astype(F32) + pair_swap(normed_part).astype(F32)
    )
    residual_one, gain_one, shift_one = norm_backward(
        normed_grad, normal_one, inverse_one, full_gains[0]
    )
    branch_grad = residual_one.astype(BF)
    context_grad = jnp.concatenate(
        [jnp.dot(branch_grad, g_out[z], preferred_element_type=F32) for z in range(2)], axis=1
    ).astype(BF)
    def outer(a, b):
        return jnp.einsum("rm,rn->mn", a, b, preferred_element_type=F32).astype(BF)

    grads = (
        jnp.stack(
            [outer(branch_grad, context[:, z * part : (z + 1) * part]) for z in range(2)]
        ),
        jnp.stack([outer(normed_low, upper[z]) for z in range(2)]),
        jnp.stack([outer(feed_grad, active[z]) for z in range(2)]),
    )
    tile = jnp.concatenate(
        [
            jnp.zeros((4, hidden), F32),
            jnp.stack([jnp.sum(v.astype(F32), axis=0) for v in upper]),
            jnp.stack(
                [
                    gain_one,
                    gain_two,
                    jnp.sum(branch_grad.astype(F32), axis=0),
                    shift_one,
                    jnp.sum(feed_grad.astype(F32), axis=0),
                    shift_two,
                ]
            ),
            jnp.zeros((4, hidden), F32),
        ]
    )
    back_chunks = (
        (3, 0, half),
        (3, half, half),
        (2, 0, half),
        (2, half, half),
        (1, 0, part),
        (0, 0, 3 * part),
    )
    out_rows, token_rows, tile_own, tile_mate, finals = back_reduce(
        result.astype(BF),
        residual_one,
        x,
        g_qkv,
        (queries, key_heads, value_heads, context, context_grad),
        totals,
        limit,
        grads,
        tile,
        back_chunks,
    )
    plane_rows = jnp.where(c == t // 2, tile_own, tile_mate)[:6].reshape(3, 2, hidden)
    plane_rows = lax.dynamic_index_in_dim(plane_rows, t % 2, 1, False)
    mine_rows = lax.dynamic_slice(tile_own, (6, (4 * d + t) * per), (6, per))
    return (
        out_rows,
        token_rows.astype(F32),
        finals[0].reshape(w_qkv.shape),
        lax.dynamic_slice(plane_rows, (0, d * per), (2, per)),
        finals[1].T,
        finals[2],
        lax.dynamic_slice(plane_rows, (2, d * bias_up.shape[0]), (1, bias_up.shape[0]))[0],
        finals[3].T,
        mine_rows[:2],
        mine_rows[2:],
    )


def solution(mesh):
    return jax.shard_map(
        chip_local if dict(mesh.shape) == {"dp": 8, "tensor": 4} else local,
        mesh=mesh,
        in_specs=(
            P("dp", "tensor", None),
            P("dp"),
            P("dp", None, "tensor"),
            P(None, ("tensor", "dp")),
            P("tensor", "dp"),
            P("dp", "tensor"),
            P(("tensor", "dp")),
            P("tensor", "dp"),
            P(None, ("dp", "tensor")),
            P(None, ("dp", "tensor")),
            P("dp", "tensor", None),
        ),
        out_specs=(
            P("dp", "tensor", None),
            P("dp", "tensor", None),
            P("dp", None, "tensor"),
            P(None, ("tensor", "dp")),
            P("tensor", "dp"),
            P("dp", "tensor"),
            P(("tensor", "dp")),
            P("tensor", "dp"),
            P(None, ("dp", "tensor")),
            P(None, ("dp", "tensor")),
        ),
        check_vma=False,
    )
```

```python
import math
from functools import partial

import jax
import jax.numpy as jnp
from jax import lax
from jax.experimental import pallas as pl
from jax.experimental.pallas import tpu as pltpu
from jax.sharding import PartitionSpec as P

DH = 64


EPSILON = 1e-05
MASKED_SCORE = -1e30


def norm_forward(values, gain_row, shift_row):
    center = values - jnp.mean(values, axis=-1, keepdims=True)
    inverse = lax.rsqrt(jnp.mean(center * center, axis=-1, keepdims=True) + EPSILON)
    normal = center * inverse
    return (normal * gain_row + shift_row, normal, inverse)


def norm_backward(incoming, normal, inverse, gain_row):
    scaled = incoming * gain_row
    first_mean = jnp.mean(scaled, axis=-1, keepdims=True)
    second_mean = jnp.mean(scaled * normal, axis=-1, keepdims=True)
    outgoing = inverse * (scaled - first_mean - normal * second_mean)
    return (outgoing, jnp.sum(incoming * normal, axis=0), jnp.sum(incoming, axis=0))


def visible_mask(offset, block_rows, length, prefix):
    row_ids = offset + jnp.arange(block_rows, dtype=jnp.int32)[:, None]
    column_ids = jnp.arange(length, dtype=jnp.int32)[None, :]
    return jnp.logical_or(column_ids < prefix, column_ids <= row_ids)


def block_scores(chosen, key_heads, offset, prefix, scaling):
    length = key_heads.shape[0]
    allowed = visible_mask(offset, chosen.shape[0], length, prefix)
    scores = (
        jnp.einsum("qhd,khd->hqk", chosen, key_heads, preferred_element_type=jnp.float32) * scaling
    )
    return jnp.where(allowed[None], scores, MASKED_SCORE)


def attention_forward(queries, key_heads, value_heads, prefix):
    length = key_heads.shape[0]
    block_rows = min(512, length)
    scaling = queries.shape[-1] ** (-0.5)
    outputs = []
    totals = []
    for offset in range(0, length, block_rows):
        scores = block_scores(
            queries[offset : offset + block_rows], key_heads, offset, prefix, scaling
        )
        row_max = jnp.max(scores, axis=-1, keepdims=True)
        log_total = jnp.log(jnp.sum(jnp.exp(scores - row_max), axis=-1, keepdims=True)) + row_max
        attn_probs = jnp.exp(scores - log_total).astype(jnp.bfloat16)
        outputs.append(
            jnp.einsum("hqk,khd->qhd", attn_probs, value_heads, preferred_element_type=jnp.float32)
        )
        totals.append(log_total)
    return (jnp.concatenate(outputs, axis=0), totals)


def attention_backward(queries, key_heads, value_heads, prefix, totals, context_grad):
    length = key_heads.shape[0]
    block_rows = min(512, length)
    scaling = queries.shape[-1] ** (-0.5)
    query_parts = []
    key_grad = jnp.zeros(key_heads.shape, jnp.float32)
    value_grad = jnp.zeros(value_heads.shape, jnp.float32)
    for number, offset in enumerate(range(0, length, block_rows)):
        chosen = queries[offset : offset + block_rows]
        grad_block = context_grad[offset : offset + block_rows]
        scores = block_scores(chosen, key_heads, offset, prefix, scaling)
        attn_probs = jnp.exp(scores - totals[number])
        probs_low = attn_probs.astype(jnp.bfloat16)
        probs_grad = jnp.einsum(
            "qhd,khd->hqk", grad_block, value_heads, preferred_element_type=jnp.float32
        )
        row_dot = jnp.sum(attn_probs * probs_grad, axis=-1, keepdims=True)
        scores_grad = (attn_probs * (probs_grad - row_dot)).astype(jnp.bfloat16)
        query_parts.append(
            jnp.einsum("hqk,khd->qhd", scores_grad, key_heads, preferred_element_type=jnp.float32)
            * scaling
        )
        key_grad = (
            key_grad
            + jnp.einsum("hqk,qhd->khd", scores_grad, chosen, preferred_element_type=jnp.float32)
            * scaling
        )
        value_grad = value_grad + jnp.einsum(
            "hqk,qhd->khd", probs_low, grad_block, preferred_element_type=jnp.float32
        )
    return (jnp.concatenate(query_parts, axis=0), key_grad, value_grad)


def local(
    tokens, prefix_len, w_qkv, bias_qv, w_out, w_up, bias_up, w_down, gains, shifts, cotangent
):
    tensor_count = lax.axis_size("tensor")
    seq_local, shard_rows, model_width = tokens.shape
    length = shard_rows * tensor_count
    full_qkv, full_bias_qv, full_out, full_up, full_bias_up, full_down = (
        lax.all_gather(w_qkv, "dp", axis=0, tiled=True),
        lax.all_gather(bias_qv, "dp", axis=1, tiled=True),
        lax.all_gather(w_out, "dp", axis=1, tiled=True),
        lax.all_gather(w_up, "dp", axis=0, tiled=True),
        lax.all_gather(bias_up, "dp", axis=0, tiled=True),
        lax.all_gather(w_down, "dp", axis=1, tiled=True),
    )
    full_gains, full_shifts = (
        lax.all_gather(gains, ("dp", "tensor"), axis=1, tiled=True),
        lax.all_gather(shifts, ("dp", "tensor"), axis=1, tiled=True),
    )
    full_gains = full_gains.astype(jnp.float32)
    full_shifts = full_shifts.astype(jnp.float32)
    bias_values = full_bias_qv.astype(jnp.float32)
    up_bias = full_bias_up.astype(jnp.float32)
    local_width = full_qkv.shape[2]
    head_count = local_width // DH
    kept_state = []
    outputs = []
    for member in range(seq_local):
        token_rows = tokens[member]
        prefix = prefix_len[member]

        def fold_tokens(piece):
            product = jnp.einsum("rd,dce->rce", piece, full_qkv, preferred_element_type=jnp.float32)
            return (piece, product)

        token_full, projected = fold_tokens(
            lax.all_gather(token_rows, "tensor", axis=0, tiled=True)
        )
        queries = (
            (projected[:, 0] + bias_values[0]).astype(jnp.bfloat16).reshape(length, head_count, DH)
        )
        key_heads = projected[:, 1].astype(jnp.bfloat16).reshape(length, head_count, DH)
        value_heads = (
            (projected[:, 2] + bias_values[1]).astype(jnp.bfloat16).reshape(length, head_count, DH)
        )
        context, totals = attention_forward(queries, key_heads, value_heads, prefix)
        context_low = context.reshape(length, local_width).astype(jnp.bfloat16)
        branch = (
            lax.psum_scatter(
                jnp.dot(context_low, full_out, preferred_element_type=jnp.float32).astype(
                    jnp.bfloat16
                ),
                "tensor",
                scatter_dimension=0,
                tiled=True,
            ).astype(jnp.float32)
            + full_shifts[0]
        )
        normed, normal_one, inverse_one = norm_forward(
            token_rows.astype(jnp.float32) + branch, full_gains[0], full_shifts[1]
        )
        normed_low = normed.astype(jnp.bfloat16)

        def fold_normed(piece):
            product = jnp.dot(piece, full_up, preferred_element_type=jnp.float32)
            return (piece, product)

        normed_full, pre_active = fold_normed(
            lax.all_gather(normed_low, "tensor", axis=0, tiled=True)
        )
        pre_active = pre_active + up_bias
        active_low = jax.nn.gelu(pre_active, approximate=False).astype(jnp.bfloat16)
        feed_out = (
            lax.psum_scatter(
                jnp.dot(active_low, full_down, preferred_element_type=jnp.float32).astype(
                    jnp.bfloat16
                ),
                "tensor",
                scatter_dimension=0,
                tiled=True,
            ).astype(jnp.float32)
            + full_shifts[2]
        )
        result, normal_two, inverse_two = norm_forward(
            normed + feed_out, full_gains[1], full_shifts[3]
        )
        outputs.append(result.astype(jnp.bfloat16))
        kept_state.append(
            (
                token_rows,
                prefix,
                token_full,
                queries,
                key_heads,
                value_heads,
                totals,
                context_low,
                normal_one,
                inverse_one,
                normed_full,
                pre_active,
                active_low,
                normal_two,
                inverse_two,
            )
        )
    back_qkv, back_out, back_up, back_down = (
        lax.all_gather(w_qkv, "dp", axis=0, tiled=True),
        lax.all_gather(w_out, "dp", axis=1, tiled=True),
        lax.all_gather(w_up, "dp", axis=0, tiled=True),
        lax.all_gather(w_down, "dp", axis=1, tiled=True),
    )
    full_shapes = (
        full_qkv.shape,
        full_bias_qv.shape,
        full_out.shape,
        full_up.shape,
        full_bias_up.shape,
        full_down.shape,
    )
    weight_grads = tuple((jnp.zeros(array_shape, jnp.float32) for array_shape in full_shapes))
    gain_grads = jnp.zeros((2, model_width), jnp.float32)
    shift_grads = jnp.zeros((4, model_width), jnp.float32)
    input_grads = []
    for member in range(seq_local):
        (
            token_rows,
            prefix,
            token_full,
            queries,
            key_heads,
            value_heads,
            totals,
            context_low,
            normal_one,
            inverse_one,
            normed_full,
            pre_active,
            active_low,
            normal_two,
            inverse_two,
        ) = kept_state[member]
        incoming = cotangent[member].astype(jnp.float32)
        residual_two, gain_two, shift_two = norm_backward(
            incoming, normal_two, inverse_two, full_gains[1]
        )
        feed_grad = residual_two.astype(jnp.bfloat16)
        fold_piece = lax.all_gather(feed_grad, "tensor", axis=0, tiled=True)
        down_grad = jnp.einsum(
            "rf,rd->fd", active_low, fold_piece, preferred_element_type=jnp.float32
        )
        fold_product = jnp.einsum(
            "rd,fd->rf", fold_piece, back_down, preferred_element_type=jnp.float32
        )
        active_grad = fold_product
        down_grad, active_grad = (down_grad, active_grad)
        layer_value, gelu_pull = jax.vjp(partial(jax.nn.gelu, approximate=False), pre_active)
        upper_grad = gelu_pull(active_grad)[0].astype(jnp.bfloat16)
        normed_grad = residual_two + lax.psum_scatter(
            jnp.einsum("rf,df->rd", upper_grad, back_up, preferred_element_type=jnp.float32).astype(
                jnp.bfloat16
            ),
            "tensor",
            scatter_dimension=0,
            tiled=True,
        ).astype(jnp.float32)
        up_grad = jnp.einsum(
            "ld,lf->df", normed_full, upper_grad, preferred_element_type=jnp.float32
        )
        up_bias_grad = jnp.sum(upper_grad.astype(jnp.float32), axis=0)
        residual_one, gain_one, shift_one = norm_backward(
            normed_grad, normal_one, inverse_one, full_gains[0]
        )
        branch_grad = residual_one.astype(jnp.bfloat16)

        def fold_branch(piece):
            out_grad = jnp.einsum(
                "rk,rd->kd", context_low, piece, preferred_element_type=jnp.float32
            )
            product = jnp.einsum("rd,kd->rk", piece, back_out, preferred_element_type=jnp.float32)
            return (out_grad, product)

        out_grad, context_grad = fold_branch(
            lax.all_gather(branch_grad, "tensor", axis=0, tiled=True)
        )
        context_grad = context_grad.astype(jnp.bfloat16).reshape(length, head_count, DH)
        query_grad, key_grad, value_grad = attention_backward(
            queries, key_heads, value_heads, prefix, totals, context_grad
        )
        mixed_grad = (
            jnp.stack([query_grad, key_grad, value_grad], axis=1)
            .astype(jnp.bfloat16)
            .reshape(length, 3, local_width)
        )
        qkv_grad = jnp.einsum(
            "ld,lce->dce", token_full, mixed_grad, preferred_element_type=jnp.float32
        )
        row_sums = jnp.sum(mixed_grad.astype(jnp.float32), axis=0)
        bias_grad = jnp.stack([row_sums[0], row_sums[2]])
        token_grad = residual_one + lax.psum_scatter(
            jnp.einsum(
                "rce,dce->rd", mixed_grad, back_qkv, preferred_element_type=jnp.float32
            ).astype(jnp.bfloat16),
            "tensor",
            scatter_dimension=0,
            tiled=True,
        ).astype(jnp.float32)
        input_grads.append(token_grad)
        gain_grads = gain_grads + jnp.stack([gain_one, gain_two])
        shift_grads = shift_grads + jnp.stack(
            [
                jnp.sum(branch_grad.astype(jnp.float32), axis=0),
                shift_one,
                jnp.sum(feed_grad.astype(jnp.float32), axis=0),
                shift_two,
            ]
        )
        member_grads = (qkv_grad, bias_grad, out_grad, up_grad, up_bias_grad, down_grad)
        weight_grads = tuple(
            (running + grad_part for running, grad_part in zip(weight_grads, member_grads))
        )
    total_qkv, total_bias, total_out, total_up, total_up_bias, total_down = weight_grads
    weight_grads = (
        lax.psum_scatter(total_qkv, "dp", scatter_dimension=0, tiled=True),
        lax.psum_scatter(total_bias, "dp", scatter_dimension=1, tiled=True),
        lax.psum_scatter(total_out, "dp", scatter_dimension=1, tiled=True),
        lax.psum_scatter(total_up, "dp", scatter_dimension=0, tiled=True),
        lax.psum_scatter(total_up_bias, "dp", scatter_dimension=0, tiled=True),
        lax.psum_scatter(total_down, "dp", scatter_dimension=1, tiled=True),
    )
    gain_share, shift_share = (
        lax.psum_scatter(gain_grads, ("dp", "tensor"), scatter_dimension=1, tiled=True),
        lax.psum_scatter(shift_grads, ("dp", "tensor"), scatter_dimension=1, tiled=True),
    )
    return (
        jnp.stack(outputs),
        jnp.stack(input_grads),
        weight_grads[0],
        weight_grads[1],
        weight_grads[2],
        weight_grads[3],
        weight_grads[4],
        weight_grads[5],
        gain_share,
        shift_share,
    )


MESH_ID = pl.DeviceIdType.MESH
BF = jnp.bfloat16
F32 = jnp.float32
ROWS = 96
SMALL = 16


def place():
    d = lax.axis_index("dp")
    t = lax.axis_index("tensor")
    k, c = d // 2, d % 2
    xb, yb = k % 2, k // 2
    dx = d + 2 - 4 * xb
    dy = d + 4 - 8 * yb
    return d, t, k, c, xb, yb, dx, dy


def remote(src, dst, send, recv, dp, tensor):
    return pltpu.make_async_remote_copy(
        src_ref=src,
        dst_ref=dst,
        send_sem=send,
        recv_sem=recv,
        device_id=(dp, tensor),
        device_id_type=MESH_ID,
    )


def enter(k, c, t, d, dx, dy):
    barrier = pltpu.get_barrier_semaphore()

    def greet(dp, tensor):
        pl.semaphore_signal(barrier, inc=1, device_id=(dp, tensor), device_id_type=MESH_ID)

    greet(dx, t)
    greet(dy, t)
    greet(d + 1 - 2 * c, t)
    for step in range(1, 4):
        other = (t + step) % 4
        greet(2 * k, other)
        greet(2 * k + 1, other)
    pl.semaphore_wait(barrier, 9)


def gather_attend(tokens, cotangent, shards, chunks, per):
    half = tokens.shape[1] // 2
    width = tokens.shape[2]
    count = len(shards)
    n_chunks = len(chunks)
    rows_of = [s.shape[0] for s in shards]
    length = tokens.shape[1] * 4
    part = shards[0].shape[1] // 3
    heads_width = 2 * part
    blocks = length // BLOCK

    def kernel(*refs):
        tok, cot = refs[0], refs[1]
        own = refs[2 : 2 + count]
        base = 2 + count
        xf, cf = refs[base], refs[base + 1]
        full = refs[base + 2 : base + 2 + count]
        small_other, q_out, k_out, v_out, o_out, lt_out, limit_out = refs[
            base + 2 + count : base + 9 + count
        ]
        stage = refs[base + 9 + count : base + 9 + 2 * count]
        (
            x_rows,
            weight,
            small_low,
            small_rows,
            load_sem,
            row_stage,
            local_sem,
            row_sem,
            ex_send,
            ex_recv,
            fw_send,
            fw_recv,
            p_send,
            p_recv,
            z_send,
            z_recv,
            a_send,
            a_recv,
            b_send,
            b_recv,
            o_send,
            o_recv,
        ) = refs[base + 9 + 2 * count :]
        d, t, k, c, xb, yb, dx, dy = place()
        mate = d + 1 - 2 * c
        u = t + c * (3 - 2 * t)
        up = t + 1 - 2 * c
        down = t - 1 + 2 * c
        source = t // 2 == c
        enter(k, c, t, d, dx, dy)

        for s in range(count):
            rows = rows_of[s]
            spot = full[s].at[t % 2, pl.ds(d * rows, rows)]

            @pl.when(source)
            def _():
                pltpu.make_async_copy(own[s], stage[s], local_sem.at[s]).start()

            @pl.when(jnp.logical_not(source))
            def _():
                remote(own[s], spot, p_send.at[s], p_recv.at[s], mate, t).start()

        def exchange(which, src, dst):
            for m in range(2):
                goal = 2 * c + m
                for core in range(2):
                    piece = src.at[m, pl.ds(core * half, half)]
                    spot = dst.at[t * 2 + core]
                    here = jnp.logical_and(goal == t, core == c)

                    @pl.when(here)
                    def _():
                        load = pltpu.make_async_copy(piece, row_stage, row_sem)
                        load.start()
                        load.wait()
                        store = pltpu.make_async_copy(row_stage, spot, row_sem)
                        store.start()
                        store.wait()

                    @pl.when(jnp.logical_not(here))
                    def _():
                        remote(
                            piece,
                            spot,
                            ex_send.at[which, 2 * m + core],
                            ex_recv.at[which, t],
                            2 * k + core,
                            goal,
                        ).start()

        def relay(which, dst):
            for origin in range(4):
                spot = dst.at[origin * 2 + c]
                local = jnp.logical_and(origin == t, c == t // 2)

                @pl.when(jnp.logical_not(local))
                def _():
                    remote(
                        spot, spot, ex_send.at[which, 0], ex_recv.at[which, origin], mate, t
                    ).wait_recv()

                remote(
                    spot, spot, fw_send.at[which, origin], fw_recv.at[which, origin], mate, t
                ).start()

        def arrived(which, dst):
            for origin in range(4):
                spot = dst.at[origin * 2 + 1 - c]
                remote(
                    spot, spot, fw_send.at[which, origin], fw_recv.at[which, origin], mate, t
                ).wait_recv()

        def settle(which, src, dst):
            for origin in range(4):
                spot = dst.at[origin * 2 + 1 - c]
                remote(
                    spot, spot, fw_send.at[which, origin], fw_recv.at[which, origin], mate, t
                ).wait_send()
            for m in range(2):
                for core in range(2):
                    here = jnp.logical_and(2 * c + m == t, core == c)

                    @pl.when(jnp.logical_not(here))
                    def _():
                        remote(
                            src.at[m, pl.ds(core * half, half)],
                            dst.at[t * 2 + core],
                            ex_send.at[which, 2 * m + core],
                            ex_recv.at[which, t],
                            mate,
                            t,
                        ).wait_send()

        def placed(s):
            @pl.when(source)
            def _():
                rows = rows_of[s]
                spot = full[s].at[t % 2, pl.ds(d * rows, rows)]
                pltpu.make_async_copy(own[s], stage[s], local_sem.at[s]).wait()
                pltpu.make_async_copy(stage[s], spot, local_sem.at[s]).start()

        def block(i, b, start, n):
            s, col, cols = chunks[i]
            zz = b + c * (1 - 2 * b)
            rows = rows_of[s]
            return full[s].at[zz, pl.ds(start * rows, n * rows), pl.ds(col, cols)]

        def z_copy(i, b, way, target):
            ref = block(i, b, 2 * k, 2)
            return remote(ref, ref, z_send.at[i, b, way], z_recv.at[i, b], d, target)

        def first_copy(i, b):
            ref = block(i, b, 2 * k, 2)
            return remote(ref, ref, a_send.at[i, b], a_recv.at[i, b], dx if b == 0 else dy, t)

        def first_arrival(i, b):
            near = k + 1 - 2 * xb if b == 0 else k + 2 - 4 * yb
            ref = block(i, b, 2 * near, 2)
            return remote(ref, ref, a_send.at[i, b], a_recv.at[i, b], dx if b == 0 else dy, t)

        def second_copies(i, arriving):
            other = 1 if arriving else 0
            row = yb + other * (1 - 2 * yb)
            ref = block(i, 0, 4 * row, 4)
            col = xb + other * (1 - 2 * xb)
            out = [remote(ref, ref, b_send.at[i, 0], b_recv.at[i, 0], dy, t)]
            for r in range(2):
                ref = block(i, 1, 2 * (2 * r + col), 2)
                out.append(remote(ref, ref, b_send.at[i, 1 + r], b_recv.at[i, 1 + r], dx, t))
            return out

        def spread(i, b):
            @pl.when(jnp.logical_and(u >= b, u < 3))
            def _():
                z_copy(i, b, 0, up).start()

            if b == 1:

                @pl.when(u == 1)
                def _():
                    z_copy(i, 1, 1, down).start()

            first_copy(i, b).start()

        waited = set()

        def own_ready(i):
            s = chunks[i][0]
            if s in waited:
                return
            waited.add(s)
            rows = rows_of[s]
            spot = full[s].at[t % 2, pl.ds(d * rows, rows)]
            twin = full[s].at[t % 2, pl.ds(mate * rows, rows)]
            pltpu.make_async_copy(stage[s], spot, local_sem.at[s]).wait()
            remote(twin, twin, p_send.at[s], p_recv.at[s], mate, t).wait_recv()

        def level_own(i):
            if chunks[i][0] not in waited:

                @pl.when(source)
                def _():
                    own_ready(i)

            for b in range(2):

                @pl.when(u == b)
                def _():
                    spread(i, b)

        def level_line(i):
            for b in (1, 0):

                @pl.when(u != b)
                def _():
                    z_copy(i, b, 0, up).wait_recv()
                    spread(i, b)

        def level_second(i):
            for b in range(2):
                first_arrival(i, b).wait_recv()
            for copy in second_copies(i, False):
                copy.start()

        def level_done(i):
            for copy in second_copies(i, True):
                copy.wait_recv()

        def expand(plane, kind):
            rows = small_rows[plane, pl.ds(kind, 8, stride=SMALL), :]
            spots = lax.broadcasted_iota(jnp.int32, (128, part), 0)
            lane = lax.broadcasted_iota(jnp.int32, (128, part), 1)
            wide = jnp.dot(
                rows,
                (spots == lane % per).astype(F32),
                precision=lax.Precision.HIGHEST,
                preferred_element_type=F32,
            )
            row = lax.broadcasted_iota(jnp.int32, (8, part), 0)
            lane = lax.broadcasted_iota(jnp.int32, (8, part), 1)
            return jnp.sum(jnp.where(lane // per == row, wide, 0.0), axis=0, keepdims=True)

        def prefix_of():
            tile = small_rows[0, pl.ds((2 * k + t // 2) * SMALL + 9, 1), 0:128]
            lane = lax.broadcasted_iota(jnp.int32, (1, 128), 1)
            member = t % 2
            value = 16.0 * jnp.sum(jnp.where(lane == member, tile, 0.0), axis=1, keepdims=True)
            value += jnp.sum(jnp.where(lane == 2 + member, tile, 0.0), axis=1, keepdims=True)
            return value

        def project():
            bias_q = jnp.concatenate([expand(0, 0), expand(1, 0)], axis=1)
            bias_v = jnp.concatenate([expand(0, 1), expand(1, 1)], axis=1)

            @pl.loop(0, blocks)
            def _(block_id):
                rows = pl.ds(block_id * BLOCK, BLOCK)
                both = [
                    jnp.dot(x_rows[rows, :], weight[z], preferred_element_type=F32)
                    for z in range(2)
                ]

                def kind(i):
                    return jnp.concatenate([v[:, i * part : (i + 1) * part] for v in both], axis=1)

                q_out[rows, :] = (kind(0) + bias_q).astype(BF)
                k_out[rows, :] = kind(1).astype(BF)
                v_out[rows, :] = (kind(2) + bias_v).astype(BF)

        load_rows = [
            pltpu.make_async_copy(xf.at[i], x_rows.at[pl.ds(i * half, half)], load_sem.at[i])
            for i in range(8)
        ]
        load_weight = pltpu.make_async_copy(full[0], weight, load_sem.at[8])
        last = count - 1
        swap = remote(full[last], small_other, o_send, o_recv, mate, t)

        placed(last)
        placed(0)
        level_own(0)
        level_own(1)
        exchange(0, tok, xf)
        for s in range(1, last):
            placed(s)
        level_line(0)
        level_line(1)
        level_second(0)
        level_own(2)
        level_own(3)
        level_second(1)
        relay(0, xf)
        level_line(2)
        level_own(4)
        level_done(0)
        swap.start()
        small_load = pltpu.make_async_copy(full[last], small_low, load_sem.at[9])
        small_load.start()
        arrived(0, xf)
        for copy in load_rows:
            copy.start()
        level_line(3)
        level_second(2)
        for i in range(5, n_chunks):
            level_own(i)
        small_load.wait()
        small_rows[...] = small_low[...].astype(F32)
        level_done(1)
        load_weight.start()
        level_second(3)
        exchange(1, cot, cf)
        for copy in load_rows:
            copy.wait()
        load_weight.wait()
        limit_out[...] = jnp.broadcast_to(prefix_of(), limit_out.shape)
        project()
        todo = []
        for i in range(4, n_chunks):
            todo.append(partial(level_line, i))
            todo.append(partial(level_second, i))
        todo.append(lambda: relay(1, cf))
        work = [
            partial(attend_rows, q_out, k_out, v_out, o_out, lt_out, prefix_of(), pair, qb)
            for pair in range(heads_width // 128)
            for qb in range(blocks)
        ]
        for step in range(max(len(todo), len(work))):
            if step < len(todo):
                todo[step]()
            if step < len(work):
                work[step]()
        for i in range(2, n_chunks):
            level_done(i)
        arrived(1, cf)
        settle(0, tok, xf)
        settle(1, cot, cf)
        for s in range(count):
            rows = rows_of[s]
            spot = full[s].at[t % 2, pl.ds(d * rows, rows)]

            @pl.when(jnp.logical_not(source))
            def _():
                remote(own[s], spot, p_send.at[s], p_recv.at[s], mate, t).wait_send()

        for i in range(n_chunks):
            for b in range(2):

                @pl.when(jnp.logical_and(u >= b, u < 3))
                def _():
                    z_copy(i, b, 0, up).wait_send()

                first_copy(i, b).wait_send()

            @pl.when(u == 1)
            def _():
                z_copy(i, 1, 1, down).wait_send()

            for copy in second_copies(i, False):
                copy.wait_send()
        swap.wait()

    any_spec = pl.BlockSpec(memory_space=pl.ANY)
    vmem = pl.BlockSpec(memory_space=pltpu.VMEM)
    dma = pltpu.SemaphoreType.DMA
    full_shapes = [jax.ShapeDtypeStruct((2, 8 * s.shape[0], s.shape[1]), s.dtype) for s in shards]
    rows_shape = jax.ShapeDtypeStruct((8, half, width), tokens.dtype)
    head_shape = jax.ShapeDtypeStruct((length, heads_width), BF)
    lt_shape = jax.ShapeDtypeStruct((heads_width // DH, 8, length), F32)
    outs = pl.pallas_call(
        kernel,
        out_shape=[
            rows_shape,
            rows_shape,
            *full_shapes,
            full_shapes[-1],
            *[head_shape] * 4,
            lt_shape,
            jax.ShapeDtypeStruct((8, 128), F32),
        ],
        in_specs=[any_spec] * (2 + count),
        out_specs=[any_spec] * (3 + count) + [vmem] * 6,
        scratch_shapes=[
            *[pltpu.VMEM(s.shape, s.dtype) for s in shards],
            pltpu.VMEM((length, width), BF),
            pltpu.VMEM((2, 8 * shards[0].shape[0], shards[0].shape[1]), BF),
            pltpu.VMEM((2, 8 * SMALL, 128), BF),
            pltpu.VMEM((2, 8 * SMALL, 128), F32),
            dma((10,)),
            pltpu.VMEM((half, width), tokens.dtype),
            dma((count,)),
            dma,
            dma((2, 4)),
            dma((2, 4)),
            dma((2, 4)),
            dma((2, 4)),
            dma((count,)),
            dma((count,)),
            dma((n_chunks, 2, 2)),
            dma((n_chunks, 2)),
            dma((n_chunks, 2)),
            dma((n_chunks, 2)),
            dma((n_chunks, 3)),
            dma((n_chunks, 3)),
            dma,
            dma,
        ],
        compiler_params=pltpu.CompilerParams(
            collective_id=1, has_side_effects=True, vmem_limit_bytes=60 * 1024 * 1024
        ),
    )(tokens, cotangent, *shards)
    return (
        outs[0].reshape(length, width),
        outs[1].reshape(length, width),
        outs[2 : 2 + count],
        outs[2 + count],
        outs[3 + count :],
    )


def gelu_parts(u):
    half = math.sqrt(0.5)
    e = jnp.exp(u * u * -0.5)
    f = 1.0 / (1.0 + (0.3275911 * half) * jnp.abs(u))
    series = 0.5 * 1.061405429 * f - 0.5 * 1.453152027
    series = series * f + 0.5 * 1.421413741
    series = series * f - 0.5 * 0.284496736
    series = series * f + 0.5 * 0.254829592
    tail = series * f * e
    share = jnp.where(u >= 0.0, 1.0 - tail, tail)
    return u * share, share + u * e * (1.0 / math.sqrt(2.0 * math.pi))


def layer_back(x, cot, weights, heads, totals, limit, small_own, small_other, per, chunks):
    part_cols = weights[0].shape[2] // 3
    heads_width = 2 * part_cols
    hidden = weights[2].shape[2]
    up_per = hidden // 8
    grads = weights
    output = x
    count = len(grads)
    n_chunks = len(chunks)
    length, width = output.shape
    half = length // 8
    blocks = length // BLOCK
    rows_of = [g.shape[1] // 8 for g in grads]

    def kernel(*refs):
        x_hbm, cot_hbm = refs[:2]
        held = refs[2 : 2 + count]
        q_ref, k_ref, v_ref, o_ref, lt_ref, limit_ref, small_a, small_b = refs[
            2 + count : 10 + count
        ]
        base = 10 + count
        res_out, tgr_out, tile_own, tile_mate = refs[base : base + 4]
        final = refs[base + 4 : base + 4 + count]
        base += 4 + count
        got1 = refs[base : base + count]
        sum1 = refs[base + count : base + 2 * count]
        got2 = refs[base + 2 * count : base + 3 * count]
        sum2 = refs[base + 3 * count : base + 4 * count]
        got3 = refs[base + 4 * count : base + 5 * count]
        sum3 = refs[base + 5 * count : base + 6 * count]
        got4 = refs[base + 6 * count : base + 7 * count]
        got5 = refs[base + 7 * count : base + 8 * count]
        (
            row_sem,
            ex_send,
            ex_recv,
            a_send,
            a_recv,
            b_send,
            b_recv,
            z_send,
            z_recv,
            y_send,
            y_recv,
            p_send,
            p_recv,
            wq,
            wo,
            wu,
            wd,
            x_rows,
            cot_rows,
            small_rows,
            row_values,
            out_both,
            n1_rows,
            inv_rows,
            residual_rows,
            res_rows,
            low_rows,
            feed_rows,
            branch_rows,
            sent,
            got,
            active,
            upper,
            do_ref,
            dots,
            acc,
            acc_rows,
            mate_got,
            load_sem,
            e_send,
            e_recv,
            s_send,
            s_recv,
            t_send,
            t_recv,
            tile_sum,
            tile_got,
        ) = refs[base + 8 * count :]
        part = (wq, wo, wu, wd)
        mixed = active
        dq, dk, dv = (
            upper.at[0, :, pl.ds(0, heads_width)],
            upper.at[0, :, pl.ds(heads_width, heads_width)],
            upper.at[1, :, pl.ds(0, heads_width)],
        )
        d, t, k, c, xb, yb, dx, dy = place()
        mate = d + 1 - 2 * c
        u = t + c * (3 - 2 * t)
        up = t + 1 - 2 * c
        down = t - 1 + 2 * c
        source = u <= 1
        enter(k, c, t, d, dx, dy)

        def plane(b):
            return b + c * (1 - 2 * b)

        def first_copies(i):
            s, col, cols = chunks[i]
            rows = rows_of[s]
            spot = pl.ds(col, cols)
            out = [
                remote(
                    part[s].at[plane(0), pl.ds((1 - yb) * 4 * rows, 4 * rows), spot],
                    got1[s].at[0, :, spot],
                    a_send.at[i, 0],
                    a_recv.at[i, 0],
                    dy,
                    t,
                )
            ]
            for r in range(2):
                out.append(
                    remote(
                        part[s].at[plane(1), pl.ds((2 * r + 1 - xb) * 2 * rows, 2 * rows), spot],
                        got1[s].at[1, pl.ds(r * 2 * rows, 2 * rows), spot],
                        a_send.at[i, 1 + r],
                        a_recv.at[i, 1 + r],
                        dx,
                        t,
                    )
                )
            return out

        def second_copies(i):
            s, col, cols = chunks[i]
            rows = rows_of[s]
            spot = pl.ds(col, cols)
            out = []
            for b, far, goal in ((0, 1 - xb, dx), (1, 1 - yb, dy)):
                out.append(
                    remote(
                        sum1[s].at[b, pl.ds(far * 2 * rows, 2 * rows), spot],
                        got2[s].at[b, :, spot],
                        b_send.at[i, b],
                        b_recv.at[i, b],
                        goal,
                        t,
                    )
                )
            return out

        def low(v, s):
            return v.astype(sum1[s].dtype)

        def level_first(i):
            for copy in first_copies(i):
                copy.start()

        def level_second(i):
            s, col, cols = chunks[i]
            rows = rows_of[s]
            spot = pl.ds(col, cols)
            for copy in first_copies(i):
                copy.wait_recv()
            mine = part[s][plane(0), pl.ds(yb * 4 * rows, 4 * rows), spot]
            sum1[s][0, :, spot] = low(mine.astype(F32) + got1[s][0, :, spot].astype(F32), s)
            for r in range(2):
                mine = part[s][plane(1), pl.ds((2 * r + xb) * 2 * rows, 2 * rows), spot]
                there = pl.ds(r * 2 * rows, 2 * rows)
                sum1[s][1, there, spot] = low(
                    mine.astype(F32) + got1[s][1, there, spot].astype(F32), s
                )
            for copy in second_copies(i):
                copy.start()

        def z_copy(i, b):
            s, col, cols = chunks[i]
            spot = pl.ds(col, cols)
            return remote(
                sum3[s].at[b, :, spot],
                got3[s].at[b, :, spot],
                z_send.at[i, b],
                z_recv.at[i, b],
                d,
                down,
            )

        def y_copy(i):
            s, col, cols = chunks[i]
            spot = pl.ds(col, cols)
            return remote(
                sum3[s].at[1, :, spot], got4[s].at[:, spot], y_send.at[i], y_recv.at[i], d, up
            )

        def level_line(i):
            s, col, cols = chunks[i]
            rows = rows_of[s]
            spot = pl.ds(col, cols)
            for copy in second_copies(i):
                copy.wait_recv()
            for b, near in ((0, xb), (1, yb)):
                mine = sum1[s][b, pl.ds(near * 2 * rows, 2 * rows), spot]
                sum2[s][b, :, spot] = mine.astype(F32) + got2[s][b, :, spot].astype(F32)

            @pl.when(u == 3)
            def _():
                for b in range(2):
                    sum3[s][b, :, spot] = low(sum2[s][b, :, spot], s)
                    z_copy(i, b).start()

            @pl.when(u == 0)
            def _():
                sum3[s][1, :, spot] = low(sum2[s][1, :, spot], s)
                y_copy(i).start()

        def level_pass(i):
            s, col, cols = chunks[i]
            spot = pl.ds(col, cols)

            @pl.when(u == 2)
            def _():
                for b in range(2):
                    z_copy(i, b).wait_recv()
                    sum3[s][b, :, spot] = low(
                        sum2[s][b, :, spot] + got3[s][b, :, spot].astype(F32), s
                    )
                    z_copy(i, b).start()

        def level_near(i):
            s, col, cols = chunks[i]
            spot = pl.ds(col, cols)

            @pl.when(u == 1)
            def _():
                z_copy(i, 0).wait_recv()
                sum3[s][0, :, spot] = low(
                    sum2[s][0, :, spot] + got3[s][0, :, spot].astype(F32), s
                )
                z_copy(i, 0).start()
                z_copy(i, 1).wait_recv()
                y_copy(i).wait_recv()
                total = (
                    sum2[s][1, :, spot]
                    + got3[s][1, :, spot].astype(F32)
                    + got4[s][:, spot].astype(F32)
                )
                finish(i, total)

            @pl.when(u == 0)
            def _():
                z_copy(i, 0).wait_recv()
                finish(i, sum2[s][0, :, spot] + got3[s][0, :, spot].astype(F32))

        def p_copy(i):
            s, col, cols = chunks[i]
            rows = rows_of[s]
            spot = pl.ds(col, cols)
            return remote(
                sum1[s].at[0, pl.ds((1 - c) * rows, rows), spot],
                got5[s].at[:, spot],
                p_send.at[i],
                p_recv.at[i],
                mate,
                t,
            )

        def finish(i, total):
            s, col, cols = chunks[i]
            rows = rows_of[s]
            spot = pl.ds(col, cols)
            for copy in second_copies(i):
                copy.wait_send()
            sum2[s][0, :, spot] = total
            sum1[s][0, pl.ds(0, 2 * rows), spot] = low(total, s)
            p_copy(i).start()
            final[s][:, spot] = sum2[s][0, pl.ds(c * rows, rows), spot]

        def level_mate(i):
            s, col, cols = chunks[i]
            spot = pl.ds(col, cols)

            @pl.when(u >= 2)
            def _():
                p_copy(i).wait_recv()
                final[s][:, spot] = got5[s][:, spot].astype(F32)

        loads = [
            pltpu.make_async_copy(src, dst, load_sem.at[i])
            for i, (src, dst) in enumerate(
                (
                    (held[1], wo),
                    (x_hbm, x_rows),
                    (held[2], wu),
                    (held[3], wd),
                    (cot_hbm, cot_rows),
                    (held[0], wq),
                )
            )
        ]

        def widen(rows, size, spot):
            n, wide = rows.shape[0], row_values.shape[1]
            at = lax.broadcasted_iota(jnp.int32, (128, wide), 0)
            lane = lax.broadcasted_iota(jnp.int32, (128, wide), 1)
            v = jnp.dot(
                rows,
                (at == lane % size).astype(F32),
                precision=lax.Precision.HIGHEST,
                preferred_element_type=F32,
            )
            row = lax.broadcasted_iota(jnp.int32, (n, wide), 0)
            lane = lax.broadcasted_iota(jnp.int32, (n, wide), 1)
            return jnp.sum(jnp.where(lane // size == spot(row), v, 0.0), axis=0, keepdims=True)

        def unpack():
            for z in range(2):
                small_rows[pl.ds((2 * c + z) * 8 * SMALL, 8 * SMALL), :] = small_a[z].astype(F32)
                small_rows[pl.ds((2 - 2 * c + z) * 8 * SMALL, 8 * SMALL), :] = small_b[z].astype(F32)
            for kind in range(6):
                rows = small_rows[pl.ds(3 + kind, 32, stride=SMALL), :]
                row_values[kind : kind + 1, :] = widen(
                    rows, per, lambda row: (row % 8) * 4 + row // 8
                )
            for z in range(2):
                rows = small_rows[pl.ds((2 * c + z) * 8 * SMALL + 2, 8, stride=SMALL), :]
                row_values[6 + z : 7 + z, :] = widen(rows, up_per, lambda row: row)

        def value_row(i):
            return row_values[i : i + 1, :]

        def swap_copy(which, i):
            rows = pl.ds(i * BLOCK, BLOCK)
            return remote(
                sent.at[rows],
                got.at[which, rows],
                e_send.at[which, i],
                e_recv.at[which, i],
                mate,
                t,
            )

        def swapped(which, i):
            rows = pl.ds(i * BLOCK, BLOCK)
            swap_copy(which, i).wait()
            return sent[rows, :].astype(F32) + got[which, rows, :].astype(F32)

        def swap(which, i, share):
            sent[pl.ds(i * BLOCK, BLOCK), :] = share.astype(BF)
            swap_copy(which, i).start()

        def normalize(v):
            center = v - jnp.mean(v, axis=1, keepdims=True)
            inverse = lax.rsqrt(jnp.mean(center * center, axis=1, keepdims=True) + EPSILON)
            return center * inverse, inverse

        def norm_pull(scaled, normal, inverse):
            first = jnp.mean(scaled, axis=1, keepdims=True)
            second = jnp.mean(scaled * normal, axis=1, keepdims=True)
            return inverse * (scaled - first - normal * second)

        def tally(row, v):
            tile_sum[0, row : row + 1, :] += jnp.sum(v, axis=0, keepdims=True)

        def branch_block(i):
            swap(0, i, dot_nt(o_ref[pl.ds(i * BLOCK, BLOCK), :], out_both[...]))

        def forward_block(i):
            rows = pl.ds(i * BLOCK, BLOCK)
            branch = swapped(0, i) + value_row(2)
            normal, inverse = normalize(x_rows[rows, :].astype(F32) + branch)
            n1_rows[rows, :] = normal
            inv_rows[rows, :] = jnp.broadcast_to(inverse, (BLOCK, 128))
            low_rows[rows, :] = (normal * value_row(0) + value_row(3)).astype(BF)
            for z in range(2):
                for col in range(0, hidden, BLOCK):
                    cols = pl.ds(col, BLOCK)
                    u = jnp.dot(low_rows[rows, :], wu[z, :, cols], preferred_element_type=F32)
                    value, slope = gelu_parts(u + row_values[6 + z : 7 + z, cols])
                    active[z, rows, cols] = value.astype(BF)
                    upper[z, rows, cols] = slope.astype(BF)
            swap(1, i, dot_nt(active[0, rows, :], wd[0]) + dot_nt(active[1, rows, :], wd[1]))

        def row_home(i):
            return jnp.logical_and(i == t, c == t // 2)

        def out_copy(i):
            return remote(
                res_rows.at[pl.ds((2 * i + c) * half, half)],
                res_out.at[t % 2, pl.ds(c * half, half)],
                ex_send.at[0, i],
                ex_recv.at[0, t % 2, c],
                2 * k + t // 2,
                i,
            )

        def output_block(i):
            rows = pl.ds(i * BLOCK, BLOCK)
            feed_out = swapped(1, i) + value_row(4)
            normed = n1_rows[rows, :] * value_row(0) + value_row(3)
            normal, inverse = normalize(normed + feed_out)
            res_rows[rows, :] = (normal * value_row(1) + value_row(5)).astype(BF)
            incoming = cot_rows[rows, :].astype(F32)
            tally(7, incoming * normal)
            tally(11, incoming)
            residual = norm_pull(incoming * value_row(1), normal, inverse)
            residual_rows[rows, :] = residual
            feed = residual.astype(BF)
            feed_rows[rows, :] = feed
            tally(10, feed.astype(F32))
            for z in range(2):
                for col in range(0, hidden, BLOCK):
                    cols = pl.ds(col, BLOCK)
                    pull = jnp.dot(feed_rows[rows, :], wd[z, :, cols], preferred_element_type=F32)
                    grad = (pull * upper[z, rows, cols].astype(F32)).astype(BF)
                    upper[z, rows, cols] = grad
                    tile_sum[0, 4 + z : 5 + z, cols] += jnp.sum(
                        grad.astype(F32), axis=0, keepdims=True
                    )
            swap(2, i, dot_nt(upper[0, rows, :], wu[0]) + dot_nt(upper[1, rows, :], wu[1]))

            @pl.when(row_home(i))
            def _():
                store = pltpu.make_async_copy(
                    res_rows.at[pl.ds((2 * i + c) * half, half)],
                    res_out.at[t % 2, pl.ds(c * half, half)],
                    row_sem,
                )
                store.start()
                store.wait()

            @pl.when(jnp.logical_not(row_home(i)))
            def _():
                out_copy(i).start()

        def branch_back_block(i):
            rows = pl.ds(i * BLOCK, BLOCK)
            grad = residual_rows[rows, :] + swapped(2, i)
            normal = n1_rows[rows, :]
            tally(6, grad * normal)
            tally(9, grad)
            residual = norm_pull(grad * value_row(0), normal, inv_rows[rows, 0:1])
            residual_rows[rows, :] = residual
            low_grad = residual.astype(BF)
            branch_rows[rows, :] = low_grad
            tally(8, low_grad.astype(F32))
            do_ref[rows, :] = jnp.dot(
                branch_rows[rows, :], out_both[...], preferred_element_type=F32
            ).astype(BF)

        def outer(left, j, right):
            return dot_tn(left[:, pl.ds(j * BLOCK, BLOCK)], right).astype(BF)

        def down_grad(z, j):
            wd[z, pl.ds(j * BLOCK, BLOCK), :] = outer(feed_rows, j, active[z])

        def up_grad(z, j):
            wu[z, pl.ds(j * BLOCK, BLOCK), :] = outer(low_rows, j, upper[z])

        def out_grad(j):
            both = outer(branch_rows, j, o_ref[...])
            for z in range(2):
                wo[z, pl.ds(j * BLOCK, BLOCK), :] = both[:, z * part_cols : (z + 1) * part_cols]

        def attention(pair, kb):
            if kb == 0:
                back_start(pair, o_ref, do_ref, dots, acc)
            back_block(
                pair, kb, q_ref, k_ref, v_ref, lt_ref, do_ref, dots, acc, dk, dv, limit_ref[0:1, 0:1]
            )
            if kb == blocks - 1:
                dq[:, pl.ds(pair * 128, 128)] = (acc[...] * DH**-0.5).astype(BF)

        def mate_copy(i):
            return remote(
                sent.at[pl.ds(i * half, half)],
                mate_got.at[i],
                t_send.at[0, i],
                t_recv.at[0, i],
                mate,
                t,
            )

        def mix(i):
            rows = pl.ds(i * BLOCK, BLOCK)
            kinds = [ref[rows, :] for ref in (dq, dk, dv)]
            share = jnp.zeros((BLOCK, width), F32)
            for z in range(2):
                both = jnp.concatenate(
                    [v[:, z * part_cols : (z + 1) * part_cols] for v in kinds], axis=1
                )
                mixed[z, rows, 0 : 3 * part_cols] = both
                share = share + dot_nt(both, wq[z])
            acc_rows[...] = share
            sent[pl.ds(i * half, half), :] = acc_rows[pl.ds((1 - c) * half, half), :].astype(BF)
            residual_rows[pl.ds((2 * i + c) * half, half), :] += acc_rows[pl.ds(c * half, half), :]
            mate_copy(i).start()

        def row_copy(i):
            return remote(
                low_rows.at[pl.ds(i * half, half)],
                tgr_out.at[t % 2, pl.ds(c * half, half)],
                t_send.at[1, i],
                t_recv.at[1, 2 * (t % 2) + c],
                2 * k + t // 2,
                i,
            )

        def send_rows(i):
            mate_copy(i).wait_recv()
            low_rows[pl.ds(i * half, half), :] = (
                residual_rows[pl.ds((2 * i + c) * half, half), :] + mate_got[i].astype(F32)
            ).astype(BF)
            here = row_home(i)

            @pl.when(here)
            def _():
                store = pltpu.make_async_copy(
                    low_rows.at[pl.ds(i * half, half)], tgr_out.at[t % 2, pl.ds(c * half, half)], row_sem
                )
                store.start()
                store.wait()

            @pl.when(jnp.logical_not(here))
            def _():
                row_copy(i).start()

        def settle_rows():
            for i in range(4):
                mate_copy(i).wait_send()

                @pl.when(jnp.logical_not(jnp.logical_and(i == t, c == t // 2)))
                def _():
                    row_copy(i).wait_send()

            for m in range(2):
                for core in range(2):
                    spot = tgr_out.at[m, pl.ds(core * half, half)]

                    @pl.when(jnp.logical_not(jnp.logical_and(2 * c + m == t, core == c)))
                    def _():
                        remote(
                            low_rows.at[pl.ds(0, half)],
                            spot,
                            t_send.at[1, 0],
                            t_recv.at[1, 2 * m + core],
                            mate,
                            t,
                        ).wait_recv()

        def weight_grad(j):
            rows = pl.ds(j * BLOCK, BLOCK)
            for z in range(2):
                wq[z, rows, :] = outer(x_rows, j, mixed[z, :, 0 : 3 * part_cols])

        def tile_copy(stage, goal_dp, goal_t, slot):
            return remote(
                tile_sum.at[stage],
                tile_got.at[slot],
                s_send.at[slot],
                s_recv.at[slot],
                goal_dp,
                goal_t,
            )

        def tile_start():
            for row, ref in ((0, dq), (2, dv)):
                sums = jnp.sum(ref[...].astype(F32), axis=0, keepdims=True)
                for z in range(2):
                    tile_sum[0, row + z : row + z + 1, 0:part_cols] = sums[
                        :, z * part_cols : (z + 1) * part_cols
                    ]
            tile_copy(0, dx, t, 0).start()

        def tile_second():
            tile_copy(0, dx, t, 0).wait_recv()
            tile_sum[1] = tile_sum[0] + tile_got[0]
            tile_copy(1, dy, t, 1).start()

        def tile_third():
            tile_copy(1, dy, t, 1).wait_recv()
            tile_sum[2] = tile_sum[1] + tile_got[1]
            for step in range(1, 4):
                tile_copy(2, d, (t + step) % 4, 1 + step).start()

        def tile_fourth():
            for step in range(1, 4):
                tile_copy(2, d, t, 1 + step).wait_recv()
            tile_sum[3] = (tile_sum[2] + tile_got[2]) + (tile_got[3] + tile_got[4])
            tile_copy(3, mate, t, 5).start()

        def tile_last():
            tile_copy(3, mate, t, 5).wait_recv()
            tile_own[...] = tile_sum[3]
            tile_mate[...] = tile_got[5]
            for slot, stage in enumerate((0, 1, 2, 2, 2, 3)):
                tile_copy(stage, mate, t, slot).wait_send()

        levels = [level_first, level_second, level_line, level_pass, level_near, level_mate]
        for copy in loads:
            copy.start()
        unpack()
        tile_sum[0] = jnp.zeros(tile_sum.shape[1:], F32)
        loads[0].wait()
        out_both[...] = jnp.concatenate([wo[0], wo[1]], axis=1)
        pl.loop(0, blocks)(branch_block)
        for copy in loads[1:4]:
            copy.wait()
        pl.loop(0, blocks)(forward_block)
        loads[4].wait()
        pl.loop(0, blocks)(output_block)
        loads[5].wait()
        pl.loop(0, width // BLOCK)(lambda j: [down_grad(z, j) for z in range(2)] and None)
        level_first(0)
        level_first(1)
        pl.loop(0, width // BLOCK)(lambda j: [up_grad(z, j) for z in range(2)] and None)
        level_first(2)
        pl.loop(0, blocks)(branch_back_block)
        pl.loop(0, width // BLOCK)(out_grad)
        work = [
            partial(attention, pair, kb)
            for pair in range(heads_width // 128)
            for kb in range(blocks)
        ]
        work += [partial(mix, i) for i in range(blocks)]
        work += [partial(weight_grad, j) for j in range(width // BLOCK)]
        done = 0
        for slot in range(n_chunks + 5):
            if slot < n_chunks - 1:
                upto = -(-len(work) * (slot + 1) // (n_chunks - 1))
                for unit in work[done:upto]:
                    unit()
                done = upto
            if slot == n_chunks - 2:
                tile_start()
            for lag, level in enumerate(levels):
                i = slot + (2 if lag == 0 else 1) - lag
                if lag == 0:
                    i = {0: 3, 1: 4, n_chunks - 2: n_chunks - 1}.get(slot, -1)
                if 0 <= i < n_chunks:
                    level(i)
            if slot == n_chunks - 2:
                for i in range(4):
                    send_rows(i)
            if slot >= n_chunks - 1:
                tail = slot - (n_chunks - 1)
                if tail < 4:
                    (tile_second, tile_third, tile_fourth, tile_last)[tail]()
        for i in range(4):

            @pl.when(jnp.logical_not(row_home(i)))
            def _():
                out_copy(i).wait_send()

        for m in range(2):
            for core in range(2):
                spot = res_out.at[m, pl.ds(core * half, half)]

                @pl.when(jnp.logical_not(jnp.logical_and(2 * c + m == t, core == c)))
                def _():
                    remote(
                        res_rows.at[pl.ds(0, half)],
                        spot,
                        ex_send.at[0, 0],
                        ex_recv.at[0, m, core],
                        mate,
                        t,
                    ).wait_recv()

        settle_rows()
        for i in range(n_chunks):
            for copy in first_copies(i):
                copy.wait_send()

            @pl.when(u >= 2)
            def _():
                for copy in second_copies(i):
                    copy.wait_send()
                for b in range(2):
                    z_copy(i, b).wait_send()

            @pl.when(u == 1)
            def _():
                z_copy(i, 0).wait_send()

            @pl.when(u == 0)
            def _():
                y_copy(i).wait_send()

            @pl.when(u <= 1)
            def _():
                p_copy(i).wait_send()

    any_spec = pl.BlockSpec(memory_space=pl.ANY)
    vmem = pl.BlockSpec(memory_space=pltpu.VMEM)
    dma = pltpu.SemaphoreType.DMA
    scratch = []
    for kind in range(8):
        for s in range(count):
            rows, cols, kept = rows_of[s], grads[s].shape[2], grads[s].dtype
            shape, dtype = (
                ((2, 4 * rows, cols), kept),
                ((2, 4 * rows, cols), kept),
                ((2, 2 * rows, cols), kept),
                ((2, 2 * rows, cols), F32),
                ((2, 2 * rows, cols), kept),
                ((2, 2 * rows, cols), kept),
                ((2 * rows, cols), kept),
                ((rows, cols), kept),
            )[kind]
            scratch.append(pltpu.VMEM(shape, dtype))
    back = jax.ShapeDtypeStruct((2, 2 * half, width), output.dtype)
    tiles = jax.ShapeDtypeStruct((16, hidden), F32)
    outs = pl.pallas_call(
        kernel,
        out_shape=[
            back,
            back,
            tiles,
            tiles,
            *[jax.ShapeDtypeStruct((r, g.shape[2]), F32) for r, g in zip(rows_of, grads)],
        ],
        in_specs=[any_spec] * (2 + count) + [vmem] * 8,
        out_specs=[any_spec, any_spec] + [vmem] * (2 + count),
        scratch_shapes=[
            *scratch,
            dma,
            dma((1, 4)),
            dma((1, 2, 2)),
            dma((n_chunks, 3)),
            dma((n_chunks, 3)),
            dma((n_chunks, 2)),
            dma((n_chunks, 2)),
            dma((n_chunks, 2)),
            dma((n_chunks, 2)),
            dma((n_chunks,)),
            dma((n_chunks,)),
            dma((n_chunks,)),
            dma((n_chunks,)),
            *[pltpu.VMEM(w.shape, BF) for w in weights],
            pltpu.VMEM((length, width), BF),
            pltpu.VMEM((length, width), BF),
            pltpu.VMEM((32 * SMALL, 128), F32),
            pltpu.VMEM((8, width), F32),
            pltpu.VMEM((width, heads_width), BF),
            pltpu.VMEM((length, width), F32),
            pltpu.VMEM((length, 128), F32),
            pltpu.VMEM((length, width), F32),
            pltpu.VMEM((length, width), BF),
            pltpu.VMEM((length, width), BF),
            pltpu.VMEM((length, width), BF),
            pltpu.VMEM((length, width), BF),
            pltpu.VMEM((length, width), BF),
            pltpu.VMEM((3, length, width), BF),
            pltpu.VMEM((2, length, hidden), BF),
            pltpu.VMEM((2, length, hidden), BF),
            pltpu.VMEM((length, heads_width), BF),
            pltpu.VMEM((8, length), F32),
            pltpu.VMEM((length, 128), F32),
            pltpu.VMEM((BLOCK, width), F32),
            pltpu.VMEM((4, half, width), BF),
            dma((6,)),
            dma((3, blocks)),
            dma((3, blocks)),
            dma((6,)),
            dma((6,)),
            dma((2, 4)),
            dma((2, 4)),
            pltpu.VMEM((4, *tiles.shape), F32),
            pltpu.VMEM((6, *tiles.shape), F32),
        ],
        compiler_params=pltpu.CompilerParams(
            collective_id=2, has_side_effects=True, vmem_limit_bytes=67043328
        ),
    )(x, cot, *weights, *heads, totals, limit, small_own, small_other)
    return outs[0], outs[1], outs[2], outs[3], outs[4:]


BLOCK = 256


def lane_half(shape, h):
    lane = lax.broadcasted_iota(jnp.int32, shape, 1)
    return lane < DH if h == 0 else lane >= DH


def reach(row_block, blocks):
    return max(row_block + 1, blocks // 2)


def dot_nt(a, b):
    return lax.dot_general(a, b, (((1,), (1,)), ((), ())), preferred_element_type=F32)


def dot_tn(a, b):
    return lax.dot_general(a, b, (((0,), (0,)), ((), ())), preferred_element_type=F32)


def attend_rows(q_ref, k_ref, v_ref, o_ref, lt_ref, limit, pair, qb):
    length = q_ref.shape[0]
    blocks = length // BLOCK
    lanes = pl.ds(pair * 128, 128)
    rows = pl.ds(qb * BLOCK, BLOCK)
    span = reach(qb, blocks) * BLOCK
    q = q_ref[rows, lanes] * jnp.asarray(DH**-0.5, BF)
    heads = []
    for h in range(2):
        half = lane_half((BLOCK, 128), h)
        s = dot_nt(jnp.where(half, q, jnp.zeros_like(q)), k_ref[pl.ds(0, span), lanes])
        clear = qb * BLOCK
        row = lax.broadcasted_iota(jnp.int32, (BLOCK, span - clear), 0) + clear
        col = lax.broadcasted_iota(jnp.int32, (BLOCK, span - clear), 1) + clear
        seen = col <= row
        if clear < length // 2:
            seen = jnp.logical_or(seen, col.astype(F32) < limit)
        tail = jnp.where(seen, s[:, clear:], MASKED_SCORE)
        s = jnp.concatenate([s[:, :clear], tail], axis=1) if clear else tail
        top = jnp.max(s, axis=1, keepdims=True)
        p = jnp.exp(s - top)
        total = jnp.sum(p, axis=1, keepdims=True)
        log_total = top + jnp.log(total)
        lt_ref[2 * pair + h, 0:1, rows] = jnp.transpose(
            jnp.broadcast_to(log_total, (BLOCK, 128))
        )[0:1, :]
        p = (p * (1.0 / total)).astype(BF)
        heads.append(jnp.dot(p, v_ref[pl.ds(0, span), lanes], preferred_element_type=F32))
    o_ref[rows, lanes] = jnp.where(lane_half((BLOCK, 128), 0), heads[0], heads[1]).astype(BF)


def back_start(pair, o_ref, do_ref, dots, acc):
    head_row = lax.broadcasted_iota(jnp.int32, (8, 128), 0)
    lane = lax.broadcasted_iota(jnp.int32, (8, 128), 1)
    pick = (lane // DH == head_row).astype(F32)
    lanes = pl.ds(pair * 128, 128)
    dots[...] = lax.dot_general(
        pick,
        do_ref[:, lanes].astype(F32) * o_ref[:, lanes].astype(F32),
        (((1,), (1,)), ((), ())),
        precision=lax.Precision.HIGHEST,
        preferred_element_type=F32,
    )
    acc[...] = jnp.zeros_like(acc)


def back_block(pair, kb, q_ref, k_ref, v_ref, lt_ref, do_ref, dots, acc, dk_ref, dv_ref, limit):
    length = q_ref.shape[0]
    blocks = length // BLOCK
    lanes = pl.ds(pair * 128, 128)
    keys_at = pl.ds(kb * BLOCK, BLOCK)
    key = k_ref[keys_at, lanes]
    value = v_ref[keys_at, lanes]
    zero = jnp.zeros((BLOCK, 128), BF)
    dk = jnp.zeros((BLOCK, 128), F32)
    dv = jnp.zeros((BLOCK, 128), F32)
    for qb in range(blocks):
        if kb >= reach(qb, blocks):
            continue
        rows = pl.ds(qb * BLOCK, BLOCK)
        q_pair = q_ref[rows, lanes] * jnp.asarray(DH**-0.5, BF)
        do_pair = do_ref[rows, lanes]
        for h in range(2):
            half = lane_half((BLOCK, 128), h)
            q = jnp.where(half, q_pair, zero)
            do = jnp.where(half, do_pair, zero)
            s = dot_nt(key, q)
            if kb >= qb:
                key_id = lax.broadcasted_iota(jnp.int32, (BLOCK, BLOCK), 0) + kb * BLOCK
                row_id = lax.broadcasted_iota(jnp.int32, (BLOCK, BLOCK), 1) + qb * BLOCK
                seen = key_id <= row_id
                if kb * BLOCK < length // 2:
                    seen = jnp.logical_or(seen, key_id.astype(F32) < limit)
                s = jnp.where(seen, s, MASKED_SCORE)
            p = jnp.exp(s - lt_ref[2 * pair + h, 0:1, rows])
            dp = dot_nt(value, do)
            ds = (p * (dp - dots[h : h + 1, rows])).astype(BF)
            dv = dv + jnp.dot(p.astype(BF), do, preferred_element_type=F32)
            dk = dk + jnp.dot(ds, q, preferred_element_type=F32)
            acc[rows, :] += dot_tn(ds, jnp.where(half, key, zero))
    dk_ref[keys_at, lanes] = dk.astype(BF)
    dv_ref[keys_at, lanes] = dv.astype(BF)


def chip_local(
    tokens, prefix_len, w_qkv, bias_qv, w_out, w_up, bias_up, w_down, gains, shifts, cotangent
):
    d, t, k, c, _, _, _, _ = place()
    part = w_qkv.shape[2]
    hidden = w_up.shape[1]

    def lanes(v):
        return jnp.pad(v, ((0, 0), (0, 128 - v.shape[1])))

    limits = jnp.concatenate([prefix_len // 16, prefix_len % 16]).astype(BF)[None]
    small = jnp.concatenate(
        [lanes(v) for v in (bias_qv, bias_up[None], gains, shifts, limits)], axis=0
    )
    small = jnp.pad(small, ((0, SMALL - small.shape[0]), (0, 0)))
    shards = (
        w_qkv.reshape(ROWS, 3 * part),
        w_out.T,
        w_up,
        w_down.T,
        small,
    )
    half = hidden // 2
    chunks = (
        (4, 0, 128),
        (0, 0, 3 * part),
        (1, 0, part),
        (2, 0, half),
        (2, half, half),
        (3, 0, half),
        (3, half, half),
    )
    x, cot, (g_qkv, g_out, g_up, g_down, g_small), small_other, heads = gather_attend(
        tokens, cotangent, shards, chunks, bias_qv.shape[1]
    )
    queries, key_heads, value_heads, context, totals, limit = heads

    per = bias_qv.shape[1]
    back_chunks = (
        (3, 0, half),
        (3, half, half),
        (2, 0, half),
        (2, half, half),
        (1, 0, part),
        (0, 0, 3 * part),
    )
    out_rows, token_rows, tile_own, tile_mate, finals = layer_back(
        x,
        cot,
        (g_qkv, g_out, g_up, g_down),
        (queries, key_heads, value_heads, context),
        totals,
        limit,
        g_small,
        small_other,
        per,
        back_chunks,
    )
    plane_rows = jnp.where(c == t // 2, tile_own, tile_mate)[:6].reshape(3, 2, hidden)
    plane_rows = lax.dynamic_index_in_dim(plane_rows, t % 2, 1, False)
    mine_rows = lax.dynamic_slice(tile_own, (6, (4 * d + t) * per), (6, per))
    return (
        out_rows,
        token_rows.astype(F32),
        finals[0].reshape(w_qkv.shape),
        lax.dynamic_slice(plane_rows, (0, d * per), (2, per)),
        finals[1].T,
        finals[2],
        lax.dynamic_slice(plane_rows, (2, d * bias_up.shape[0]), (1, bias_up.shape[0]))[0],
        finals[3].T,
        mine_rows[:2],
        mine_rows[2:],
    )


def solution(mesh):
    return jax.shard_map(
        chip_local if dict(mesh.shape) == {"dp": 8, "tensor": 4} else local,
        mesh=mesh,
        in_specs=(
            P("dp", "tensor", None),
            P("dp"),
            P("dp", None, "tensor"),
            P(None, ("tensor", "dp")),
            P("tensor", "dp"),
            P("dp", "tensor"),
            P(("tensor", "dp")),
            P("tensor", "dp"),
            P(None, ("dp", "tensor")),
            P(None, ("dp", "tensor")),
            P("dp", "tensor", None),
        ),
        out_specs=(
            P("dp", "tensor", None),
            P("dp", "tensor", None),
            P("dp", None, "tensor"),
            P(None, ("tensor", "dp")),
            P("tensor", "dp"),
            P("dp", "tensor"),
            P(("tensor", "dp")),
            P("tensor", "dp"),
            P(None, ("dp", "tensor")),
            P(None, ("dp", "tensor")),
        ),
        check_vma=False,
    )
```

```python
import math
import types
from functools import partial

import jax
import jax.numpy as jnp
from jax import lax
from jax.experimental import pallas as pl
from jax.experimental.pallas import tpu as pltpu
from jax.sharding import PartitionSpec as P

DH = 64


EPSILON = 1e-05
MASKED_SCORE = -1e30


def norm_forward(values, gain_row, shift_row):
    center = values - jnp.mean(values, axis=-1, keepdims=True)
    inverse = lax.rsqrt(jnp.mean(center * center, axis=-1, keepdims=True) + EPSILON)
    normal = center * inverse
    return (normal * gain_row + shift_row, normal, inverse)


def norm_backward(incoming, normal, inverse, gain_row):
    scaled = incoming * gain_row
    first_mean = jnp.mean(scaled, axis=-1, keepdims=True)
    second_mean = jnp.mean(scaled * normal, axis=-1, keepdims=True)
    outgoing = inverse * (scaled - first_mean - normal * second_mean)
    return (outgoing, jnp.sum(incoming * normal, axis=0), jnp.sum(incoming, axis=0))


def visible_mask(offset, block_rows, length, prefix):
    row_ids = offset + jnp.arange(block_rows, dtype=jnp.int32)[:, None]
    column_ids = jnp.arange(length, dtype=jnp.int32)[None, :]
    return jnp.logical_or(column_ids < prefix, column_ids <= row_ids)


def block_scores(chosen, key_heads, offset, prefix, scaling):
    length = key_heads.shape[0]
    allowed = visible_mask(offset, chosen.shape[0], length, prefix)
    scores = (
        jnp.einsum("qhd,khd->hqk", chosen, key_heads, preferred_element_type=jnp.float32) * scaling
    )
    return jnp.where(allowed[None], scores, MASKED_SCORE)


def attention_forward(queries, key_heads, value_heads, prefix):
    length = key_heads.shape[0]
    block_rows = min(512, length)
    scaling = queries.shape[-1] ** (-0.5)
    outputs = []
    totals = []
    for offset in range(0, length, block_rows):
        scores = block_scores(
            queries[offset : offset + block_rows], key_heads, offset, prefix, scaling
        )
        row_max = jnp.max(scores, axis=-1, keepdims=True)
        log_total = jnp.log(jnp.sum(jnp.exp(scores - row_max), axis=-1, keepdims=True)) + row_max
        attn_probs = jnp.exp(scores - log_total).astype(jnp.bfloat16)
        outputs.append(
            jnp.einsum("hqk,khd->qhd", attn_probs, value_heads, preferred_element_type=jnp.float32)
        )
        totals.append(log_total)
    return (jnp.concatenate(outputs, axis=0), totals)


def attention_backward(queries, key_heads, value_heads, prefix, totals, context_grad):
    length = key_heads.shape[0]
    block_rows = min(512, length)
    scaling = queries.shape[-1] ** (-0.5)
    query_parts = []
    key_grad = jnp.zeros(key_heads.shape, jnp.float32)
    value_grad = jnp.zeros(value_heads.shape, jnp.float32)
    for number, offset in enumerate(range(0, length, block_rows)):
        chosen = queries[offset : offset + block_rows]
        grad_block = context_grad[offset : offset + block_rows]
        scores = block_scores(chosen, key_heads, offset, prefix, scaling)
        attn_probs = jnp.exp(scores - totals[number])
        probs_low = attn_probs.astype(jnp.bfloat16)
        probs_grad = jnp.einsum(
            "qhd,khd->hqk", grad_block, value_heads, preferred_element_type=jnp.float32
        )
        row_dot = jnp.sum(attn_probs * probs_grad, axis=-1, keepdims=True)
        scores_grad = (attn_probs * (probs_grad - row_dot)).astype(jnp.bfloat16)
        query_parts.append(
            jnp.einsum("hqk,khd->qhd", scores_grad, key_heads, preferred_element_type=jnp.float32)
            * scaling
        )
        key_grad = (
            key_grad
            + jnp.einsum("hqk,qhd->khd", scores_grad, chosen, preferred_element_type=jnp.float32)
            * scaling
        )
        value_grad = value_grad + jnp.einsum(
            "hqk,qhd->khd", probs_low, grad_block, preferred_element_type=jnp.float32
        )
    return (jnp.concatenate(query_parts, axis=0), key_grad, value_grad)


def local(
    tokens, prefix_len, w_qkv, bias_qv, w_out, w_up, bias_up, w_down, gains, shifts, cotangent
):
    tensor_count = lax.axis_size("tensor")
    seq_local, shard_rows, model_width = tokens.shape
    length = shard_rows * tensor_count
    full_qkv, full_bias_qv, full_out, full_up, full_bias_up, full_down = (
        lax.all_gather(w_qkv, "dp", axis=0, tiled=True),
        lax.all_gather(bias_qv, "dp", axis=1, tiled=True),
        lax.all_gather(w_out, "dp", axis=1, tiled=True),
        lax.all_gather(w_up, "dp", axis=0, tiled=True),
        lax.all_gather(bias_up, "dp", axis=0, tiled=True),
        lax.all_gather(w_down, "dp", axis=1, tiled=True),
    )
    full_gains, full_shifts = (
        lax.all_gather(gains, ("dp", "tensor"), axis=1, tiled=True),
        lax.all_gather(shifts, ("dp", "tensor"), axis=1, tiled=True),
    )
    full_gains = full_gains.astype(jnp.float32)
    full_shifts = full_shifts.astype(jnp.float32)
    bias_values = full_bias_qv.astype(jnp.float32)
    up_bias = full_bias_up.astype(jnp.float32)
    local_width = full_qkv.shape[2]
    head_count = local_width // DH
    kept_state = []
    outputs = []
    for member in range(seq_local):
        token_rows = tokens[member]
        prefix = prefix_len[member]

        def fold_tokens(piece):
            product = jnp.einsum("rd,dce->rce", piece, full_qkv, preferred_element_type=jnp.float32)
            return (piece, product)

        token_full, projected = fold_tokens(
            lax.all_gather(token_rows, "tensor", axis=0, tiled=True)
        )
        queries = (
            (projected[:, 0] + bias_values[0]).astype(jnp.bfloat16).reshape(length, head_count, DH)
        )
        key_heads = projected[:, 1].astype(jnp.bfloat16).reshape(length, head_count, DH)
        value_heads = (
            (projected[:, 2] + bias_values[1]).astype(jnp.bfloat16).reshape(length, head_count, DH)
        )
        context, totals = attention_forward(queries, key_heads, value_heads, prefix)
        context_low = context.reshape(length, local_width).astype(jnp.bfloat16)
        branch = (
            lax.psum_scatter(
                jnp.dot(context_low, full_out, preferred_element_type=jnp.float32).astype(
                    jnp.bfloat16
                ),
                "tensor",
                scatter_dimension=0,
                tiled=True,
            ).astype(jnp.float32)
            + full_shifts[0]
        )
        normed, normal_one, inverse_one = norm_forward(
            token_rows.astype(jnp.float32) + branch, full_gains[0], full_shifts[1]
        )
        normed_low = normed.astype(jnp.bfloat16)

        def fold_normed(piece):
            product = jnp.dot(piece, full_up, preferred_element_type=jnp.float32)
            return (piece, product)

        normed_full, pre_active = fold_normed(
            lax.all_gather(normed_low, "tensor", axis=0, tiled=True)
        )
        pre_active = pre_active + up_bias
        active_low = jax.nn.gelu(pre_active, approximate=False).astype(jnp.bfloat16)
        feed_out = (
            lax.psum_scatter(
                jnp.dot(active_low, full_down, preferred_element_type=jnp.float32).astype(
                    jnp.bfloat16
                ),
                "tensor",
                scatter_dimension=0,
                tiled=True,
            ).astype(jnp.float32)
            + full_shifts[2]
        )
        result, normal_two, inverse_two = norm_forward(
            normed + feed_out, full_gains[1], full_shifts[3]
        )
        outputs.append(result.astype(jnp.bfloat16))
        kept_state.append(
            (
                token_rows,
                prefix,
                token_full,
                queries,
                key_heads,
                value_heads,
                totals,
                context_low,
                normal_one,
                inverse_one,
                normed_full,
                pre_active,
                active_low,
                normal_two,
                inverse_two,
            )
        )
    back_qkv, back_out, back_up, back_down = (
        lax.all_gather(w_qkv, "dp", axis=0, tiled=True),
        lax.all_gather(w_out, "dp", axis=1, tiled=True),
        lax.all_gather(w_up, "dp", axis=0, tiled=True),
        lax.all_gather(w_down, "dp", axis=1, tiled=True),
    )
    full_shapes = (
        full_qkv.shape,
        full_bias_qv.shape,
        full_out.shape,
        full_up.shape,
        full_bias_up.shape,
        full_down.shape,
    )
    weight_grads = tuple((jnp.zeros(array_shape, jnp.float32) for array_shape in full_shapes))
    gain_grads = jnp.zeros((2, model_width), jnp.float32)
    shift_grads = jnp.zeros((4, model_width), jnp.float32)
    input_grads = []
    for member in range(seq_local):
        (
            token_rows,
            prefix,
            token_full,
            queries,
            key_heads,
            value_heads,
            totals,
            context_low,
            normal_one,
            inverse_one,
            normed_full,
            pre_active,
            active_low,
            normal_two,
            inverse_two,
        ) = kept_state[member]
        incoming = cotangent[member].astype(jnp.float32)
        residual_two, gain_two, shift_two = norm_backward(
            incoming, normal_two, inverse_two, full_gains[1]
        )
        feed_grad = residual_two.astype(jnp.bfloat16)
        fold_piece = lax.all_gather(feed_grad, "tensor", axis=0, tiled=True)
        down_grad = jnp.einsum(
            "rf,rd->fd", active_low, fold_piece, preferred_element_type=jnp.float32
        )
        fold_product = jnp.einsum(
            "rd,fd->rf", fold_piece, back_down, preferred_element_type=jnp.float32
        )
        active_grad = fold_product
        down_grad, active_grad = (down_grad, active_grad)
        layer_value, gelu_pull = jax.vjp(partial(jax.nn.gelu, approximate=False), pre_active)
        upper_grad = gelu_pull(active_grad)[0].astype(jnp.bfloat16)
        normed_grad = residual_two + lax.psum_scatter(
            jnp.einsum("rf,df->rd", upper_grad, back_up, preferred_element_type=jnp.float32).astype(
                jnp.bfloat16
            ),
            "tensor",
            scatter_dimension=0,
            tiled=True,
        ).astype(jnp.float32)
        up_grad = jnp.einsum(
            "ld,lf->df", normed_full, upper_grad, preferred_element_type=jnp.float32
        )
        up_bias_grad = jnp.sum(upper_grad.astype(jnp.float32), axis=0)
        residual_one, gain_one, shift_one = norm_backward(
            normed_grad, normal_one, inverse_one, full_gains[0]
        )
        branch_grad = residual_one.astype(jnp.bfloat16)

        def fold_branch(piece):
            out_grad = jnp.einsum(
                "rk,rd->kd", context_low, piece, preferred_element_type=jnp.float32
            )
            product = jnp.einsum("rd,kd->rk", piece, back_out, preferred_element_type=jnp.float32)
            return (out_grad, product)

        out_grad, context_grad = fold_branch(
            lax.all_gather(branch_grad, "tensor", axis=0, tiled=True)
        )
        context_grad = context_grad.astype(jnp.bfloat16).reshape(length, head_count, DH)
        query_grad, key_grad, value_grad = attention_backward(
            queries, key_heads, value_heads, prefix, totals, context_grad
        )
        mixed_grad = (
            jnp.stack([query_grad, key_grad, value_grad], axis=1)
            .astype(jnp.bfloat16)
            .reshape(length, 3, local_width)
        )
        qkv_grad = jnp.einsum(
            "ld,lce->dce", token_full, mixed_grad, preferred_element_type=jnp.float32
        )
        row_sums = jnp.sum(mixed_grad.astype(jnp.float32), axis=0)
        bias_grad = jnp.stack([row_sums[0], row_sums[2]])
        token_grad = residual_one + lax.psum_scatter(
            jnp.einsum(
                "rce,dce->rd", mixed_grad, back_qkv, preferred_element_type=jnp.float32
            ).astype(jnp.bfloat16),
            "tensor",
            scatter_dimension=0,
            tiled=True,
        ).astype(jnp.float32)
        input_grads.append(token_grad)
        gain_grads = gain_grads + jnp.stack([gain_one, gain_two])
        shift_grads = shift_grads + jnp.stack(
            [
                jnp.sum(branch_grad.astype(jnp.float32), axis=0),
                shift_one,
                jnp.sum(feed_grad.astype(jnp.float32), axis=0),
                shift_two,
            ]
        )
        member_grads = (qkv_grad, bias_grad, out_grad, up_grad, up_bias_grad, down_grad)
        weight_grads = tuple(
            (running + grad_part for running, grad_part in zip(weight_grads, member_grads))
        )
    total_qkv, total_bias, total_out, total_up, total_up_bias, total_down = weight_grads
    weight_grads = (
        lax.psum_scatter(total_qkv, "dp", scatter_dimension=0, tiled=True),
        lax.psum_scatter(total_bias, "dp", scatter_dimension=1, tiled=True),
        lax.psum_scatter(total_out, "dp", scatter_dimension=1, tiled=True),
        lax.psum_scatter(total_up, "dp", scatter_dimension=0, tiled=True),
        lax.psum_scatter(total_up_bias, "dp", scatter_dimension=0, tiled=True),
        lax.psum_scatter(total_down, "dp", scatter_dimension=1, tiled=True),
    )
    gain_share, shift_share = (
        lax.psum_scatter(gain_grads, ("dp", "tensor"), scatter_dimension=1, tiled=True),
        lax.psum_scatter(shift_grads, ("dp", "tensor"), scatter_dimension=1, tiled=True),
    )
    return (
        jnp.stack(outputs),
        jnp.stack(input_grads),
        weight_grads[0],
        weight_grads[1],
        weight_grads[2],
        weight_grads[3],
        weight_grads[4],
        weight_grads[5],
        gain_share,
        shift_share,
    )


MESH_ID = pl.DeviceIdType.MESH
BF = jnp.bfloat16
F32 = jnp.float32
ROWS = 96
SMALL = 16


def place():
    d = lax.axis_index("dp")
    t = lax.axis_index("tensor")
    k, c = d // 2, d % 2
    xb, yb = k % 2, k // 2
    dx = d + 2 - 4 * xb
    dy = d + 4 - 8 * yb
    return d, t, k, c, xb, yb, dx, dy


def remote(src, dst, send, recv, dp, tensor):
    return pltpu.make_async_remote_copy(
        src_ref=src,
        dst_ref=dst,
        send_sem=send,
        recv_sem=recv,
        device_id=(dp, tensor),
        device_id_type=MESH_ID,
    )


def enter(k, c, t, d, dx, dy):
    barrier = pltpu.get_barrier_semaphore()

    def greet(dp, tensor):
        pl.semaphore_signal(barrier, inc=1, device_id=(dp, tensor), device_id_type=MESH_ID)

    greet(dx, t)
    greet(dy, t)
    greet(d + 1 - 2 * c, t)
    for step in range(1, 4):
        other = (t + step) % 4
        greet(2 * k, other)
        greet(2 * k + 1, other)
    pl.semaphore_wait(barrier, 9)


def gather_steps(place_of, tok, cot, xf, cf, own, full, small_other, sems, chunks):
    d, t, k, c, xb, yb, dx, dy = place_of
    (
        local_sem,
        row_sem,
        ex_send,
        ex_recv,
        fw_send,
        fw_recv,
        p_send,
        p_recv,
        z_send,
        z_recv,
        a_send,
        a_recv,
        b_send,
        b_recv,
        o_send,
        o_recv,
    ) = sems
    mate = d + 1 - 2 * c
    u = t + c * (3 - 2 * t)
    up = t + 1 - 2 * c
    down = t - 1 + 2 * c
    source = t // 2 == c
    half = tok.shape[1] // 2
    rows_of = [w.shape[0] for w in own]

    def shard_spot(s, dp):
        rows = rows_of[s]
        return full[s].at[t % 2, pl.ds(dp * rows, rows)]

    def placed(s):
        @pl.when(source)
        def _():
            pltpu.make_async_copy(own[s], shard_spot(s, d), local_sem.at[s]).start()

        @pl.when(jnp.logical_not(source))
        def _():
            remote(own[s], shard_spot(s, d), p_send.at[s], p_recv.at[s], mate, t).start()

    def row_spot(dst, origin, core):
        return dst.at[pl.ds((origin * 2 + core) * half, half)]

    def exchange(which, src, dst, start=True):
        for m in range(2):
            goal = 2 * c + m
            for core in range(2):
                piece = src.at[m, pl.ds(core * half, half)]
                spot = row_spot(dst, t, core)
                here = jnp.logical_and(goal == t, core == c)
                copy = remote(
                    piece,
                    spot,
                    ex_send.at[which, 2 * m + core],
                    ex_recv.at[which, t],
                    2 * k + core,
                    goal,
                )
                local = pltpu.make_async_copy(piece, spot, row_sem.at[which])

                @pl.when(here)
                def _():
                    if start:
                        local.start()

                @pl.when(jnp.logical_not(here))
                def _():
                    if start:
                        copy.start()
                    else:
                        copy.wait_send()

    def forward(which, dst, origin, core):
        spot = row_spot(dst, origin, core)
        return remote(spot, spot, fw_send.at[which, origin], fw_recv.at[which, origin], mate, t)

    def relay(which, src, dst):
        for origin in range(4):
            spot = row_spot(dst, origin, c)
            here = jnp.logical_and(origin == t, c == t // 2)

            @pl.when(here)
            def _():
                pltpu.make_async_copy(
                    src.at[0, pl.ds(0, half)], spot, row_sem.at[which]
                ).wait()

            @pl.when(jnp.logical_not(here))
            def _():
                remote(
                    spot, spot, ex_send.at[which, 0], ex_recv.at[which, origin], mate, t
                ).wait_recv()

            forward(which, dst, origin, c).start()

    def arrived(which, dst):
        for origin in range(4):
            forward(which, dst, origin, 1 - c).wait_recv()

    def block(i, b, start, n):
        s, col, cols = chunks[i]
        rows = rows_of[s]
        return full[s].at[
            b + c * (1 - 2 * b), pl.ds(start * rows, n * rows), pl.ds(col, cols)
        ]

    def z_copy(i, b, way, target):
        ref = block(i, b, 2 * k, 2)
        return remote(ref, ref, z_send.at[i, b, way], z_recv.at[i, b], d, target)

    def first_copy(i, b):
        ref = block(i, b, 2 * k, 2)
        return remote(ref, ref, a_send.at[i, b], a_recv.at[i, b], dx if b == 0 else dy, t)

    def first_arrival(i, b):
        near = k + 1 - 2 * xb if b == 0 else k + 2 - 4 * yb
        ref = block(i, b, 2 * near, 2)
        return remote(ref, ref, a_send.at[i, b], a_recv.at[i, b], dx if b == 0 else dy, t)

    def second_copies(i, arriving):
        other = 1 if arriving else 0
        row = yb + other * (1 - 2 * yb)
        ref = block(i, 0, 4 * row, 4)
        col = xb + other * (1 - 2 * xb)
        out = [remote(ref, ref, b_send.at[i, 0], b_recv.at[i, 0], dy, t)]
        for r in range(2):
            ref = block(i, 1, 2 * (2 * r + col), 2)
            out.append(remote(ref, ref, b_send.at[i, 1 + r], b_recv.at[i, 1 + r], dx, t))
        return out

    def spread(i, b):
        @pl.when(jnp.logical_and(u >= b, u < 3))
        def _():
            z_copy(i, b, 0, up).start()

        if b == 1:

            @pl.when(u == 1)
            def _():
                z_copy(i, 1, 1, down).start()

        first_copy(i, b).start()

    waited = set()

    def level_own(i):
        s = chunks[i][0]
        if s not in waited:
            waited.add(s)

            @pl.when(source)
            def _():
                pltpu.make_async_copy(own[s], shard_spot(s, d), local_sem.at[s]).wait()
                twin = shard_spot(s, mate)
                remote(twin, twin, p_send.at[s], p_recv.at[s], mate, t).wait_recv()

        for b in range(2):

            @pl.when(u == b)
            def _():
                spread(i, b)

    def level_line(i):
        for b in (1, 0):

            @pl.when(u != b)
            def _():
                z_copy(i, b, 0, up).wait_recv()
                spread(i, b)

    def level_second(i):
        for b in range(2):
            first_arrival(i, b).wait_recv()
        for copy in second_copies(i, False):
            copy.start()

    def level_done(i):
        for copy in second_copies(i, True):
            copy.wait_recv()

    last = len(own) - 1
    swap = remote(full[last], small_other, o_send, o_recv, mate, t)

    def sent_all():
        for which, src, dst in ((0, tok, xf), (1, cot, cf)):
            for origin in range(4):
                forward(which, dst, origin, c).wait_send()
            exchange(which, src, dst, False)
        for s in range(len(own)):

            @pl.when(jnp.logical_not(source))
            def _():
                remote(own[s], shard_spot(s, d), p_send.at[s], p_recv.at[s], mate, t).wait_send()

        for i in range(len(chunks)):
            for b in range(2):

                @pl.when(jnp.logical_and(u >= b, u < 3))
                def _():
                    z_copy(i, b, 0, up).wait_send()

                first_copy(i, b).wait_send()

            @pl.when(u == 1)
            def _():
                z_copy(i, 1, 1, down).wait_send()

            for copy in second_copies(i, False):
                copy.wait_send()

    return types.SimpleNamespace(
        placed=placed,
        exchange=exchange,
        relay=relay,
        arrived=arrived,
        own=level_own,
        line=level_line,
        second=level_second,
        done=level_done,
        swap=swap,
        sent_all=sent_all,
    )


def gather_sems(shards, n_chunks):
    dma = pltpu.SemaphoreType.DMA
    return [
        dma((shards,)),
        dma((2,)),
        dma((2, 4)),
        dma((2, 4)),
        dma((2, 4)),
        dma((2, 4)),
        dma((shards,)),
        dma((shards,)),
        dma((n_chunks, 2, 2)),
        dma((n_chunks, 2)),
        dma((n_chunks, 2)),
        dma((n_chunks, 2)),
        dma((n_chunks, 3)),
        dma((n_chunks, 3)),
        dma,
        dma,
    ]


def gelu_parts(u):
    half = math.sqrt(0.5)
    e = jnp.exp(u * u * -0.5)
    f = 1.0 / (1.0 + (0.3275911 * half) * jnp.abs(u))
    series = 0.5 * 1.061405429 * f - 0.5 * 1.453152027
    series = series * f + 0.5 * 1.421413741
    series = series * f - 0.5 * 0.284496736
    series = series * f + 0.5 * 0.254829592
    tail = series * f * e
    share = jnp.where(u >= 0.0, 1.0 - tail, tail)
    return u * share, share + u * e * (1.0 / math.sqrt(2.0 * math.pi))


def layer(tokens, cotangent, shards, per, arrivals, chunks):
    weights = [jax.ShapeDtypeStruct((2, 8 * w.shape[0], w.shape[1]), BF) for w in shards[:-1]]
    part_cols = weights[0].shape[2] // 3
    heads_width = 2 * part_cols
    hidden = weights[2].shape[2]
    up_per = hidden // 8
    grads = weights
    length, width = 4 * tokens.shape[1], tokens.shape[2]
    count = len(grads)
    n_chunks = len(chunks)
    half = length // 8
    blocks = length // BLOCK
    rows_of = [g.shape[1] // 8 for g in grads]

    n_sems = len(gather_sems(1, 1))

    def kernel(*refs):
        tok, cot = refs[:2]
        own = refs[2 : 3 + count]
        base = 3 + count
        res_out, tgr_out, tile_own, tile_mate = refs[base : base + 4]
        final = refs[base + 4 : base + 4 + count]
        sems = refs[base + 4 + count : base + 4 + count + n_sems]
        base += 4 + count + n_sems
        got1 = refs[base : base + count]
        sum1 = refs[base + count : base + 2 * count]
        got2 = refs[base + 2 * count : base + 3 * count]
        sum2 = refs[base + 3 * count : base + 4 * count]
        got3 = refs[base + 4 * count : base + 5 * count]
        sum3 = refs[base + 5 * count : base + 6 * count]
        got4 = refs[base + 6 * count : base + 7 * count]
        got5 = refs[base + 7 * count : base + 8 * count]
        (
            row_sem,
            ex_send,
            ex_recv,
            a_send,
            a_recv,
            b_send,
            b_recv,
            z_send,
            z_recv,
            y_send,
            y_recv,
            p_send,
            p_recv,
            wq,
            wo,
            wu,
            wd,
            q_ref,
            k_ref,
            v_ref,
            o_ref,
            lt_ref,
            small_a,
            small_b,
            x_rows,
            cot_rows,
            small_rows,
            row_values,
            out_both,
            n1_rows,
            inv_rows,
            residual_rows,
            res_rows,
            low_rows,
            feed_rows,
            branch_rows,
            sent,
            got,
            active,
            upper,
            do_ref,
            dots,
            acc,
            acc_rows,
            mate_got,
            e_send,
            e_recv,
            s_send,
            s_recv,
            t_send,
            t_recv,
            tile_sum,
            tile_got,
        ) = refs[base + 8 * count :]
        part = (wq, wo, wu, wd)
        mixed = active
        dq, dk, dv = (
            upper.at[0, :, pl.ds(0, heads_width)],
            upper.at[0, :, pl.ds(heads_width, heads_width)],
            upper.at[1, :, pl.ds(0, heads_width)],
        )
        d, t, k, c, xb, yb, dx, dy = place()
        mate = d + 1 - 2 * c
        u = t + c * (3 - 2 * t)
        up = t + 1 - 2 * c
        down = t - 1 + 2 * c
        source = u <= 1
        enter(k, c, t, d, dx, dy)

        def plane(b):
            return b + c * (1 - 2 * b)

        def first_copies(i):
            s, col, cols = chunks[i]
            rows = rows_of[s]
            spot = pl.ds(col, cols)
            out = [
                remote(
                    part[s].at[plane(0), pl.ds((1 - yb) * 4 * rows, 4 * rows), spot],
                    got1[s].at[0, :, spot],
                    a_send.at[i, 0],
                    a_recv.at[i, 0],
                    dy,
                    t,
                )
            ]
            for r in range(2):
                out.append(
                    remote(
                        part[s].at[plane(1), pl.ds((2 * r + 1 - xb) * 2 * rows, 2 * rows), spot],
                        got1[s].at[1, pl.ds(r * 2 * rows, 2 * rows), spot],
                        a_send.at[i, 1 + r],
                        a_recv.at[i, 1 + r],
                        dx,
                        t,
                    )
                )
            return out

        def second_copies(i):
            s, col, cols = chunks[i]
            rows = rows_of[s]
            spot = pl.ds(col, cols)
            out = []
            for b, far, goal in ((0, 1 - xb, dx), (1, 1 - yb, dy)):
                out.append(
                    remote(
                        sum1[s].at[b, pl.ds(far * 2 * rows, 2 * rows), spot],
                        got2[s].at[b, :, spot],
                        b_send.at[i, b],
                        b_recv.at[i, b],
                        goal,
                        t,
                    )
                )
            return out

        def low(v, s):
            return v.astype(sum1[s].dtype)

        def level_first(i):
            for copy in first_copies(i):
                copy.start()

        def level_second(i):
            s, col, cols = chunks[i]
            rows = rows_of[s]
            spot = pl.ds(col, cols)
            for copy in first_copies(i):
                copy.wait_recv()
            mine = part[s][plane(0), pl.ds(yb * 4 * rows, 4 * rows), spot]
            sum1[s][0, :, spot] = low(mine.astype(F32) + got1[s][0, :, spot].astype(F32), s)
            for r in range(2):
                mine = part[s][plane(1), pl.ds((2 * r + xb) * 2 * rows, 2 * rows), spot]
                there = pl.ds(r * 2 * rows, 2 * rows)
                sum1[s][1, there, spot] = low(
                    mine.astype(F32) + got1[s][1, there, spot].astype(F32), s
                )
            for copy in second_copies(i):
                copy.start()

        def z_copy(i, b):
            s, col, cols = chunks[i]
            spot = pl.ds(col, cols)
            return remote(
                sum3[s].at[b, :, spot],
                got3[s].at[b, :, spot],
                z_send.at[i, b],
                z_recv.at[i, b],
                d,
                down,
            )

        def y_copy(i):
            s, col, cols = chunks[i]
            spot = pl.ds(col, cols)
            return remote(
                sum3[s].at[1, :, spot], got4[s].at[:, spot], y_send.at[i], y_recv.at[i], d, up
            )

        def level_line(i):
            s, col, cols = chunks[i]
            rows = rows_of[s]
            spot = pl.ds(col, cols)
            for copy in second_copies(i):
                copy.wait_recv()
            for b, near in ((0, xb), (1, yb)):
                mine = sum1[s][b, pl.ds(near * 2 * rows, 2 * rows), spot]
                sum2[s][b, :, spot] = mine.astype(F32) + got2[s][b, :, spot].astype(F32)

            @pl.when(u == 3)
            def _():
                for b in range(2):
                    sum3[s][b, :, spot] = low(sum2[s][b, :, spot], s)
                    z_copy(i, b).start()

            @pl.when(u == 0)
            def _():
                sum3[s][1, :, spot] = low(sum2[s][1, :, spot], s)
                y_copy(i).start()

        def level_pass(i):
            s, col, cols = chunks[i]
            spot = pl.ds(col, cols)

            @pl.when(u == 2)
            def _():
                for b in range(2):
                    z_copy(i, b).wait_recv()
                    sum3[s][b, :, spot] = low(
                        sum2[s][b, :, spot] + got3[s][b, :, spot].astype(F32), s
                    )
                    z_copy(i, b).start()

        def level_near(i):
            s, col, cols = chunks[i]
            spot = pl.ds(col, cols)

            @pl.when(u == 1)
            def _():
                z_copy(i, 0).wait_recv()
                sum3[s][0, :, spot] = low(
                    sum2[s][0, :, spot] + got3[s][0, :, spot].astype(F32), s
                )
                z_copy(i, 0).start()
                z_copy(i, 1).wait_recv()
                y_copy(i).wait_recv()
                total = (
                    sum2[s][1, :, spot]
                    + got3[s][1, :, spot].astype(F32)
                    + got4[s][:, spot].astype(F32)
                )
                finish(i, total)

            @pl.when(u == 0)
            def _():
                z_copy(i, 0).wait_recv()
                finish(i, sum2[s][0, :, spot] + got3[s][0, :, spot].astype(F32))

        def p_copy(i):
            s, col, cols = chunks[i]
            rows = rows_of[s]
            spot = pl.ds(col, cols)
            return remote(
                sum1[s].at[0, pl.ds((1 - c) * rows, rows), spot],
                got5[s].at[:, spot],
                p_send.at[i],
                p_recv.at[i],
                mate,
                t,
            )

        def finish(i, total):
            s, col, cols = chunks[i]
            rows = rows_of[s]
            spot = pl.ds(col, cols)
            for copy in second_copies(i):
                copy.wait_send()
            sum2[s][0, :, spot] = total
            sum1[s][0, pl.ds(0, 2 * rows), spot] = low(total, s)
            p_copy(i).start()
            final[s][:, spot] = sum2[s][0, pl.ds(c * rows, rows), spot]

        def level_mate(i):
            s, col, cols = chunks[i]
            spot = pl.ds(col, cols)

            @pl.when(u >= 2)
            def _():
                p_copy(i).wait_recv()
                final[s][:, spot] = got5[s][:, spot].astype(F32)

        def widen(rows, size, spot):
            n, wide = rows.shape[0], row_values.shape[1]
            at = lax.broadcasted_iota(jnp.int32, (128, wide), 0)
            lane = lax.broadcasted_iota(jnp.int32, (128, wide), 1)
            v = jnp.dot(
                rows,
                (at == lane % size).astype(F32),
                precision=lax.Precision.HIGHEST,
                preferred_element_type=F32,
            )
            row = lax.broadcasted_iota(jnp.int32, (n, wide), 0)
            lane = lax.broadcasted_iota(jnp.int32, (n, wide), 1)
            return jnp.sum(jnp.where(lane // size == spot(row), v, 0.0), axis=0, keepdims=True)

        def unpack():
            for z in range(2):
                small_rows[pl.ds((2 * c + z) * 8 * SMALL, 8 * SMALL), :] = small_a[z].astype(F32)
                small_rows[pl.ds((2 - 2 * c + z) * 8 * SMALL, 8 * SMALL), :] = small_b[z].astype(F32)
            for kind in range(6):
                rows = small_rows[pl.ds(3 + kind, 32, stride=SMALL), :]
                row_values[kind : kind + 1, :] = widen(
                    rows, per, lambda row: (row % 8) * 4 + row // 8
                )
            for z in range(2):
                rows = small_rows[pl.ds((2 * c + z) * 8 * SMALL + 2, 8, stride=SMALL), :]
                row_values[6 + z : 7 + z, :] = widen(rows, up_per, lambda row: row)

        def bias_row(kind):
            out = []
            for z in range(2):
                rows = small_rows[pl.ds((2 * c + z) * 8 * SMALL + kind, 8, stride=SMALL), :]
                out.append(widen(rows, per, lambda row: row)[:, :part_cols])
            return jnp.concatenate(out, axis=1)

        def prefix_value():
            tile = small_rows[pl.ds((2 * k + t // 2) * SMALL + 9, 1), :]
            lane = lax.broadcasted_iota(jnp.int32, (1, 128), 1)
            member = t % 2
            sixteens = jnp.sum(jnp.where(lane == member, tile, 0.0), axis=1, keepdims=True)
            units = jnp.sum(jnp.where(lane == 2 + member, tile, 0.0), axis=1, keepdims=True)
            return 16.0 * sixteens + units

        def project_block(bias_q, bias_v, i):
            rows = pl.ds(i * BLOCK, BLOCK)
            both = [
                jnp.dot(x_rows[rows, :], wq[z], preferred_element_type=F32) for z in range(2)
            ]

            def kind(j):
                return jnp.concatenate(
                    [v[:, j * part_cols : (j + 1) * part_cols] for v in both], axis=1
                )

            q_ref[rows, :] = (kind(0) + bias_q).astype(BF)
            k_ref[rows, :] = kind(1).astype(BF)
            v_ref[rows, :] = (kind(2) + bias_v).astype(BF)

        def value_row(i):
            return row_values[i : i + 1, :]

        def swap_copy(which, i):
            rows = pl.ds(i * BLOCK, BLOCK)
            return remote(
                sent.at[rows],
                got.at[which % 2, rows],
                e_send.at[which, i],
                e_recv.at[which, i],
                mate,
                t,
            )

        def swapped(which, i):
            rows = pl.ds(i * BLOCK, BLOCK)
            swap_copy(which, i).wait()
            return sent[rows, :].astype(F32) + got[which % 2, rows, :].astype(F32)

        def swap(which, i, share):
            sent[pl.ds(i * BLOCK, BLOCK), :] = share.astype(BF)
            swap_copy(which, i).start()

        def normalize(v):
            center = v - jnp.mean(v, axis=1, keepdims=True)
            inverse = lax.rsqrt(jnp.mean(center * center, axis=1, keepdims=True) + EPSILON)
            return center * inverse, inverse

        def norm_pull(scaled, normal, inverse):
            first = jnp.mean(scaled, axis=1, keepdims=True)
            second = jnp.mean(scaled * normal, axis=1, keepdims=True)
            return inverse * (scaled - first - normal * second)

        def tally(row, v):
            tile_sum[0, row : row + 1, :] += jnp.sum(v, axis=0, keepdims=True)

        def branch_block(i):
            swap(0, i, dot_nt(o_ref[pl.ds(i * BLOCK, BLOCK), :], out_both[...]))

        def forward_block(i):
            rows = pl.ds(i * BLOCK, BLOCK)
            branch = swapped(0, i) + value_row(2)
            normal, inverse = normalize(x_rows[rows, :].astype(F32) + branch)
            n1_rows[rows, :] = normal
            inv_rows[rows, :] = jnp.broadcast_to(inverse, (BLOCK, 128))
            low_rows[rows, :] = (normal * value_row(0) + value_row(3)).astype(BF)
            for z in range(2):
                for col in range(0, hidden, BLOCK):
                    cols = pl.ds(col, BLOCK)
                    u = jnp.dot(low_rows[rows, :], wu[z, :, cols], preferred_element_type=F32)
                    value, slope = gelu_parts(u + row_values[6 + z : 7 + z, cols])
                    active[z, rows, cols] = value.astype(BF)
                    upper[z, rows, cols] = slope.astype(BF)

        def down_block(i):
            rows = pl.ds(i * BLOCK, BLOCK)
            swap(1, i, dot_nt(active[0, rows, :], wd[0]) + dot_nt(active[1, rows, :], wd[1]))

        def row_home(i):
            return jnp.logical_and(i == t, c == t // 2)

        def out_copy(i):
            return remote(
                res_rows.at[pl.ds((2 * i + c) * half, half)],
                res_out.at[t % 2, pl.ds(c * half, half)],
                ex_send.at[0, i],
                ex_recv.at[0, t % 2, c],
                2 * k + t // 2,
                i,
            )

        def output_block(i):
            rows = pl.ds(i * BLOCK, BLOCK)
            feed_out = swapped(1, i) + value_row(4)
            normed = n1_rows[rows, :] * value_row(0) + value_row(3)
            normal, inverse = normalize(normed + feed_out)
            res_rows[rows, :] = (normal * value_row(1) + value_row(5)).astype(BF)
            incoming = cot_rows[rows, :].astype(F32)
            tally(7, incoming * normal)
            tally(11, incoming)
            residual = norm_pull(incoming * value_row(1), normal, inverse)
            residual_rows[rows, :] = residual
            feed = residual.astype(BF)
            feed_rows[rows, :] = feed
            tally(10, feed.astype(F32))
            for z in range(2):
                for col in range(0, hidden, BLOCK):
                    cols = pl.ds(col, BLOCK)
                    pull = jnp.dot(feed_rows[rows, :], wd[z, :, cols], preferred_element_type=F32)
                    grad = (pull * upper[z, rows, cols].astype(F32)).astype(BF)
                    upper[z, rows, cols] = grad
                    tile_sum[0, 4 + z : 5 + z, cols] += jnp.sum(
                        grad.astype(F32), axis=0, keepdims=True
                    )
            swap(2, i, dot_nt(upper[0, rows, :], wu[0]) + dot_nt(upper[1, rows, :], wu[1]))

            @pl.when(row_home(i))
            def _():
                store = pltpu.make_async_copy(
                    res_rows.at[pl.ds((2 * i + c) * half, half)],
                    res_out.at[t % 2, pl.ds(c * half, half)],
                    row_sem,
                )
                store.start()
                store.wait()

            @pl.when(jnp.logical_not(row_home(i)))
            def _():
                out_copy(i).start()

        def branch_back_block(i):
            rows = pl.ds(i * BLOCK, BLOCK)
            grad = residual_rows[rows, :] + swapped(2, i)
            normal = n1_rows[rows, :]
            tally(6, grad * normal)
            tally(9, grad)
            residual = norm_pull(grad * value_row(0), normal, inv_rows[rows, 0:1])
            residual_rows[rows, :] = residual
            low_grad = residual.astype(BF)
            branch_rows[rows, :] = low_grad
            tally(8, low_grad.astype(F32))
            do_ref[rows, :] = jnp.dot(
                branch_rows[rows, :], out_both[...], preferred_element_type=F32
            ).astype(BF)

        def outer(left, j, right):
            return dot_tn(left[:, pl.ds(j * BLOCK, BLOCK)], right).astype(BF)

        def down_grad(z, j):
            wd[z, pl.ds(j * BLOCK, BLOCK), :] = outer(feed_rows, j, active[z])

        def up_grad(z, j):
            wu[z, pl.ds(j * BLOCK, BLOCK), :] = outer(low_rows, j, upper[z])

        def out_grad(j):
            both = outer(branch_rows, j, o_ref[...])
            for z in range(2):
                wo[z, pl.ds(j * BLOCK, BLOCK), :] = both[:, z * part_cols : (z + 1) * part_cols]

        def attention(pair, kb):
            if kb == 0:
                back_start(pair, o_ref, do_ref, dots, acc)
            back_block(
                pair, kb, q_ref, k_ref, v_ref, lt_ref, do_ref, dots, acc, dk, dv, limit
            )
            if kb == blocks - 1:
                dq[:, pl.ds(pair * 128, 128)] = (acc[...] * DH**-0.5).astype(BF)

        def mate_copy(i):
            return remote(
                sent.at[pl.ds(i * half, half)],
                mate_got.at[i],
                t_send.at[0, i],
                t_recv.at[0, i],
                mate,
                t,
            )

        def mix(i):
            rows = pl.ds(i * BLOCK, BLOCK)
            kinds = [ref[rows, :] for ref in (dq, dk, dv)]
            share = jnp.zeros((BLOCK, width), F32)
            for z in range(2):
                both = jnp.concatenate(
                    [v[:, z * part_cols : (z + 1) * part_cols] for v in kinds], axis=1
                )
                mixed[z, rows, 0 : 3 * part_cols] = both
                share = share + dot_nt(both, wq[z])
            acc_rows[...] = share
            sent[pl.ds(i * half, half), :] = acc_rows[pl.ds((1 - c) * half, half), :].astype(BF)
            residual_rows[pl.ds((2 * i + c) * half, half), :] += acc_rows[pl.ds(c * half, half), :]
            mate_copy(i).start()

        def row_copy(i):
            return remote(
                low_rows.at[pl.ds(i * half, half)],
                tgr_out.at[t % 2, pl.ds(c * half, half)],
                t_send.at[1, i],
                t_recv.at[1, 2 * (t % 2) + c],
                2 * k + t // 2,
                i,
            )

        def send_rows(i):
            mate_copy(i).wait_recv()
            low_rows[pl.ds(i * half, half), :] = (
                residual_rows[pl.ds((2 * i + c) * half, half), :] + mate_got[i].astype(F32)
            ).astype(BF)
            here = row_home(i)

            @pl.when(here)
            def _():
                store = pltpu.make_async_copy(
                    low_rows.at[pl.ds(i * half, half)], tgr_out.at[t % 2, pl.ds(c * half, half)], row_sem
                )
                store.start()
                store.wait()

            @pl.when(jnp.logical_not(here))
            def _():
                row_copy(i).start()

        def settle_rows():
            for i in range(4):
                mate_copy(i).wait_send()

                @pl.when(jnp.logical_not(jnp.logical_and(i == t, c == t // 2)))
                def _():
                    row_copy(i).wait_send()

            for m in range(2):
                for core in range(2):
                    spot = tgr_out.at[m, pl.ds(core * half, half)]

                    @pl.when(jnp.logical_not(jnp.logical_and(2 * c + m == t, core == c)))
                    def _():
                        remote(
                            low_rows.at[pl.ds(0, half)],
                            spot,
                            t_send.at[1, 0],
                            t_recv.at[1, 2 * m + core],
                            mate,
                            t,
                        ).wait_recv()

        def weight_grad(j):
            rows = pl.ds(j * BLOCK, BLOCK)
            for z in range(2):
                wq[z, rows, :] = outer(x_rows, j, mixed[z, :, 0 : 3 * part_cols])

        def tile_copy(stage, goal_dp, goal_t, slot):
            return remote(
                tile_sum.at[stage],
                tile_got.at[slot],
                s_send.at[slot],
                s_recv.at[slot],
                goal_dp,
                goal_t,
            )

        def tile_start():
            for row, ref in ((0, dq), (2, dv)):
                sums = jnp.sum(ref[...].astype(F32), axis=0, keepdims=True)
                for z in range(2):
                    tile_sum[0, row + z : row + z + 1, 0:part_cols] = sums[
                        :, z * part_cols : (z + 1) * part_cols
                    ]
            tile_copy(0, dx, t, 0).start()

        def tile_second():
            tile_copy(0, dx, t, 0).wait_recv()
            tile_sum[1] = tile_sum[0] + tile_got[0]
            tile_copy(1, dy, t, 1).start()

        def tile_third():
            tile_copy(1, dy, t, 1).wait_recv()
            tile_sum[2] = tile_sum[1] + tile_got[1]
            for step in range(1, 4):
                tile_copy(2, d, (t + step) % 4, 1 + step).start()

        def tile_fourth():
            for step in range(1, 4):
                tile_copy(2, d, t, 1 + step).wait_recv()
            tile_sum[3] = (tile_sum[2] + tile_got[2]) + (tile_got[3] + tile_got[4])
            tile_copy(3, mate, t, 5).start()

        def tile_last():
            tile_copy(3, mate, t, 5).wait_recv()
            tile_own[...] = tile_sum[3]
            tile_mate[...] = tile_got[5]
            for slot, stage in enumerate((0, 1, 2, 2, 2, 3)):
                tile_copy(stage, mate, t, slot).wait_send()

        levels = [level_first, level_second, level_line, level_pass, level_near, level_mate]
        come = gather_steps(
            (d, t, k, c, xb, yb, dx, dy),
            tok,
            cot,
            x_rows,
            cot_rows,
            own,
            (wq, wo, wu, wd, small_a),
            small_b,
            sems,
            arrivals,
        )
        come.placed(4)
        for i in range(4):
            come.placed(i)
        tile_sum[0] = jnp.zeros(tile_sum.shape[1:], F32)
        for i in range(3):
            come.own(i)
        come.line(0)
        come.line(1)
        come.second(0)
        come.line(2)
        come.exchange(0, tok, x_rows)
        come.own(3)
        come.own(4)
        come.second(1)
        come.done(0)
        come.swap.start()
        come.second(2)
        come.relay(0, tok, x_rows)
        come.line(3)
        come.own(5)
        come.own(6)
        come.swap.wait()
        unpack()
        limit = prefix_value()
        bias_q, bias_v = bias_row(0), bias_row(1)
        come.arrived(0, x_rows)
        come.done(1)
        pl.loop(0, blocks)(partial(project_block, bias_q, bias_v))
        come.line(4)
        come.second(3)
        todo = {
            2: partial(come.line, 5),
            4: partial(come.second, 4),
            6: partial(come.line, 6),
            7: partial(come.exchange, 1, cot, cot_rows),
            9: partial(come.second, 5),
        }
        for unit in range(heads_width // 128 * blocks):
            if unit in todo:
                todo[unit]()
            attend_rows(
                q_ref, k_ref, v_ref, o_ref, lt_ref, limit, unit // blocks, unit % blocks
            )
        come.done(2)
        out_both[...] = jnp.concatenate([wo[0], wo[1]], axis=1)
        pl.loop(0, blocks)(branch_block)
        come.done(3)
        come.done(4)
        come.second(6)
        pl.loop(0, blocks)(forward_block)
        come.done(5)
        come.done(6)
        pl.loop(0, blocks)(down_block)
        come.relay(1, cot, cot_rows)
        come.arrived(1, cot_rows)
        pl.loop(0, blocks)(output_block)
        come.sent_all()
        pl.loop(0, width // BLOCK)(lambda j: [down_grad(z, j) for z in range(2)] and None)
        level_first(0)
        level_first(1)
        pl.loop(0, width // BLOCK)(lambda j: [up_grad(z, j) for z in range(2)] and None)
        level_first(2)
        pl.loop(0, blocks)(branch_back_block)
        pl.loop(0, width // BLOCK)(out_grad)
        work = [
            partial(attention, pair, kb)
            for pair in range(heads_width // 128)
            for kb in range(blocks)
        ]
        work += [partial(mix, i) for i in range(blocks)]
        work += [partial(weight_grad, j) for j in range(width // BLOCK)]
        done = 0
        for slot in range(n_chunks + 5):
            if slot < n_chunks - 1:
                upto = -(-len(work) * (slot + 1) // (n_chunks - 1))
                for unit in work[done:upto]:
                    unit()
                done = upto
            if slot == n_chunks - 2:
                tile_start()
            for lag, level in enumerate(levels):
                i = slot + (2 if lag == 0 else 1) - lag
                if lag == 0:
                    i = {0: 3, 1: 4, n_chunks - 2: n_chunks - 1}.get(slot, -1)
                if 0 <= i < n_chunks:
                    level(i)
            if slot == n_chunks - 2:
                for i in range(4):
                    send_rows(i)
            if slot >= n_chunks - 1:
                tail = slot - (n_chunks - 1)
                if tail < 4:
                    (tile_second, tile_third, tile_fourth, tile_last)[tail]()
        for i in range(4):

            @pl.when(jnp.logical_not(row_home(i)))
            def _():
                out_copy(i).wait_send()

        for m in range(2):
            for core in range(2):
                spot = res_out.at[m, pl.ds(core * half, half)]

                @pl.when(jnp.logical_not(jnp.logical_and(2 * c + m == t, core == c)))
                def _():
                    remote(
                        res_rows.at[pl.ds(0, half)],
                        spot,
                        ex_send.at[0, 0],
                        ex_recv.at[0, m, core],
                        mate,
                        t,
                    ).wait_recv()

        settle_rows()
        for i in range(n_chunks):
            for copy in first_copies(i):
                copy.wait_send()

            @pl.when(u >= 2)
            def _():
                for copy in second_copies(i):
                    copy.wait_send()
                for b in range(2):
                    z_copy(i, b).wait_send()

            @pl.when(u == 1)
            def _():
                z_copy(i, 0).wait_send()

            @pl.when(u == 0)
            def _():
                y_copy(i).wait_send()

            @pl.when(u <= 1)
            def _():
                p_copy(i).wait_send()

    any_spec = pl.BlockSpec(memory_space=pl.ANY)
    vmem = pl.BlockSpec(memory_space=pltpu.VMEM)
    dma = pltpu.SemaphoreType.DMA
    scratch = []
    for kind in range(8):
        for s in range(count):
            rows, cols, kept = rows_of[s], grads[s].shape[2], grads[s].dtype
            shape, dtype = (
                ((2, 4 * rows, cols), kept),
                ((2, 4 * rows, cols), kept),
                ((2, 2 * rows, cols), kept),
                ((2, 2 * rows, cols), F32),
                ((2, 2 * rows, cols), kept),
                ((2, 2 * rows, cols), kept),
                ((2 * rows, cols), kept),
                ((rows, cols), kept),
            )[kind]
            scratch.append(pltpu.VMEM(shape, dtype))
    back = jax.ShapeDtypeStruct((2, 2 * half, width), BF)
    tiles = jax.ShapeDtypeStruct((16, hidden), F32)
    outs = pl.pallas_call(
        kernel,
        out_shape=[
            back,
            back,
            tiles,
            tiles,
            *[jax.ShapeDtypeStruct((r, g.shape[2]), F32) for r, g in zip(rows_of, grads)],
        ],
        in_specs=[any_spec] * (3 + count),
        out_specs=[any_spec, any_spec] + [vmem] * (2 + count),
        scratch_shapes=[
            *gather_sems(count + 1, len(arrivals)),
            *scratch,
            dma,
            dma((1, 4)),
            dma((1, 2, 2)),
            dma((n_chunks, 3)),
            dma((n_chunks, 3)),
            dma((n_chunks, 2)),
            dma((n_chunks, 2)),
            dma((n_chunks, 2)),
            dma((n_chunks, 2)),
            dma((n_chunks,)),
            dma((n_chunks,)),
            dma((n_chunks,)),
            dma((n_chunks,)),
            *[pltpu.VMEM(w.shape, BF) for w in weights],
            *[pltpu.VMEM((length, heads_width), BF)] * 4,
            pltpu.VMEM((heads_width // DH, 8, length), F32),
            pltpu.VMEM((2, 8 * SMALL, 128), BF),
            pltpu.VMEM((2, 8 * SMALL, 128), BF),
            pltpu.VMEM((length, width), BF),
            pltpu.VMEM((length, width), BF),
            pltpu.VMEM((32 * SMALL, 128), F32),
            pltpu.VMEM((8, width), F32),
            pltpu.VMEM((width, heads_width), BF),
            pltpu.VMEM((length, width), F32),
            pltpu.VMEM((length, 128), F32),
            pltpu.VMEM((length, width), F32),
            pltpu.VMEM((length, width), BF),
            pltpu.VMEM((length, width), BF),
            pltpu.VMEM((length, width), BF),
            pltpu.VMEM((length, width), BF),
            pltpu.VMEM((length, width), BF),
            pltpu.VMEM((2, length, width), BF),
            pltpu.VMEM((2, length, hidden), BF),
            pltpu.VMEM((2, length, hidden), BF),
            pltpu.VMEM((length, heads_width), BF),
            pltpu.VMEM((8, length), F32),
            pltpu.VMEM((length, 128), F32),
            pltpu.VMEM((BLOCK, width), F32),
            pltpu.VMEM((4, half, width), BF),
            dma((3, blocks)),
            dma((3, blocks)),
            dma((6,)),
            dma((6,)),
            dma((2, 4)),
            dma((2, 4)),
            pltpu.VMEM((4, *tiles.shape), F32),
            pltpu.VMEM((6, *tiles.shape), F32),
        ],
        compiler_params=pltpu.CompilerParams(
            collective_id=2, has_side_effects=True, vmem_limit_bytes=67043328
        ),
    )(tokens, cotangent, *shards)
    return outs[0], outs[1], outs[2], outs[3], outs[4:]


BLOCK = 256


def lane_half(shape, h):
    lane = lax.broadcasted_iota(jnp.int32, shape, 1)
    return lane < DH if h == 0 else lane >= DH


def reach(row_block, blocks):
    return max(row_block + 1, blocks // 2)


def dot_nt(a, b):
    return lax.dot_general(a, b, (((1,), (1,)), ((), ())), preferred_element_type=F32)


def dot_tn(a, b):
    return lax.dot_general(a, b, (((0,), (0,)), ((), ())), preferred_element_type=F32)


def attend_rows(q_ref, k_ref, v_ref, o_ref, lt_ref, limit, pair, qb):
    length = q_ref.shape[0]
    blocks = length // BLOCK
    lanes = pl.ds(pair * 128, 128)
    rows = pl.ds(qb * BLOCK, BLOCK)
    span = reach(qb, blocks) * BLOCK
    q = q_ref[rows, lanes] * jnp.asarray(DH**-0.5, BF)
    heads = []
    for h in range(2):
        half = lane_half((BLOCK, 128), h)
        s = dot_nt(jnp.where(half, q, jnp.zeros_like(q)), k_ref[pl.ds(0, span), lanes])
        clear = qb * BLOCK
        row = lax.broadcasted_iota(jnp.int32, (BLOCK, span - clear), 0) + clear
        col = lax.broadcasted_iota(jnp.int32, (BLOCK, span - clear), 1) + clear
        seen = col <= row
        if clear < length // 2:
            seen = jnp.logical_or(seen, col.astype(F32) < limit)
        tail = jnp.where(seen, s[:, clear:], MASKED_SCORE)
        s = jnp.concatenate([s[:, :clear], tail], axis=1) if clear else tail
        top = jnp.max(s, axis=1, keepdims=True)
        p = jnp.exp(s - top)
        total = jnp.sum(p, axis=1, keepdims=True)
        log_total = top + jnp.log(total)
        lt_ref[2 * pair + h, 0:1, rows] = jnp.transpose(
            jnp.broadcast_to(log_total, (BLOCK, 128))
        )[0:1, :]
        p = (p * (1.0 / total)).astype(BF)
        heads.append(jnp.dot(p, v_ref[pl.ds(0, span), lanes], preferred_element_type=F32))
    o_ref[rows, lanes] = jnp.where(lane_half((BLOCK, 128), 0), heads[0], heads[1]).astype(BF)


def back_start(pair, o_ref, do_ref, dots, acc):
    head_row = lax.broadcasted_iota(jnp.int32, (8, 128), 0)
    lane = lax.broadcasted_iota(jnp.int32, (8, 128), 1)
    pick = (lane // DH == head_row).astype(F32)
    lanes = pl.ds(pair * 128, 128)
    dots[...] = lax.dot_general(
        pick,
        do_ref[:, lanes].astype(F32) * o_ref[:, lanes].astype(F32),
        (((1,), (1,)), ((), ())),
        precision=lax.Precision.HIGHEST,
        preferred_element_type=F32,
    )
    acc[...] = jnp.zeros_like(acc)


def back_block(pair, kb, q_ref, k_ref, v_ref, lt_ref, do_ref, dots, acc, dk_ref, dv_ref, limit):
    length = q_ref.shape[0]
    blocks = length // BLOCK
    lanes = pl.ds(pair * 128, 128)
    keys_at = pl.ds(kb * BLOCK, BLOCK)
    key = k_ref[keys_at, lanes]
    value = v_ref[keys_at, lanes]
    zero = jnp.zeros((BLOCK, 128), BF)
    dk = jnp.zeros((BLOCK, 128), F32)
    dv = jnp.zeros((BLOCK, 128), F32)
    for qb in range(blocks):
        if kb >= reach(qb, blocks):
            continue
        rows = pl.ds(qb * BLOCK, BLOCK)
        q_pair = q_ref[rows, lanes] * jnp.asarray(DH**-0.5, BF)
        do_pair = do_ref[rows, lanes]
        for h in range(2):
            half = lane_half((BLOCK, 128), h)
            q = jnp.where(half, q_pair, zero)
            do = jnp.where(half, do_pair, zero)
            s = dot_nt(key, q)
            if kb >= qb:
                key_id = lax.broadcasted_iota(jnp.int32, (BLOCK, BLOCK), 0) + kb * BLOCK
                row_id = lax.broadcasted_iota(jnp.int32, (BLOCK, BLOCK), 1) + qb * BLOCK
                seen = key_id <= row_id
                if kb * BLOCK < length // 2:
                    seen = jnp.logical_or(seen, key_id.astype(F32) < limit)
                s = jnp.where(seen, s, MASKED_SCORE)
            p = jnp.exp(s - lt_ref[2 * pair + h, 0:1, rows])
            dp = dot_nt(value, do)
            ds = (p * (dp - dots[h : h + 1, rows])).astype(BF)
            dv = dv + jnp.dot(p.astype(BF), do, preferred_element_type=F32)
            dk = dk + jnp.dot(ds, q, preferred_element_type=F32)
            acc[rows, :] += dot_tn(ds, jnp.where(half, key, zero))
    dk_ref[keys_at, lanes] = dk.astype(BF)
    dv_ref[keys_at, lanes] = dv.astype(BF)


def chip_local(
    tokens, prefix_len, w_qkv, bias_qv, w_out, w_up, bias_up, w_down, gains, shifts, cotangent
):
    d, t, k, c, _, _, _, _ = place()
    part = w_qkv.shape[2]
    hidden = w_up.shape[1]

    def lanes(v):
        return jnp.pad(v, ((0, 0), (0, 128 - v.shape[1])))

    limits = jnp.concatenate([prefix_len // 16, prefix_len % 16]).astype(BF)[None]
    small = jnp.concatenate(
        [lanes(v) for v in (bias_qv, bias_up[None], gains, shifts, limits)], axis=0
    )
    small = jnp.pad(small, ((0, SMALL - small.shape[0]), (0, 0)))
    shards = (
        w_qkv.reshape(ROWS, 3 * part),
        w_out.T,
        w_up,
        w_down.T,
        small,
    )
    half = hidden // 2
    chunks = (
        (4, 0, 128),
        (0, 0, 3 * part),
        (1, 0, part),
        (2, 0, half),
        (2, half, half),
        (3, 0, half),
        (3, half, half),
    )
    per = bias_qv.shape[1]
    back_chunks = (
        (3, 0, half),
        (3, half, half),
        (2, 0, half),
        (2, half, half),
        (1, 0, part),
        (0, 0, 3 * part),
    )
    out_rows, token_rows, tile_own, tile_mate, finals = layer(
        tokens, cotangent, shards, per, chunks, back_chunks
    )
    plane_rows = jnp.where(c == t // 2, tile_own, tile_mate)[:6].reshape(3, 2, hidden)
    plane_rows = lax.dynamic_index_in_dim(plane_rows, t % 2, 1, False)
    mine_rows = lax.dynamic_slice(tile_own, (6, (4 * d + t) * per), (6, per))
    return (
        out_rows,
        token_rows.astype(F32),
        finals[0].reshape(w_qkv.shape),
        lax.dynamic_slice(plane_rows, (0, d * per), (2, per)),
        finals[1].T,
        finals[2],
        lax.dynamic_slice(plane_rows, (2, d * bias_up.shape[0]), (1, bias_up.shape[0]))[0],
        finals[3].T,
        mine_rows[:2],
        mine_rows[2:],
    )


def solution(mesh):
    return jax.shard_map(
        chip_local if dict(mesh.shape) == {"dp": 8, "tensor": 4} else local,
        mesh=mesh,
        in_specs=(
            P("dp", "tensor", None),
            P("dp"),
            P("dp", None, "tensor"),
            P(None, ("tensor", "dp")),
            P("tensor", "dp"),
            P("dp", "tensor"),
            P(("tensor", "dp")),
            P("tensor", "dp"),
            P(None, ("dp", "tensor")),
            P(None, ("dp", "tensor")),
            P("dp", "tensor", None),
        ),
        out_specs=(
            P("dp", "tensor", None),
            P("dp", "tensor", None),
            P("dp", None, "tensor"),
            P(None, ("tensor", "dp")),
            P("tensor", "dp"),
            P("dp", "tensor"),
            P(("tensor", "dp")),
            P("tensor", "dp"),
            P(None, ("dp", "tensor")),
            P(None, ("dp", "tensor")),
        ),
        check_vma=False,
    )
```

```python
import math
import types
from functools import partial

import jax
import jax.numpy as jnp
from jax import lax
from jax.experimental import pallas as pl
from jax.experimental.pallas import tpu as pltpu
from jax.sharding import PartitionSpec as P

DH = 64


EPSILON = 1e-05
MASKED_SCORE = -1e30


def norm_forward(values, gain_row, shift_row):
    center = values - jnp.mean(values, axis=-1, keepdims=True)
    inverse = lax.rsqrt(jnp.mean(center * center, axis=-1, keepdims=True) + EPSILON)
    normal = center * inverse
    return (normal * gain_row + shift_row, normal, inverse)


def norm_backward(incoming, normal, inverse, gain_row):
    scaled = incoming * gain_row
    first_mean = jnp.mean(scaled, axis=-1, keepdims=True)
    second_mean = jnp.mean(scaled * normal, axis=-1, keepdims=True)
    outgoing = inverse * (scaled - first_mean - normal * second_mean)
    return (outgoing, jnp.sum(incoming * normal, axis=0), jnp.sum(incoming, axis=0))


def visible_mask(offset, block_rows, length, prefix):
    row_ids = offset + jnp.arange(block_rows, dtype=jnp.int32)[:, None]
    column_ids = jnp.arange(length, dtype=jnp.int32)[None, :]
    return jnp.logical_or(column_ids < prefix, column_ids <= row_ids)


def block_scores(chosen, key_heads, offset, prefix, scaling):
    length = key_heads.shape[0]
    allowed = visible_mask(offset, chosen.shape[0], length, prefix)
    scores = (
        jnp.einsum("qhd,khd->hqk", chosen, key_heads, preferred_element_type=jnp.float32) * scaling
    )
    return jnp.where(allowed[None], scores, MASKED_SCORE)


def attention_forward(queries, key_heads, value_heads, prefix):
    length = key_heads.shape[0]
    block_rows = min(512, length)
    scaling = queries.shape[-1] ** (-0.5)
    outputs = []
    totals = []
    for offset in range(0, length, block_rows):
        scores = block_scores(
            queries[offset : offset + block_rows], key_heads, offset, prefix, scaling
        )
        row_max = jnp.max(scores, axis=-1, keepdims=True)
        log_total = jnp.log(jnp.sum(jnp.exp(scores - row_max), axis=-1, keepdims=True)) + row_max
        attn_probs = jnp.exp(scores - log_total).astype(jnp.bfloat16)
        outputs.append(
            jnp.einsum("hqk,khd->qhd", attn_probs, value_heads, preferred_element_type=jnp.float32)
        )
        totals.append(log_total)
    return (jnp.concatenate(outputs, axis=0), totals)


def attention_backward(queries, key_heads, value_heads, prefix, totals, context_grad):
    length = key_heads.shape[0]
    block_rows = min(512, length)
    scaling = queries.shape[-1] ** (-0.5)
    query_parts = []
    key_grad = jnp.zeros(key_heads.shape, jnp.float32)
    value_grad = jnp.zeros(value_heads.shape, jnp.float32)
    for number, offset in enumerate(range(0, length, block_rows)):
        chosen = queries[offset : offset + block_rows]
        grad_block = context_grad[offset : offset + block_rows]
        scores = block_scores(chosen, key_heads, offset, prefix, scaling)
        attn_probs = jnp.exp(scores - totals[number])
        probs_low = attn_probs.astype(jnp.bfloat16)
        probs_grad = jnp.einsum(
            "qhd,khd->hqk", grad_block, value_heads, preferred_element_type=jnp.float32
        )
        row_dot = jnp.sum(attn_probs * probs_grad, axis=-1, keepdims=True)
        scores_grad = (attn_probs * (probs_grad - row_dot)).astype(jnp.bfloat16)
        query_parts.append(
            jnp.einsum("hqk,khd->qhd", scores_grad, key_heads, preferred_element_type=jnp.float32)
            * scaling
        )
        key_grad = (
            key_grad
            + jnp.einsum("hqk,qhd->khd", scores_grad, chosen, preferred_element_type=jnp.float32)
            * scaling
        )
        value_grad = value_grad + jnp.einsum(
            "hqk,qhd->khd", probs_low, grad_block, preferred_element_type=jnp.float32
        )
    return (jnp.concatenate(query_parts, axis=0), key_grad, value_grad)


def local(
    tokens, prefix_len, w_qkv, bias_qv, w_out, w_up, bias_up, w_down, gains, shifts, cotangent
):
    tensor_count = lax.axis_size("tensor")
    seq_local, shard_rows, model_width = tokens.shape
    length = shard_rows * tensor_count
    full_qkv, full_bias_qv, full_out, full_up, full_bias_up, full_down = (
        lax.all_gather(w_qkv, "dp", axis=0, tiled=True),
        lax.all_gather(bias_qv, "dp", axis=1, tiled=True),
        lax.all_gather(w_out, "dp", axis=1, tiled=True),
        lax.all_gather(w_up, "dp", axis=0, tiled=True),
        lax.all_gather(bias_up, "dp", axis=0, tiled=True),
        lax.all_gather(w_down, "dp", axis=1, tiled=True),
    )
    full_gains, full_shifts = (
        lax.all_gather(gains, ("dp", "tensor"), axis=1, tiled=True),
        lax.all_gather(shifts, ("dp", "tensor"), axis=1, tiled=True),
    )
    full_gains = full_gains.astype(jnp.float32)
    full_shifts = full_shifts.astype(jnp.float32)
    bias_values = full_bias_qv.astype(jnp.float32)
    up_bias = full_bias_up.astype(jnp.float32)
    local_width = full_qkv.shape[2]
    head_count = local_width // DH
    kept_state = []
    outputs = []
    for member in range(seq_local):
        token_rows = tokens[member]
        prefix = prefix_len[member]

        def fold_tokens(piece):
            product = jnp.einsum("rd,dce->rce", piece, full_qkv, preferred_element_type=jnp.float32)
            return (piece, product)

        token_full, projected = fold_tokens(
            lax.all_gather(token_rows, "tensor", axis=0, tiled=True)
        )
        queries = (
            (projected[:, 0] + bias_values[0]).astype(jnp.bfloat16).reshape(length, head_count, DH)
        )
        key_heads = projected[:, 1].astype(jnp.bfloat16).reshape(length, head_count, DH)
        value_heads = (
            (projected[:, 2] + bias_values[1]).astype(jnp.bfloat16).reshape(length, head_count, DH)
        )
        context, totals = attention_forward(queries, key_heads, value_heads, prefix)
        context_low = context.reshape(length, local_width).astype(jnp.bfloat16)
        branch = (
            lax.psum_scatter(
                jnp.dot(context_low, full_out, preferred_element_type=jnp.float32).astype(
                    jnp.bfloat16
                ),
                "tensor",
                scatter_dimension=0,
                tiled=True,
            ).astype(jnp.float32)
            + full_shifts[0]
        )
        normed, normal_one, inverse_one = norm_forward(
            token_rows.astype(jnp.float32) + branch, full_gains[0], full_shifts[1]
        )
        normed_low = normed.astype(jnp.bfloat16)

        def fold_normed(piece):
            product = jnp.dot(piece, full_up, preferred_element_type=jnp.float32)
            return (piece, product)

        normed_full, pre_active = fold_normed(
            lax.all_gather(normed_low, "tensor", axis=0, tiled=True)
        )
        pre_active = pre_active + up_bias
        active_low = jax.nn.gelu(pre_active, approximate=False).astype(jnp.bfloat16)
        feed_out = (
            lax.psum_scatter(
                jnp.dot(active_low, full_down, preferred_element_type=jnp.float32).astype(
                    jnp.bfloat16
                ),
                "tensor",
                scatter_dimension=0,
                tiled=True,
            ).astype(jnp.float32)
            + full_shifts[2]
        )
        result, normal_two, inverse_two = norm_forward(
            normed + feed_out, full_gains[1], full_shifts[3]
        )
        outputs.append(result.astype(jnp.bfloat16))
        kept_state.append(
            (
                token_rows,
                prefix,
                token_full,
                queries,
                key_heads,
                value_heads,
                totals,
                context_low,
                normal_one,
                inverse_one,
                normed_full,
                pre_active,
                active_low,
                normal_two,
                inverse_two,
            )
        )
    back_qkv, back_out, back_up, back_down = (
        lax.all_gather(w_qkv, "dp", axis=0, tiled=True),
        lax.all_gather(w_out, "dp", axis=1, tiled=True),
        lax.all_gather(w_up, "dp", axis=0, tiled=True),
        lax.all_gather(w_down, "dp", axis=1, tiled=True),
    )
    full_shapes = (
        full_qkv.shape,
        full_bias_qv.shape,
        full_out.shape,
        full_up.shape,
        full_bias_up.shape,
        full_down.shape,
    )
    weight_grads = tuple((jnp.zeros(array_shape, jnp.float32) for array_shape in full_shapes))
    gain_grads = jnp.zeros((2, model_width), jnp.float32)
    shift_grads = jnp.zeros((4, model_width), jnp.float32)
    input_grads = []
    for member in range(seq_local):
        (
            token_rows,
            prefix,
            token_full,
            queries,
            key_heads,
            value_heads,
            totals,
            context_low,
            normal_one,
            inverse_one,
            normed_full,
            pre_active,
            active_low,
            normal_two,
            inverse_two,
        ) = kept_state[member]
        incoming = cotangent[member].astype(jnp.float32)
        residual_two, gain_two, shift_two = norm_backward(
            incoming, normal_two, inverse_two, full_gains[1]
        )
        feed_grad = residual_two.astype(jnp.bfloat16)
        fold_piece = lax.all_gather(feed_grad, "tensor", axis=0, tiled=True)
        down_grad = jnp.einsum(
            "rf,rd->fd", active_low, fold_piece, preferred_element_type=jnp.float32
        )
        fold_product = jnp.einsum(
            "rd,fd->rf", fold_piece, back_down, preferred_element_type=jnp.float32
        )
        active_grad = fold_product
        down_grad, active_grad = (down_grad, active_grad)
        layer_value, gelu_pull = jax.vjp(partial(jax.nn.gelu, approximate=False), pre_active)
        upper_grad = gelu_pull(active_grad)[0].astype(jnp.bfloat16)
        normed_grad = residual_two + lax.psum_scatter(
            jnp.einsum("rf,df->rd", upper_grad, back_up, preferred_element_type=jnp.float32).astype(
                jnp.bfloat16
            ),
            "tensor",
            scatter_dimension=0,
            tiled=True,
        ).astype(jnp.float32)
        up_grad = jnp.einsum(
            "ld,lf->df", normed_full, upper_grad, preferred_element_type=jnp.float32
        )
        up_bias_grad = jnp.sum(upper_grad.astype(jnp.float32), axis=0)
        residual_one, gain_one, shift_one = norm_backward(
            normed_grad, normal_one, inverse_one, full_gains[0]
        )
        branch_grad = residual_one.astype(jnp.bfloat16)

        def fold_branch(piece):
            out_grad = jnp.einsum(
                "rk,rd->kd", context_low, piece, preferred_element_type=jnp.float32
            )
            product = jnp.einsum("rd,kd->rk", piece, back_out, preferred_element_type=jnp.float32)
            return (out_grad, product)

        out_grad, context_grad = fold_branch(
            lax.all_gather(branch_grad, "tensor", axis=0, tiled=True)
        )
        context_grad = context_grad.astype(jnp.bfloat16).reshape(length, head_count, DH)
        query_grad, key_grad, value_grad = attention_backward(
            queries, key_heads, value_heads, prefix, totals, context_grad
        )
        mixed_grad = (
            jnp.stack([query_grad, key_grad, value_grad], axis=1)
            .astype(jnp.bfloat16)
            .reshape(length, 3, local_width)
        )
        qkv_grad = jnp.einsum(
            "ld,lce->dce", token_full, mixed_grad, preferred_element_type=jnp.float32
        )
        row_sums = jnp.sum(mixed_grad.astype(jnp.float32), axis=0)
        bias_grad = jnp.stack([row_sums[0], row_sums[2]])
        token_grad = residual_one + lax.psum_scatter(
            jnp.einsum(
                "rce,dce->rd", mixed_grad, back_qkv, preferred_element_type=jnp.float32
            ).astype(jnp.bfloat16),
            "tensor",
            scatter_dimension=0,
            tiled=True,
        ).astype(jnp.float32)
        input_grads.append(token_grad)
        gain_grads = gain_grads + jnp.stack([gain_one, gain_two])
        shift_grads = shift_grads + jnp.stack(
            [
                jnp.sum(branch_grad.astype(jnp.float32), axis=0),
                shift_one,
                jnp.sum(feed_grad.astype(jnp.float32), axis=0),
                shift_two,
            ]
        )
        member_grads = (qkv_grad, bias_grad, out_grad, up_grad, up_bias_grad, down_grad)
        weight_grads = tuple(
            (running + grad_part for running, grad_part in zip(weight_grads, member_grads))
        )
    total_qkv, total_bias, total_out, total_up, total_up_bias, total_down = weight_grads
    weight_grads = (
        lax.psum_scatter(total_qkv, "dp", scatter_dimension=0, tiled=True),
        lax.psum_scatter(total_bias, "dp", scatter_dimension=1, tiled=True),
        lax.psum_scatter(total_out, "dp", scatter_dimension=1, tiled=True),
        lax.psum_scatter(total_up, "dp", scatter_dimension=0, tiled=True),
        lax.psum_scatter(total_up_bias, "dp", scatter_dimension=0, tiled=True),
        lax.psum_scatter(total_down, "dp", scatter_dimension=1, tiled=True),
    )
    gain_share, shift_share = (
        lax.psum_scatter(gain_grads, ("dp", "tensor"), scatter_dimension=1, tiled=True),
        lax.psum_scatter(shift_grads, ("dp", "tensor"), scatter_dimension=1, tiled=True),
    )
    return (
        jnp.stack(outputs),
        jnp.stack(input_grads),
        weight_grads[0],
        weight_grads[1],
        weight_grads[2],
        weight_grads[3],
        weight_grads[4],
        weight_grads[5],
        gain_share,
        shift_share,
    )


MESH_ID = pl.DeviceIdType.MESH
BF = jnp.bfloat16
F32 = jnp.float32
ROWS = 96
SMALL = 16


def place():
    d = lax.axis_index("dp")
    t = lax.axis_index("tensor")
    k, c = d // 2, d % 2
    xb, yb = k % 2, k // 2
    dx = d + 2 - 4 * xb
    dy = d + 4 - 8 * yb
    return d, t, k, c, xb, yb, dx, dy


def remote(src, dst, send, recv, dp, tensor):
    return pltpu.make_async_remote_copy(
        src_ref=src,
        dst_ref=dst,
        send_sem=send,
        recv_sem=recv,
        device_id=(dp, tensor),
        device_id_type=MESH_ID,
    )


def enter(k, c, t, d, dx, dy):
    barrier = pltpu.get_barrier_semaphore()

    def greet(dp, tensor):
        pl.semaphore_signal(barrier, inc=1, device_id=(dp, tensor), device_id_type=MESH_ID)

    greet(dx, t)
    greet(dy, t)
    greet(d + 1 - 2 * c, t)
    for step in range(1, 4):
        other = (t + step) % 4
        greet(2 * k, other)
        greet(2 * k + 1, other)
    pl.semaphore_wait(barrier, 9)


def gather_steps(place_of, tok, cot, xf, cf, own, full, small_other, sems, chunks):
    d, t, k, c, xb, yb, dx, dy = place_of
    (
        local_sem,
        row_sem,
        ex_send,
        ex_recv,
        fw_send,
        fw_recv,
        p_send,
        p_recv,
        z_send,
        z_recv,
        a_send,
        a_recv,
        b_send,
        b_recv,
        o_send,
        o_recv,
    ) = sems
    mate = d + 1 - 2 * c
    u = t + c * (3 - 2 * t)
    up = t + 1 - 2 * c
    down = t - 1 + 2 * c
    source = t // 2 == c
    half = tok.shape[1] // 2
    rows_of = [w.shape[0] for w in own]

    def shard_spot(s, dp):
        rows = rows_of[s]
        return full[s].at[t % 2, pl.ds(dp * rows, rows)]

    def placed(s):
        @pl.when(source)
        def _():
            pltpu.make_async_copy(own[s], shard_spot(s, d), local_sem.at[s]).start()

        @pl.when(jnp.logical_not(source))
        def _():
            remote(own[s], shard_spot(s, d), p_send.at[s], p_recv.at[s], mate, t).start()

    def row_spot(dst, origin, core):
        return dst.at[pl.ds((origin * 2 + core) * half, half)]

    def exchange(which, src, dst, start=True):
        for m in range(2):
            goal = 2 * c + m
            for core in range(2):
                piece = src.at[m, pl.ds(core * half, half)]
                spot = row_spot(dst, t, core)
                here = jnp.logical_and(goal == t, core == c)
                copy = remote(
                    piece,
                    spot,
                    ex_send.at[which, 2 * m + core],
                    ex_recv.at[which, t],
                    2 * k + core,
                    goal,
                )
                local = pltpu.make_async_copy(piece, spot, row_sem.at[which])

                @pl.when(here)
                def _():
                    if start:
                        local.start()

                @pl.when(jnp.logical_not(here))
                def _():
                    if start:
                        copy.start()
                    else:
                        copy.wait_send()

    def forward(which, dst, origin, core):
        spot = row_spot(dst, origin, core)
        return remote(spot, spot, fw_send.at[which, origin], fw_recv.at[which, origin], mate, t)

    def relay(which, src, dst):
        for origin in range(4):
            spot = row_spot(dst, origin, c)
            here = jnp.logical_and(origin == t, c == t // 2)

            @pl.when(here)
            def _():
                pltpu.make_async_copy(
                    src.at[0, pl.ds(0, half)], spot, row_sem.at[which]
                ).wait()

            @pl.when(jnp.logical_not(here))
            def _():
                remote(
                    spot, spot, ex_send.at[which, 0], ex_recv.at[which, origin], mate, t
                ).wait_recv()

            forward(which, dst, origin, c).start()

    def arrived(which, dst):
        for origin in range(4):
            forward(which, dst, origin, 1 - c).wait_recv()

    def block(i, b, start, n):
        s, col, cols = chunks[i]
        rows = rows_of[s]
        return full[s].at[
            b + c * (1 - 2 * b), pl.ds(start * rows, n * rows), pl.ds(col, cols)
        ]

    def z_copy(i, b, way, target):
        ref = block(i, b, 2 * k, 2)
        return remote(ref, ref, z_send.at[i, b, way], z_recv.at[i, b], d, target)

    def first_copy(i, b):
        ref = block(i, b, 2 * k, 2)
        return remote(ref, ref, a_send.at[i, b], a_recv.at[i, b], dx if b == 0 else dy, t)

    def first_arrival(i, b):
        near = k + 1 - 2 * xb if b == 0 else k + 2 - 4 * yb
        ref = block(i, b, 2 * near, 2)
        return remote(ref, ref, a_send.at[i, b], a_recv.at[i, b], dx if b == 0 else dy, t)

    def second_copies(i, arriving):
        other = 1 if arriving else 0
        row = yb + other * (1 - 2 * yb)
        ref = block(i, 0, 4 * row, 4)
        col = xb + other * (1 - 2 * xb)
        out = [remote(ref, ref, b_send.at[i, 0], b_recv.at[i, 0], dy, t)]
        for r in range(2):
            ref = block(i, 1, 2 * (2 * r + col), 2)
            out.append(remote(ref, ref, b_send.at[i, 1 + r], b_recv.at[i, 1 + r], dx, t))
        return out

    def spread(i, b):
        @pl.when(jnp.logical_and(u >= b, u < 3))
        def _():
            z_copy(i, b, 0, up).start()

        if b == 1:

            @pl.when(u == 1)
            def _():
                z_copy(i, 1, 1, down).start()

        first_copy(i, b).start()

    waited = set()

    def level_own(i):
        s = chunks[i][0]
        if s not in waited:
            waited.add(s)

            @pl.when(source)
            def _():
                pltpu.make_async_copy(own[s], shard_spot(s, d), local_sem.at[s]).wait()
                twin = shard_spot(s, mate)
                remote(twin, twin, p_send.at[s], p_recv.at[s], mate, t).wait_recv()

        for b in range(2):

            @pl.when(u == b)
            def _():
                spread(i, b)

    def level_line(i):
        for b in (1, 0):

            @pl.when(u != b)
            def _():
                z_copy(i, b, 0, up).wait_recv()
                spread(i, b)

    def level_second(i):
        for b in range(2):
            first_arrival(i, b).wait_recv()
        for copy in second_copies(i, False):
            copy.start()

    def level_done(i):
        for copy in second_copies(i, True):
            copy.wait_recv()

    last = len(own) - 1
    swap = remote(full[last], small_other, o_send, o_recv, mate, t)

    def sent_all():
        for which, src, dst in ((0, tok, xf), (1, cot, cf)):
            for origin in range(4):
                forward(which, dst, origin, c).wait_send()
            exchange(which, src, dst, False)
        for s in range(len(own)):

            @pl.when(jnp.logical_not(source))
            def _():
                remote(own[s], shard_spot(s, d), p_send.at[s], p_recv.at[s], mate, t).wait_send()

        for i in range(len(chunks)):
            for b in range(2):

                @pl.when(jnp.logical_and(u >= b, u < 3))
                def _():
                    z_copy(i, b, 0, up).wait_send()

                first_copy(i, b).wait_send()

            @pl.when(u == 1)
            def _():
                z_copy(i, 1, 1, down).wait_send()

            for copy in second_copies(i, False):
                copy.wait_send()

    return types.SimpleNamespace(
        placed=placed,
        exchange=exchange,
        relay=relay,
        arrived=arrived,
        own=level_own,
        line=level_line,
        second=level_second,
        done=level_done,
        swap=swap,
        sent_all=sent_all,
    )


def gather_sems(shards, n_chunks):
    dma = pltpu.SemaphoreType.DMA
    return [
        dma((shards,)),
        dma((2,)),
        dma((2, 4)),
        dma((2, 4)),
        dma((2, 4)),
        dma((2, 4)),
        dma((shards,)),
        dma((shards,)),
        dma((n_chunks, 2, 2)),
        dma((n_chunks, 2)),
        dma((n_chunks, 2)),
        dma((n_chunks, 2)),
        dma((n_chunks, 3)),
        dma((n_chunks, 3)),
        dma,
        dma,
    ]


def gelu_parts(u):
    half = math.sqrt(0.5)
    e = jnp.exp(u * u * -0.5)
    f = 1.0 / (1.0 + (0.3275911 * half) * jnp.abs(u))
    series = 0.5 * 1.061405429 * f - 0.5 * 1.453152027
    series = series * f + 0.5 * 1.421413741
    series = series * f - 0.5 * 0.284496736
    series = series * f + 0.5 * 0.254829592
    tail = series * f * e
    share = jnp.where(u >= 0.0, 1.0 - tail, tail)
    return u * share, share + u * e * (1.0 / math.sqrt(2.0 * math.pi))


def layer(tokens, cotangent, prefix_len, small, shards, arrivals, chunks):
    weights = [jax.ShapeDtypeStruct((2, 8 * w.shape[0], w.shape[1]), BF) for w in shards]
    part_cols = weights[0].shape[2] // 3
    heads_width = 2 * part_cols
    hidden = weights[2].shape[2]
    up_per = hidden // 8
    per = small[0].shape[1]
    grads = weights
    length, width = 4 * tokens.shape[1], tokens.shape[2]
    count = len(grads)
    n_chunks = len(chunks)
    half = length // 8
    blocks = length // BLOCK
    rows_of = [g.shape[1] // 8 for g in grads]

    n_sems = len(gather_sems(1, 1))

    def kernel(*refs):
        tok, cot = refs[:2]
        prefix_ref = refs[2]
        small_refs = refs[3:7]
        own = refs[7 : 7 + count]
        base = 7 + count
        res_out, tgr_out, tile_own, tile_mate = refs[base : base + 4]
        final = refs[base + 4 : base + 4 + count]
        sems = refs[base + 4 + count : base + 4 + count + n_sems]
        base += 4 + count + n_sems
        got1 = refs[base : base + count]
        sum1 = refs[base + count : base + 2 * count]
        got2 = refs[base + 2 * count : base + 3 * count]
        sum2 = refs[base + 3 * count : base + 4 * count]
        got3 = refs[base + 4 * count : base + 5 * count]
        sum3 = refs[base + 5 * count : base + 6 * count]
        got4 = refs[base + 6 * count : base + 7 * count]
        got5 = refs[base + 7 * count : base + 8 * count]
        (
            row_sem,
            ex_send,
            ex_recv,
            a_send,
            a_recv,
            b_send,
            b_recv,
            z_send,
            z_recv,
            y_send,
            y_recv,
            p_send,
            p_recv,
            wq,
            wo,
            wu,
            wd,
            q_ref,
            k_ref,
            v_ref,
            o_ref,
            lt_ref,
            small_own,
            small_a,
            small_b,
            x_rows,
            small_rows,
            row_values,
            out_both,
            n1_rows,
            inv_rows,
            residual_rows,
            res_rows,
            low_rows,
            feed_rows,
            branch_rows,
            sent,
            pool,
            active,
            upper,
            do_ref,
            dots,
            acc,
            acc_rows,
            e_send,
            e_recv,
            s_send,
            s_recv,
            t_send,
            t_recv,
            tile_sum,
            tile_got,
        ) = refs[base + 8 * count :]
        cot_rows = pool.at[2]
        part = (wq, wo, wu, pool.at[pl.ds(1, 2), pl.ds(0, width)])
        mixed = active
        dq, dk, dv = (
            upper.at[0, :, pl.ds(0, heads_width)],
            upper.at[0, :, pl.ds(heads_width, heads_width)],
            upper.at[1, :, pl.ds(0, heads_width)],
        )
        d, t, k, c, xb, yb, dx, dy = place()
        mate = d + 1 - 2 * c
        u = t + c * (3 - 2 * t)
        up = t + 1 - 2 * c
        down = t - 1 + 2 * c
        source = u <= 1
        enter(k, c, t, d, dx, dy)

        def plane(b):
            return b + c * (1 - 2 * b)

        def first_copies(i):
            s, col, cols = chunks[i]
            rows = rows_of[s]
            spot = pl.ds(col, cols)
            out = [
                remote(
                    part[s].at[plane(0), pl.ds((1 - yb) * 4 * rows, 4 * rows), spot],
                    got1[s].at[0, :, spot],
                    a_send.at[i, 0],
                    a_recv.at[i, 0],
                    dy,
                    t,
                )
            ]
            for r in range(2):
                out.append(
                    remote(
                        part[s].at[plane(1), pl.ds((2 * r + 1 - xb) * 2 * rows, 2 * rows), spot],
                        got1[s].at[1, pl.ds(r * 2 * rows, 2 * rows), spot],
                        a_send.at[i, 1 + r],
                        a_recv.at[i, 1 + r],
                        dx,
                        t,
                    )
                )
            return out

        def second_copies(i):
            s, col, cols = chunks[i]
            rows = rows_of[s]
            spot = pl.ds(col, cols)
            out = []
            for b, far, goal in ((0, 1 - xb, dx), (1, 1 - yb, dy)):
                out.append(
                    remote(
                        sum1[s].at[b, pl.ds(far * 2 * rows, 2 * rows), spot],
                        got2[s].at[b, :, spot],
                        b_send.at[i, b],
                        b_recv.at[i, b],
                        goal,
                        t,
                    )
                )
            return out

        def low(v, s):
            return v.astype(sum1[s].dtype)

        def level_first(i):
            for copy in first_copies(i):
                copy.start()

        def level_second(i):
            s, col, cols = chunks[i]
            rows = rows_of[s]
            spot = pl.ds(col, cols)
            for copy in first_copies(i):
                copy.wait_recv()
            mine = part[s][plane(0), pl.ds(yb * 4 * rows, 4 * rows), spot]
            sum1[s][0, :, spot] = low(mine.astype(F32) + got1[s][0, :, spot].astype(F32), s)
            for r in range(2):
                mine = part[s][plane(1), pl.ds((2 * r + xb) * 2 * rows, 2 * rows), spot]
                there = pl.ds(r * 2 * rows, 2 * rows)
                sum1[s][1, there, spot] = low(
                    mine.astype(F32) + got1[s][1, there, spot].astype(F32), s
                )
            for copy in second_copies(i):
                copy.start()

        def z_copy(i, b):
            s, col, cols = chunks[i]
            spot = pl.ds(col, cols)
            return remote(
                sum3[s].at[b, :, spot],
                got3[s].at[b, :, spot],
                z_send.at[i, b],
                z_recv.at[i, b],
                d,
                down,
            )

        def y_copy(i):
            s, col, cols = chunks[i]
            spot = pl.ds(col, cols)
            return remote(
                sum3[s].at[1, :, spot], got4[s].at[:, spot], y_send.at[i], y_recv.at[i], d, up
            )

        def level_line(i):
            s, col, cols = chunks[i]
            rows = rows_of[s]
            spot = pl.ds(col, cols)
            for copy in second_copies(i):
                copy.wait_recv()
            for b, near in ((0, xb), (1, yb)):
                mine = sum1[s][b, pl.ds(near * 2 * rows, 2 * rows), spot]
                sum2[s][b, :, spot] = mine.astype(F32) + got2[s][b, :, spot].astype(F32)

            @pl.when(u == 3)
            def _():
                for b in range(2):
                    sum3[s][b, :, spot] = low(sum2[s][b, :, spot], s)
                    z_copy(i, b).start()

            @pl.when(u == 0)
            def _():
                sum3[s][1, :, spot] = low(sum2[s][1, :, spot], s)
                y_copy(i).start()

        def level_pass(i):
            s, col, cols = chunks[i]
            spot = pl.ds(col, cols)

            @pl.when(u == 2)
            def _():
                for b in range(2):
                    z_copy(i, b).wait_recv()
                    sum3[s][b, :, spot] = low(
                        sum2[s][b, :, spot] + got3[s][b, :, spot].astype(F32), s
                    )
                    z_copy(i, b).start()

        def level_near(i):
            s, col, cols = chunks[i]
            spot = pl.ds(col, cols)

            @pl.when(u == 1)
            def _():
                z_copy(i, 0).wait_recv()
                sum3[s][0, :, spot] = low(
                    sum2[s][0, :, spot] + got3[s][0, :, spot].astype(F32), s
                )
                z_copy(i, 0).start()
                z_copy(i, 1).wait_recv()
                y_copy(i).wait_recv()
                total = (
                    sum2[s][1, :, spot]
                    + got3[s][1, :, spot].astype(F32)
                    + got4[s][:, spot].astype(F32)
                )
                finish(i, total)

            @pl.when(u == 0)
            def _():
                z_copy(i, 0).wait_recv()
                finish(i, sum2[s][0, :, spot] + got3[s][0, :, spot].astype(F32))

        def p_copy(i):
            s, col, cols = chunks[i]
            rows = rows_of[s]
            spot = pl.ds(col, cols)
            return remote(
                sum1[s].at[0, pl.ds((1 - c) * rows, rows), spot],
                got5[s].at[:, spot],
                p_send.at[i],
                p_recv.at[i],
                mate,
                t,
            )

        def finish(i, total):
            s, col, cols = chunks[i]
            rows = rows_of[s]
            spot = pl.ds(col, cols)
            for copy in second_copies(i):
                copy.wait_send()
            sum2[s][0, :, spot] = total
            sum1[s][0, pl.ds(0, 2 * rows), spot] = low(total, s)
            p_copy(i).start()
            final[s][:, spot] = sum2[s][0, pl.ds(c * rows, rows), spot]

        def level_mate(i):
            s, col, cols = chunks[i]
            spot = pl.ds(col, cols)

            @pl.when(u >= 2)
            def _():
                p_copy(i).wait_recv()
                final[s][:, spot] = got5[s][:, spot].astype(F32)

        def pack():
            row_values[...] = jnp.zeros_like(row_values)
            tile = small_rows.at[pl.ds(0, SMALL)]
            tile[...] = jnp.zeros((SMALL, 128), F32)
            row = 0
            for ref in small_refs:
                tile[row : row + ref.shape[0], 0 : ref.shape[1]] = ref[...].astype(F32)
                row += ref.shape[0]
            lane = lax.broadcasted_iota(jnp.int32, (1, 128), 1)
            line = jnp.zeros((1, 128), jnp.int32)
            for member in range(2):
                value = prefix_ref[member]
                line = jnp.where(lane == member, value // 16, line)
                line = jnp.where(lane == 2 + member, value % 16, line)
            tile[row : row + 1, :] = line.astype(F32)
            small_own[...] = tile[...].astype(BF)

        def widen(rows, size, spot):
            n, wide = rows.shape[0], row_values.shape[1]
            at = lax.broadcasted_iota(jnp.int32, (128, wide), 0)
            lane = lax.broadcasted_iota(jnp.int32, (128, wide), 1)
            v = jnp.dot(
                rows,
                (at == lane % size).astype(F32),
                precision=lax.Precision.HIGHEST,
                preferred_element_type=F32,
            )
            row = lax.broadcasted_iota(jnp.int32, (n, wide), 0)
            lane = lax.broadcasted_iota(jnp.int32, (n, wide), 1)
            return jnp.sum(jnp.where(lane // size == spot(row), v, 0.0), axis=0, keepdims=True)

        def unpack():
            for z in range(2):
                small_rows[pl.ds((2 * c + z) * 8 * SMALL, 8 * SMALL), :] = small_a[z].astype(F32)
                small_rows[pl.ds((2 - 2 * c + z) * 8 * SMALL, 8 * SMALL), :] = small_b[z].astype(F32)
            for kind in range(6):
                rows = small_rows[pl.ds(3 + kind, 32, stride=SMALL), :]
                row_values[kind : kind + 1, :] = widen(
                    rows, per, lambda row: (row % 8) * 4 + row // 8
                )
            for z in range(2):
                rows = small_rows[pl.ds((2 * c + z) * 8 * SMALL + 2, 8, stride=SMALL), :]
                row_values[6 + z : 7 + z, :] = widen(rows, up_per, lambda row: row)

        def bias_row(kind):
            out = []
            for z in range(2):
                rows = small_rows[pl.ds((2 * c + z) * 8 * SMALL + kind, 8, stride=SMALL), :]
                out.append(widen(rows, per, lambda row: row)[:, :part_cols])
            return jnp.concatenate(out, axis=1)

        def prefix_value():
            tile = small_rows[pl.ds((2 * k + t // 2) * SMALL + 9, 1), :]
            lane = lax.broadcasted_iota(jnp.int32, (1, 128), 1)
            member = t % 2
            sixteens = jnp.sum(jnp.where(lane == member, tile, 0.0), axis=1, keepdims=True)
            units = jnp.sum(jnp.where(lane == 2 + member, tile, 0.0), axis=1, keepdims=True)
            return 16.0 * sixteens + units

        def project_block(bias_q, bias_v, i):
            rows = pl.ds(i * BLOCK, BLOCK)
            both = [
                jnp.dot(x_rows[rows, :], wq[z], preferred_element_type=F32) for z in range(2)
            ]

            def kind(j):
                return jnp.concatenate(
                    [v[:, j * part_cols : (j + 1) * part_cols] for v in both], axis=1
                )

            q_ref[rows, :] = (kind(0) + bias_q).astype(BF)
            k_ref[rows, :] = kind(1).astype(BF)
            v_ref[rows, :] = (kind(2) + bias_v).astype(BF)

        def value_row(i):
            return row_values[i : i + 1, :]

        def swap_copy(which, i):
            rows = pl.ds(i * BLOCK, BLOCK)
            return remote(
                sent.at[rows],
                pool.at[which % 2, rows],
                e_send.at[which, i],
                e_recv.at[which, i],
                mate,
                t,
            )

        def swapped(which, i):
            rows = pl.ds(i * BLOCK, BLOCK)
            swap_copy(which, i).wait()
            return sent[rows, :].astype(F32) + pool[which % 2, rows, :].astype(F32)

        def swap(which, i, share):
            sent[pl.ds(i * BLOCK, BLOCK), :] = share.astype(BF)
            swap_copy(which, i).start()

        def normalize(v):
            center = v - jnp.mean(v, axis=1, keepdims=True)
            inverse = lax.rsqrt(jnp.mean(center * center, axis=1, keepdims=True) + EPSILON)
            return center * inverse, inverse

        def norm_pull(scaled, normal, inverse):
            first = jnp.mean(scaled, axis=1, keepdims=True)
            second = jnp.mean(scaled * normal, axis=1, keepdims=True)
            return inverse * (scaled - first - normal * second)

        def tally(row, v):
            tile_sum[0, row : row + 1, :] += jnp.sum(v, axis=0, keepdims=True)

        def branch_block(i):
            swap(0, i, dot_nt(o_ref[pl.ds(i * BLOCK, BLOCK), :], out_both[...]))

        def forward_block(i):
            rows = pl.ds(i * BLOCK, BLOCK)
            branch = swapped(0, i) + value_row(2)
            normal, inverse = normalize(x_rows[rows, :].astype(F32) + branch)
            n1_rows[rows, :] = normal
            inv_rows[rows, :] = jnp.broadcast_to(inverse, (BLOCK, 128))
            low_rows[rows, :] = (normal * value_row(0) + value_row(3)).astype(BF)

        def up_block(col, i):
            rows, cols = pl.ds(i * BLOCK, BLOCK), pl.ds(col, BLOCK)
            for z in range(2):
                u = jnp.dot(low_rows[rows, :], wu[z, :, cols], preferred_element_type=F32)
                value, slope = gelu_parts(u + row_values[6 + z : 7 + z, cols])
                active[z, rows, cols] = value.astype(BF)
                upper[z, rows, cols] = slope.astype(BF)

        def down_block(col, i):
            rows, cols = pl.ds(i * BLOCK, BLOCK), pl.ds(col, BLOCK)
            share = dot_nt(active[0, rows, cols], wd[0, :, cols])
            share = share + dot_nt(active[1, rows, cols], wd[1, :, cols])
            if col:
                share = share + residual_rows[rows, :]
            if col + BLOCK < hidden:
                residual_rows[rows, :] = share
            else:
                swap(1, i, share)

        def row_home(i):
            return jnp.logical_and(i == t, c == t // 2)

        def out_copy(i):
            return remote(
                res_rows.at[pl.ds((2 * i + c) * half, half)],
                res_out.at[t % 2, pl.ds(c * half, half)],
                ex_send.at[0, i],
                ex_recv.at[0, t % 2, c],
                2 * k + t // 2,
                i,
            )

        def output_block(i):
            rows = pl.ds(i * BLOCK, BLOCK)
            feed_out = swapped(1, i) + value_row(4)
            normed = n1_rows[rows, :] * value_row(0) + value_row(3)
            normal, inverse = normalize(normed + feed_out)
            res_rows[rows, :] = (normal * value_row(1) + value_row(5)).astype(BF)
            incoming = cot_rows[rows, :].astype(F32)
            tally(7, incoming * normal)
            tally(11, incoming)
            residual = norm_pull(incoming * value_row(1), normal, inverse)
            residual_rows[rows, :] = residual
            feed = residual.astype(BF)
            feed_rows[rows, :] = feed
            tally(10, feed.astype(F32))
            @pl.when(row_home(i))
            def _():
                store = pltpu.make_async_copy(
                    res_rows.at[pl.ds((2 * i + c) * half, half)],
                    res_out.at[t % 2, pl.ds(c * half, half)],
                    row_sem,
                )
                store.start()
                store.wait()

            @pl.when(jnp.logical_not(row_home(i)))
            def _():
                out_copy(i).start()

        def feed_back_block(i):
            rows = pl.ds(i * BLOCK, BLOCK)
            for z in range(2):
                for col in range(0, hidden, BLOCK):
                    cols = pl.ds(col, BLOCK)
                    pull = jnp.dot(feed_rows[rows, :], wd[z, :, cols], preferred_element_type=F32)
                    grad = (pull * upper[z, rows, cols].astype(F32)).astype(BF)
                    upper[z, rows, cols] = grad
                    tile_sum[0, 4 + z : 5 + z, cols] += jnp.sum(
                        grad.astype(F32), axis=0, keepdims=True
                    )
            swap(2, i, dot_nt(upper[0, rows, :], wu[0]) + dot_nt(upper[1, rows, :], wu[1]))

        def branch_back_block(i):
            rows = pl.ds(i * BLOCK, BLOCK)
            grad = residual_rows[rows, :] + swapped(2, i)
            normal = n1_rows[rows, :]
            tally(6, grad * normal)
            tally(9, grad)
            residual = norm_pull(grad * value_row(0), normal, inv_rows[rows, 0:1])
            residual_rows[rows, :] = residual
            low_grad = residual.astype(BF)
            branch_rows[rows, :] = low_grad
            tally(8, low_grad.astype(F32))
            do_ref[rows, :] = jnp.dot(
                branch_rows[rows, :], out_both[...], preferred_element_type=F32
            ).astype(BF)

        def outer(left, j, right):
            return dot_tn(left[:, pl.ds(j * BLOCK, BLOCK)], right).astype(BF)

        def down_grad(z, j):
            pool[1 + z, pl.ds(j * BLOCK, BLOCK), :] = outer(feed_rows, j, active[z])

        def up_grad(z, j):
            wu[z, pl.ds(j * BLOCK, BLOCK), :] = outer(low_rows, j, upper[z])

        def out_grad(j):
            both = outer(branch_rows, j, o_ref[...])
            for z in range(2):
                wo[z, pl.ds(j * BLOCK, BLOCK), :] = both[:, z * part_cols : (z + 1) * part_cols]

        def attention(pair, kb):
            if kb == 0:
                back_start(pair, o_ref, do_ref, dots, acc)
            back_block(
                pair, kb, q_ref, k_ref, v_ref, lt_ref, do_ref, dots, acc, dk, dv, limit
            )
            if kb == blocks - 1:
                dq[:, pl.ds(pair * 128, 128)] = (acc[...] * DH**-0.5).astype(BF)

        def mate_spot(i):
            return pool.at[1 + i // 2, pl.ds(length - BLOCK + i % 2 * half, half)]

        def mate_copy(i):
            return remote(
                sent.at[pl.ds(i * half, half)],
                mate_spot(i),
                t_send.at[0, i],
                t_recv.at[0, i],
                mate,
                t,
            )

        def mix(i):
            rows = pl.ds(i * BLOCK, BLOCK)
            kinds = [ref[rows, :] for ref in (dq, dk, dv)]
            share = jnp.zeros((BLOCK, width), F32)
            for z in range(2):
                both = jnp.concatenate(
                    [v[:, z * part_cols : (z + 1) * part_cols] for v in kinds], axis=1
                )
                mixed[z, rows, 0 : 3 * part_cols] = both
                share = share + dot_nt(both, wq[z])
            acc_rows[...] = share
            sent[pl.ds(i * half, half), :] = acc_rows[pl.ds((1 - c) * half, half), :].astype(BF)
            residual_rows[pl.ds((2 * i + c) * half, half), :] += acc_rows[pl.ds(c * half, half), :]
            mate_copy(i).start()

        def row_copy(i):
            return remote(
                low_rows.at[pl.ds(i * half, half)],
                tgr_out.at[t % 2, pl.ds(c * half, half)],
                t_send.at[1, i],
                t_recv.at[1, 2 * (t % 2) + c],
                2 * k + t // 2,
                i,
            )

        def send_rows(i):
            mate_copy(i).wait_recv()
            low_rows[pl.ds(i * half, half), :] = (
                residual_rows[pl.ds((2 * i + c) * half, half), :] + mate_spot(i)[...].astype(F32)
            ).astype(BF)
            here = row_home(i)

            @pl.when(here)
            def _():
                store = pltpu.make_async_copy(
                    low_rows.at[pl.ds(i * half, half)], tgr_out.at[t % 2, pl.ds(c * half, half)], row_sem
                )
                store.start()
                store.wait()

            @pl.when(jnp.logical_not(here))
            def _():
                row_copy(i).start()

        def settle_rows():
            for i in range(4):
                mate_copy(i).wait_send()

                @pl.when(jnp.logical_not(jnp.logical_and(i == t, c == t // 2)))
                def _():
                    row_copy(i).wait_send()

            for m in range(2):
                for core in range(2):
                    spot = tgr_out.at[m, pl.ds(core * half, half)]

                    @pl.when(jnp.logical_not(jnp.logical_and(2 * c + m == t, core == c)))
                    def _():
                        remote(
                            low_rows.at[pl.ds(0, half)],
                            spot,
                            t_send.at[1, 0],
                            t_recv.at[1, 2 * m + core],
                            mate,
                            t,
                        ).wait_recv()

        def weight_grad(j):
            rows = pl.ds(j * BLOCK, BLOCK)
            for z in range(2):
                wq[z, rows, :] = outer(x_rows, j, mixed[z, :, 0 : 3 * part_cols])

        def tile_copy(stage, goal_dp, goal_t, slot):
            return remote(
                tile_sum.at[stage],
                tile_got.at[slot],
                s_send.at[slot],
                s_recv.at[slot],
                goal_dp,
                goal_t,
            )

        def tile_start():
            for row, ref in ((0, dq), (2, dv)):
                sums = jnp.sum(ref[...].astype(F32), axis=0, keepdims=True)
                for z in range(2):
                    tile_sum[0, row + z : row + z + 1, 0:part_cols] = sums[
                        :, z * part_cols : (z + 1) * part_cols
                    ]
            tile_copy(0, dx, t, 0).start()

        def tile_second():
            tile_copy(0, dx, t, 0).wait_recv()
            tile_sum[1] = tile_sum[0] + tile_got[0]
            tile_copy(1, dy, t, 1).start()

        def tile_third():
            tile_copy(1, dy, t, 1).wait_recv()
            tile_sum[2] = tile_sum[1] + tile_got[1]
            for step in range(1, 4):
                tile_copy(2, d, (t + step) % 4, 1 + step).start()

        def tile_fourth():
            for step in range(1, 4):
                tile_copy(2, d, t, 1 + step).wait_recv()
            tile_sum[3] = (tile_sum[2] + tile_got[2]) + (tile_got[3] + tile_got[4])
            tile_copy(3, mate, t, 5).start()

        def tile_last():
            tile_copy(3, mate, t, 5).wait_recv()
            tile_own[...] = tile_sum[3]
            tile_mate[...] = tile_got[5]
            for slot, stage in enumerate((0, 1, 2, 2, 2, 3)):
                tile_copy(stage, mate, t, slot).wait_send()

        levels = [level_first, level_second, level_line, level_pass, level_near, level_mate]
        come = gather_steps(
            (d, t, k, c, xb, yb, dx, dy),
            tok,
            cot,
            x_rows,
            cot_rows,
            (*own, small_own),
            (wq, wo, wu, wd, small_a),
            small_b,
            sems,
            arrivals,
        )
        pack()
        come.placed(4)
        for i in range(4):
            come.placed(i)
        tile_sum[0] = jnp.zeros(tile_sum.shape[1:], F32)
        for i in range(5):
            come.own(i)
        for i in range(4):
            come.line(i)
        come.exchange(0, tok, x_rows)
        for i in range(3):
            come.own(5 + i)
            come.second(i)
        come.line(4)
        come.second(3)
        come.done(0)
        come.swap.start()
        come.second(4)
        come.relay(0, tok, x_rows)
        for i in range(8, 11):
            come.own(i)
        come.swap.wait()
        unpack()
        limit = prefix_value()
        bias_q, bias_v = bias_row(0), bias_row(1)
        come.line(5)
        come.arrived(0, x_rows)
        for i in range(1, 4):
            come.done(i)
        pl.loop(0, blocks)(partial(project_block, bias_q, bias_v))
        todo = [
            (come.line, 6),
            (come.second, 5),
            (come.line, 7),
            None,
            (come.line, 8),
            (come.second, 6),
            (come.line, 9),
            None,
            (come.line, 10),
            (come.exchange, 1, cot, cot_rows),
            (come.second, 7),
            None,
        ]
        for unit in range(heads_width // 128 * blocks):
            if todo[unit]:
                todo[unit][0](*todo[unit][1:])
            attend_rows(
                q_ref, k_ref, v_ref, o_ref, lt_ref, limit, unit // blocks, unit % blocks
            )
        come.done(4)
        out_both[...] = jnp.concatenate([wo[0], wo[1]], axis=1)
        pl.loop(0, blocks)(branch_block)
        pl.loop(0, blocks)(forward_block)
        come.second(8)
        for j in range(hidden // BLOCK):
            come.done(5 + 2 * j)
            pl.loop(0, blocks)(partial(up_block, j * BLOCK))
            if j < 2:
                come.second(9 + j)
            else:
                come.relay(1, cot, cot_rows)
            come.done(6 + 2 * j)
            pl.loop(0, blocks)(partial(down_block, j * BLOCK))
        come.arrived(1, cot_rows)
        pl.loop(0, blocks)(output_block)
        come.sent_all()
        pl.loop(0, width // BLOCK)(lambda j: [down_grad(z, j) for z in range(2)] and None)
        for i in range(2):
            level_first(i)
        pl.loop(0, blocks)(feed_back_block)
        pl.loop(0, width // BLOCK)(lambda j: [up_grad(z, j) for z in range(2)] and None)
        level_first(2)
        pl.loop(0, blocks)(branch_back_block)
        pl.loop(0, width // BLOCK)(out_grad)
        work = [
            partial(attention, pair, kb)
            for pair in range(heads_width // 128)
            for kb in range(blocks)
        ]
        work += [partial(mix, i) for i in range(blocks)]
        work += [partial(weight_grad, j) for j in range(width // BLOCK)]
        done = 0
        late = 5
        for slot in range(n_chunks + 4):
            for lag, level in enumerate(levels[1:]):
                if 0 <= slot - lag < n_chunks:
                    level(slot - lag)
            if slot + 3 < late:
                level_first(slot + 3)
            if slot < late:
                upto = -(-len(work) * (slot + 1) // late)
                for unit in work[done:upto]:
                    unit()
                done = upto
            if slot == late - 1:
                for i in range(late, n_chunks):
                    level_first(i)
                tile_start()
                for i in range(4):
                    send_rows(i)
            elif slot >= late and slot - late < 4:
                (tile_second, tile_third, tile_fourth, tile_last)[slot - late]()
        for i in range(4):

            @pl.when(jnp.logical_not(row_home(i)))
            def _():
                out_copy(i).wait_send()

        for m in range(2):
            for core in range(2):
                spot = res_out.at[m, pl.ds(core * half, half)]

                @pl.when(jnp.logical_not(jnp.logical_and(2 * c + m == t, core == c)))
                def _():
                    remote(
                        res_rows.at[pl.ds(0, half)],
                        spot,
                        ex_send.at[0, 0],
                        ex_recv.at[0, m, core],
                        mate,
                        t,
                    ).wait_recv()

        settle_rows()
        for i in range(n_chunks):
            for copy in first_copies(i):
                copy.wait_send()

            @pl.when(u >= 2)
            def _():
                for copy in second_copies(i):
                    copy.wait_send()
                for b in range(2):
                    z_copy(i, b).wait_send()

            @pl.when(u == 1)
            def _():
                z_copy(i, 0).wait_send()

            @pl.when(u == 0)
            def _():
                y_copy(i).wait_send()

            @pl.when(u <= 1)
            def _():
                p_copy(i).wait_send()

    any_spec = pl.BlockSpec(memory_space=pl.ANY)
    vmem = pl.BlockSpec(memory_space=pltpu.VMEM)
    dma = pltpu.SemaphoreType.DMA
    scratch = []
    for kind in range(8):
        for s in range(count):
            rows, cols, kept = rows_of[s], grads[s].shape[2], grads[s].dtype
            shape, dtype = (
                ((2, 4 * rows, cols), kept),
                ((2, 4 * rows, cols), kept),
                ((2, 2 * rows, cols), kept),
                ((2, 2 * rows, cols), F32),
                ((2, 2 * rows, cols), kept),
                ((2, 2 * rows, cols), kept),
                ((2 * rows, cols), kept),
                ((rows, cols), kept),
            )[kind]
            scratch.append(pltpu.VMEM(shape, dtype))
    back = jax.ShapeDtypeStruct((2, 2 * half, width), BF)
    tiles = jax.ShapeDtypeStruct((16, hidden), F32)
    outs = pl.pallas_call(
        kernel,
        out_shape=[
            back,
            back,
            tiles,
            tiles,
            *[jax.ShapeDtypeStruct((r, g.shape[2]), F32) for r, g in zip(rows_of, grads)],
        ],
        in_specs=[any_spec] * 2
        + [pl.BlockSpec(memory_space=pltpu.SMEM)]
        + [vmem] * 4
        + [any_spec] * count,
        out_specs=[any_spec, any_spec] + [vmem] * (2 + count),
        scratch_shapes=[
            *gather_sems(count + 1, len(arrivals)),
            *scratch,
            dma,
            dma((1, 4)),
            dma((1, 2, 2)),
            dma((n_chunks, 3)),
            dma((n_chunks, 3)),
            dma((n_chunks, 2)),
            dma((n_chunks, 2)),
            dma((n_chunks, 2)),
            dma((n_chunks, 2)),
            dma((n_chunks,)),
            dma((n_chunks,)),
            dma((n_chunks,)),
            dma((n_chunks,)),
            *[pltpu.VMEM(w.shape, BF) for w in weights],
            *[pltpu.VMEM((length, heads_width), BF)] * 4,
            pltpu.VMEM((heads_width // DH, 8, length), F32),
            pltpu.VMEM((SMALL, 128), BF),
            pltpu.VMEM((2, 8 * SMALL, 128), BF),
            pltpu.VMEM((2, 8 * SMALL, 128), BF),
            pltpu.VMEM((length, width), BF),
            pltpu.VMEM((32 * SMALL, 128), F32),
            pltpu.VMEM((8, width), F32),
            pltpu.VMEM((width, heads_width), BF),
            pltpu.VMEM((length, width), F32),
            pltpu.VMEM((length, 128), F32),
            pltpu.VMEM((length, width), F32),
            pltpu.VMEM((length, width), BF),
            pltpu.VMEM((length, width), BF),
            pltpu.VMEM((length, width), BF),
            pltpu.VMEM((length, width), BF),
            pltpu.VMEM((length, width), BF),
            pltpu.VMEM((3, length, width), BF),
            pltpu.VMEM((2, length, hidden), BF),
            pltpu.VMEM((2, length, hidden), BF),
            pltpu.VMEM((length, heads_width), BF),
            pltpu.VMEM((8, length), F32),
            pltpu.VMEM((length, 128), F32),
            pltpu.VMEM((BLOCK, width), F32),
            dma((3, blocks)),
            dma((3, blocks)),
            dma((6,)),
            dma((6,)),
            dma((2, 4)),
            dma((2, 4)),
            pltpu.VMEM((4, *tiles.shape), F32),
            pltpu.VMEM((6, *tiles.shape), F32),
        ],
        compiler_params=pltpu.CompilerParams(
            collective_id=2, has_side_effects=True, vmem_limit_bytes=67043328
        ),
    )(tokens, cotangent, prefix_len, *small, *shards)
    return outs[0], outs[1], outs[2], outs[3], outs[4:]


BLOCK = 256


def lane_half(shape, h):
    lane = lax.broadcasted_iota(jnp.int32, shape, 1)
    return lane < DH if h == 0 else lane >= DH


def reach(row_block, blocks):
    return max(row_block + 1, blocks // 2)


def dot_nt(a, b):
    return lax.dot_general(a, b, (((1,), (1,)), ((), ())), preferred_element_type=F32)


def dot_tn(a, b):
    return lax.dot_general(a, b, (((0,), (0,)), ((), ())), preferred_element_type=F32)


def attend_rows(q_ref, k_ref, v_ref, o_ref, lt_ref, limit, pair, qb):
    length = q_ref.shape[0]
    blocks = length // BLOCK
    lanes = pl.ds(pair * 128, 128)
    rows = pl.ds(qb * BLOCK, BLOCK)
    span = reach(qb, blocks) * BLOCK
    q = q_ref[rows, lanes] * jnp.asarray(DH**-0.5, BF)
    heads = []
    for h in range(2):
        half = lane_half((BLOCK, 128), h)
        s = dot_nt(jnp.where(half, q, jnp.zeros_like(q)), k_ref[pl.ds(0, span), lanes])
        clear = qb * BLOCK
        row = lax.broadcasted_iota(jnp.int32, (BLOCK, span - clear), 0) + clear
        col = lax.broadcasted_iota(jnp.int32, (BLOCK, span - clear), 1) + clear
        seen = col <= row
        if clear < length // 2:
            seen = jnp.logical_or(seen, col.astype(F32) < limit)
        tail = jnp.where(seen, s[:, clear:], MASKED_SCORE)
        s = jnp.concatenate([s[:, :clear], tail], axis=1) if clear else tail
        top = jnp.max(s, axis=1, keepdims=True)
        p = jnp.exp(s - top)
        total = jnp.sum(p, axis=1, keepdims=True)
        log_total = top + jnp.log(total)
        lt_ref[2 * pair + h, 0:1, rows] = jnp.transpose(
            jnp.broadcast_to(log_total, (BLOCK, 128))
        )[0:1, :]
        context = jnp.dot(p.astype(BF), v_ref[pl.ds(0, span), lanes], preferred_element_type=F32)
        heads.append(context * (1.0 / total))
    o_ref[rows, lanes] = jnp.where(lane_half((BLOCK, 128), 0), heads[0], heads[1]).astype(BF)


def back_start(pair, o_ref, do_ref, dots, acc):
    head_row = lax.broadcasted_iota(jnp.int32, (8, 128), 0)
    lane = lax.broadcasted_iota(jnp.int32, (8, 128), 1)
    pick = (lane // DH == head_row).astype(F32)
    lanes = pl.ds(pair * 128, 128)
    dots[...] = lax.dot_general(
        pick,
        do_ref[:, lanes].astype(F32) * o_ref[:, lanes].astype(F32),
        (((1,), (1,)), ((), ())),
        precision=lax.Precision.HIGHEST,
        preferred_element_type=F32,
    )
    acc[...] = jnp.zeros_like(acc)


def back_block(pair, kb, q_ref, k_ref, v_ref, lt_ref, do_ref, dots, acc, dk_ref, dv_ref, limit):
    length = q_ref.shape[0]
    blocks = length // BLOCK
    lanes = pl.ds(pair * 128, 128)
    keys_at = pl.ds(kb * BLOCK, BLOCK)
    key = k_ref[keys_at, lanes]
    value = v_ref[keys_at, lanes]
    zero = jnp.zeros((BLOCK, 128), BF)
    dk = jnp.zeros((BLOCK, 128), F32)
    dv = jnp.zeros((BLOCK, 128), F32)
    for qb in range(blocks):
        if kb >= reach(qb, blocks):
            continue
        rows = pl.ds(qb * BLOCK, BLOCK)
        q_pair = q_ref[rows, lanes] * jnp.asarray(DH**-0.5, BF)
        do_pair = do_ref[rows, lanes]
        for h in range(2):
            half = lane_half((BLOCK, 128), h)
            q = jnp.where(half, q_pair, zero)
            do = jnp.where(half, do_pair, zero)
            s = dot_nt(key, q)
            if kb >= qb:
                key_id = lax.broadcasted_iota(jnp.int32, (BLOCK, BLOCK), 0) + kb * BLOCK
                row_id = lax.broadcasted_iota(jnp.int32, (BLOCK, BLOCK), 1) + qb * BLOCK
                seen = key_id <= row_id
                if kb * BLOCK < length // 2:
                    seen = jnp.logical_or(seen, key_id.astype(F32) < limit)
                s = jnp.where(seen, s, MASKED_SCORE)
            p = jnp.exp(s - lt_ref[2 * pair + h, 0:1, rows])
            dp = dot_nt(value, do)
            ds = (p * (dp - dots[h : h + 1, rows])).astype(BF)
            dv = dv + jnp.dot(p.astype(BF), do, preferred_element_type=F32)
            dk = dk + jnp.dot(ds, q, preferred_element_type=F32)
            acc[rows, :] += dot_tn(ds, jnp.where(half, key, zero))
    dk_ref[keys_at, lanes] = dk.astype(BF)
    dv_ref[keys_at, lanes] = dv.astype(BF)


def chip_local(
    tokens, prefix_len, w_qkv, bias_qv, w_out, w_up, bias_up, w_down, gains, shifts, cotangent
):
    d, t, k, c, _, _, _, _ = place()
    part = w_qkv.shape[2]
    hidden = w_up.shape[1]

    shards = (
        w_qkv.reshape(ROWS, 3 * part),
        w_out.T,
        w_up,
        w_down.T,
    )
    third = hidden // 3
    first = [(0, 0, 256), (0, 256, 128), (0, 384, 3 * part - 384)]
    up_chunks = [(2, i * third, third) for i in range(3)]
    down_chunks = [(3, i * third, third) for i in range(3)]
    chunks = [(4, 0, 128), *first, (1, 0, part)]
    for pair in zip(up_chunks, down_chunks):
        chunks.extend(pair)
    per = bias_qv.shape[1]
    small = (bias_qv, bias_up[None], gains, shifts)
    half = hidden // 2
    back_chunks = [(i, h * half, half) for i in (3, 2) for h in range(2)]
    back_chunks += [(1, 0, part), (0, 0, 256), (0, 256, 3 * part - 256)]
    out_rows, token_rows, tile_own, tile_mate, finals = layer(
        tokens, cotangent, prefix_len, small, shards, chunks, back_chunks
    )
    plane_rows = jnp.where(c == t // 2, tile_own, tile_mate)[:6].reshape(3, 2, hidden)
    plane_rows = lax.dynamic_index_in_dim(plane_rows, t % 2, 1, False)
    mine_rows = lax.dynamic_slice(tile_own, (6, (4 * d + t) * per), (6, per))
    return (
        out_rows,
        token_rows.astype(F32),
        finals[0].reshape(w_qkv.shape),
        lax.dynamic_slice(plane_rows, (0, d * per), (2, per)),
        finals[1].T,
        finals[2],
        lax.dynamic_slice(plane_rows, (2, d * bias_up.shape[0]), (1, bias_up.shape[0]))[0],
        finals[3].T,
        mine_rows[:2],
        mine_rows[2:],
    )


def solution(mesh):
    return jax.shard_map(
        chip_local if dict(mesh.shape) == {"dp": 8, "tensor": 4} else local,
        mesh=mesh,
        in_specs=(
            P("dp", "tensor", None),
            P("dp"),
            P("dp", None, "tensor"),
            P(None, ("tensor", "dp")),
            P("tensor", "dp"),
            P("dp", "tensor"),
            P(("tensor", "dp")),
            P("tensor", "dp"),
            P(None, ("dp", "tensor")),
            P(None, ("dp", "tensor")),
            P("dp", "tensor", None),
        ),
        out_specs=(
            P("dp", "tensor", None),
            P("dp", "tensor", None),
            P("dp", None, "tensor"),
            P(None, ("tensor", "dp")),
            P("tensor", "dp"),
            P("dp", "tensor"),
            P(("tensor", "dp")),
            P("tensor", "dp"),
            P(None, ("dp", "tensor")),
            P(None, ("dp", "tensor")),
        ),
        check_vma=False,
    )
```
